32 devices in a mesh: px: 2 (over x), py: 16 (over z, y, core).
Axes of the slice: x: 2, y: 2, z: 4, core: 2. Of those that a mesh axis runs over, the one named last changes fastest.
Arguments:
- populations: float32 [19, 2, 256, 512], P(None, None, ('py', 'px')), may hold values from 0.02 to 0.12
- pore: int32 [2, 256, 512], P(None, ('py', 'px')), may hold values 0 or 1
Outputs:
- flow: float32 [19, 2, 256, 512], P(None, None, 'py', 'px')
The draws below stay inside these ranges and needn't reach their ends.
All inputs are finite; a program needn't handle non-finite values. No bound on the sum of `pore` on one device may be relied on, other than what follows from the above.
Results may differ from the reference program's by a relative error of at most 0.0001.
Values sent between devices are 32-bit elements; how exact they have to be, the bound alone decides.
A program may use at most 128 MiB of HBM per device.

```python
import jax
import jax.numpy as jnp

Q = 19
NZ = 2
STEPS = 2
NX = 512
NY = 256


def with_ends(values, key, least, largest):
    extent = values.shape
    index_at = [jax.random.randint(jax.random.fold_in(key, axis), (), 0, extent[axis]) for axis in range(len(extent))]
    values = values.at[tuple(index_at)].set(least)
    longest = extent.index(max(extent))
    index_at[longest] = (index_at[longest] + 1) % extent[longest]
    return values.at[tuple(index_at)].set(largest)


def block_levels(rng, dims, shards, low, top_value):
    factor_of = 1.0
    for dim, blocks in shards:
        heights = jax.random.uniform(jax.random.fold_in(jax.random.fold_in(rng, 6), dim), (blocks,), jnp.float32, low / len(shards), top_value / len(shards))
        factor_of = factor_of * jnp.repeat(jnp.exp(heights), dims[dim] // blocks).reshape((-1,) + (1,) * (len(dims) - 1 - dim))
    return factor_of


def setup_inputs(seed: int = 0) -> dict:
    streams_of = jax.random.split(jax.random.key(seed), 3)
    populations = jnp.clip(0.02 + 0.09999999776482582 * jax.random.uniform(streams_of[0], (Q, NZ, NY, NX), jnp.float32) ** block_levels(streams_of[0], (Q, NZ, NY, NX), ((2, 32),), -0.2, 0.2), 0.02, 0.12)
    pore = with_ends((jax.random.randint(streams_of[1], (NZ, NY, NX), 0, 4) < 3).astype(jnp.int32), jax.random.fold_in(streams_of[1], 1), 0, 1)
    return {"populations": populations, "pore": pore}


lattice_velocity = [(0, 0, 0), (1, 0, 0), (-1, 0, 0), (0, 1, 0), (0, -1, 0), (0, 0, 1), (0, 0, -1),
                    (1, 1, 0), (-1, -1, 0), (1, -1, 0), (-1, 1, 0), (1, 0, 1), (-1, 0, -1), (1, 0, -1),
                    (-1, 0, 1), (0, 1, 1), (0, -1, -1), (0, 1, -1), (0, -1, 1)]
lattice_weights = [1.0 / 3.0] + [1.0 / 18.0] * 6 + [1.0 / 36.0] * 12
opposite = [0, 2, 1, 4, 3, 6, 5, 8, 7, 10, 9, 12, 11, 14, 13, 16, 15, 18, 17]
relax_time = 0.8
body_force = 0.005


def moment(fields, column):
    total = jnp.zeros_like(fields[0])
    for slot in range(len(lattice_velocity)):
        vector = lattice_velocity[slot]
        if vector[column] != 0:
            total = total + float(vector[column]) * fields[slot]
    return total


def collide(fields, fluid):
    density = jnp.where(fluid > 0.5, jnp.sum(fields, axis=0), 1.0)
    vel_first = moment(fields, 0) / density
    vel_second = moment(fields, 1) / density
    vel_third = moment(fields, 2) / density + relax_time * body_force
    speed = vel_first * vel_first + vel_second * vel_second + vel_third * vel_third
    result = []
    for slot in range(len(lattice_velocity)):
        vector = lattice_velocity[slot]
        along = vector[0] * vel_first + vector[1] * vel_second + vector[2] * vel_third
        equil = lattice_weights[slot] * density * (1.0 + 3.0 * along + 4.5 * along * along - 1.5 * speed)
        result.append(fields[slot] - (fields[slot] - equil) / relax_time)
    return jnp.stack(result) * fluid[None]


def reference(populations, pore):
    fluid = pore.astype(jnp.float32)
    fields = populations
    for step in range(STEPS):
        post = collide(fields, fluid)
        result = []
        for slot in range(len(lattice_velocity)):
            vector = lattice_velocity[slot]
            source = jnp.roll(post[slot], (vector[2], vector[1], vector[0]), axis=(0, 1, 2))
            open_cell = jnp.roll(fluid, (vector[2], vector[1], vector[0]), axis=(0, 1, 2))
            result.append(jnp.where(open_cell > 0.5, source, post[opposite[slot]]))
        fields = jnp.stack(result) * fluid[None]
    return fields
```

```python
import functools

import jax
import jax.numpy as jnp
from jax import lax
from jax.experimental import pallas as pl
from jax.experimental.pallas import tpu as pltpu
from jax.sharding import PartitionSpec as P

MESH = pl.DeviceIdType.MESH

lattice_velocity = [
    (0, 0, 0),
    (1, 0, 0),
    (-1, 0, 0),
    (0, 1, 0),
    (0, -1, 0),
    (0, 0, 1),
    (0, 0, -1),
    (1, 1, 0),
    (-1, -1, 0),
    (1, -1, 0),
    (-1, 1, 0),
    (1, 0, 1),
    (-1, 0, -1),
    (1, 0, -1),
    (-1, 0, 1),
    (0, 1, 1),
    (0, -1, -1),
    (0, 1, -1),
    (0, -1, 1),
]
lattice_weights = [1.0 / 3.0] + [1.0 / 18.0] * 6 + [1.0 / 36.0] * 12
opposite = [0, 2, 1, 4, 3, 6, 5, 8, 7, 10, 9, 12, 11, 14, 13, 16, 15, 18, 17]
relax_time = 0.8
body_force = 0.005

Q = len(lattice_velocity)
LANES = 128
ROWS = 8
HALO = 2
VMEM_LIMIT = 32 * 1024 * 1024
SOLID = -3.0e38
TINY = 1.0e-30

order = sorted(range(Q), key=lambda slot: lattice_velocity[slot][1])
place_of = [order.index(slot) for slot in range(Q)]
RISE = sum(1 for vector in lattice_velocity if vector[1] < 0)
FALL = Q - sum(1 for vector in lattice_velocity if vector[1] > 0)
REST = place_of[0]


def total(values):
    return functools.reduce(lambda x, y: x + y, values)


def collide_tile(fields, is_open, guard, closed):
    keep = 1.0 - 1.0 / relax_time
    gain = 1.0 / relax_time
    density = jnp.where(is_open, total(fields), 1.0)
    inverse = 1.0 / density
    vel = []
    for column in range(3):
        plus = [fields[s] for s in range(Q) if lattice_velocity[s][column] > 0]
        minus = [fields[s] for s in range(Q) if lattice_velocity[s][column] < 0]
        vel.append((total(plus) - total(minus)) * inverse)
    vel[2] = vel[2] + relax_time * body_force
    speed = vel[0] * vel[0] + vel[1] * vel[1] + vel[2] * vel[2]
    base = 1.0 - 1.5 * speed
    result = [None] * Q
    scaled = {w: density * (gain * w) for w in sorted(set(lattice_weights))}

    def close(value):
        return jnp.where(is_open, value + guard if guard else value, closed)

    result[0] = close(keep * fields[0] + scaled[lattice_weights[0]] * base)
    for slot in range(1, Q, 2):
        other = opposite[slot]
        along = None
        for column in range(3):
            sign = lattice_velocity[slot][column]
            if sign == 0:
                continue
            term = vel[column]
            if along is None:
                along = term if sign > 0 else -term
            else:
                along = along + term if sign > 0 else along - term
        weight = scaled[lattice_weights[slot]]
        triple = 3.0 * along
        even = weight * (base + 0.5 * triple * triple)
        odd = weight * triple
        result[slot] = close(keep * fields[slot] + (even + odd))
        result[other] = close(keep * fields[other] + (even - odd))
    return result


def stream(load, sides, slot, plane, tile, closed):
    tiles, planes = sides
    dx, dy, dz = lattice_velocity[slot]
    source = (plane - dz) % planes
    value = load(slot, source, tile, dy)
    if dx:
        lane = lax.broadcasted_iota(jnp.int32, value.shape, 1)
        beside = load(slot, source, (tile - dx) % tiles, dy)
        value = jnp.where(lane == (LANES - 1 if dx > 0 else 0), beside, value)
        value = pltpu.roll(value, dx % LANES, 1)
    if slot:
        value = jnp.where(value != closed, value, load(opposite[slot], plane, tile, 0))
    return value


def kernel(
    across, along, pop_ref, pore_ref, post2,
    raw, voxels, box, post, sides, ring, packs, edges, ring_edges,
    load_sem, n_send, n_recv, h_send, h_recv,
):
    _, planes, strips, rows, _ = box.shape
    wt = strips // across
    height = across * rows
    groups = edges.shape[0]
    per_group = LANES // 4
    slabs = Q * planes
    me = lax.axis_index("px")
    here = lax.axis_index("py")
    up = lax.rem(here + along - 1, along)
    down = lax.rem(here + 1, along)

    load_pore = pltpu.make_async_copy(pore_ref, voxels, load_sem.at[0])
    load_pore.start()

    def load_tile(step, k):
        tile = lax.rem(me + step, across) * wt + k
        cols = pl.ds(pl.multiple_of(tile * LANES, LANES), LANES)
        return pltpu.make_async_copy(
            pop_ref.at[:, :, :, cols], raw.at[:, :, tile], load_sem.at[1 + (step - 1) * wt + k]
        )

    for step in range(1, across + 1):
        for k in range(wt):
            load_tile(step, k).start()

    barrier = pltpu.get_barrier_semaphore()
    for step in range(1, across):
        pl.semaphore_signal(barrier, inc=1, device_id=(lax.rem(me + step, across), here), device_id_type=MESH)
    for to in (up, down):
        pl.semaphore_signal(barrier, inc=1, device_id=(me, to), device_id_type=MESH)
    load_pore.wait()

    def collide_strip(tile, own):
        cols = pl.ds(pl.multiple_of(tile * LANES, LANES), LANES)
        for plane in range(planes):
            fields = [raw[slot, plane, tile] for slot in range(Q)]
            is_open = voxels[plane, :, cols] > 0
            result = collide_tile(fields, is_open, TINY, 0.0)
            for slot in range(Q):
                box[place_of[slot], plane, tile] = result[slot]
                if own is not None:
                    at = pl.ds(pl.multiple_of(me * rows, ROWS), rows)
                    post[place_of[slot], plane, own, at, :] = result[slot]

    def outer(source):
        return (rows - HALO, rows) if source == across - 1 else (0, HALO)

    def inner(source):
        return (0, HALO) if source == across - 1 else (rows - HALO, rows)

    def rest(source):
        return (0, rows - HALO) if source == across - 1 else (HALO, rows)

    def middle(source):
        return (HALO, rows - HALO)

    def send(source, target, n):
        if n == 1:
            src, dst = packs.at[target], edges.at[:, source * rows : (source + 1) * rows, :]
        else:
            low, high = (outer, None, rest, inner, middle)[n](source)
            first, last = ((0, wt), None, (0, wt - 1), (wt - 1, wt), (wt - 1, wt))[n]
            src = box.at[:, :, target * wt + first : target * wt + last, low:high, :]
            start = source * rows
            dst = post.at[:, :, first:last, start + low : start + high, :]
        return pltpu.make_async_remote_copy(
            src_ref=src,
            dst_ref=dst,
            send_sem=n_send.at[target, n],
            recv_sem=n_recv.at[source, n],
            device_id=(target, here),
            device_id_type=MESH,
        )

    pieces = [0, 1, 2, 3, 4] if wt > 1 else [0, 1, 3, 4]

    def relay(way):
        if way == 0:
            near, beyond, part, to = 0, 1, (0, RISE), up
            near_to, beyond_to, low, low_to = ROWS - 2, ROWS - 1, 0, ROWS - HALO
        else:
            near, beyond, part, to = height - 1, height - 2, (FALL, Q), down
            near_to, beyond_to, low, low_to = 1, 0, height - HALO, 0
        some = slice(*part)
        refs = [
            (post.at[:, :, :, near : near + 1, :],
             ring.at[:, :, 0:wt, near_to : near_to + 1, :]),
            (post.at[some, :, :, beyond : beyond + 1, :],
             ring.at[some, :, 0:wt, beyond_to : beyond_to + 1, :]),
            (edges.at[:, low : low + HALO, :], ring_edges.at[:, low_to : low_to + HALO, :]),
        ]
        return [
            pltpu.make_async_remote_copy(
                src_ref=src,
                dst_ref=dst,
                send_sem=h_send.at[way, n],
                recv_sem=h_recv.at[way, n],
                device_id=(me, to),
                device_id_type=MESH,
            )
            for n, (src, dst) in enumerate(refs)
        ]

    def peers(mine):
        return [(mine + step) % across for step in range(1, across)]

    def on_each(action):
        for mine in range(across):
            pl.when(me == mine)(functools.partial(action, mine))

    def begin(wanted):
        def action(mine):
            for n in pieces:
                if n in wanted:
                    for target in peers(mine):
                        send(mine, target, n).start()

        on_each(action)

    for step in range(1, across):
        for k in range(wt):
            load_tile(step, k).wait()
            collide_strip(lax.rem(me + step, across) * wt + k, None)
        if step == 1:
            pl.semaphore_wait(barrier, across - 1 + 2)
    begin((0,))
    for k in range(wt):
        load_tile(across, k).wait()
        collide_strip(me * wt + k, k)

    lane = lax.broadcasted_iota(jnp.int32, (rows, LANES), 1)
    for step in range(1, across + 1):
        target = lax.rem(me + step, across)
        first = lax.rem((target + 1) * wt, strips)
        last = lax.rem(target * wt + strips - 1, strips)
        own_at = pl.ds(pl.multiple_of(me * rows, ROWS), rows)
        for group in range(groups):
            packed = jnp.zeros((rows, LANES), jnp.float32)
            for place in range(per_group):
                slab = group * per_group + place
                if slab >= slabs:
                    break
                field, plane = slab // planes, slab % planes
                edge = jnp.where(lane < LANES // 2, box[field, plane, first], box[field, plane, last])
                if step == across:
                    sides[field, plane, own_at, :] = edge
                if place == 0:
                    packed = edge
                else:
                    moved = pltpu.roll(edge, 4 * place, 1)
                    packed = jnp.where((lane >= 4 * place - 2) & (lane < 4 * place + 2), moved, packed)
            if step == across:
                edges[group, own_at, :] = packed
            else:
                packs[target, group] = packed
        if step == across - 1:
            begin((1, 2, 3, 4))

    ends = ((0, 0), (across - 1, 1))

    def relay_own(mine):
        for source, way in ends:
            if source == mine:
                for copy in relay(way):
                    copy.start()

    on_each(relay_own)

    def unpack(packs_of, at, store):
        for slab in range(slabs):
            group, place = slab // per_group, slab % per_group
            packed = packs_of[group, at, :]
            moved = pltpu.roll(packed, LANES - 4 * place, 1) if place else packed
            store(slab // planes, slab % planes, moved)

    def relay_rest(mine):
        for source in peers(mine):
            send(source, mine, 0).wait_recv()
            send(source, mine, 1).wait_recv()
            for end, way in ends:
                if source == end:
                    for copy in relay(way):
                        copy.start()

    on_each(relay_rest)

    def settle(wanted):
        def action(mine):
            for source in peers(mine):
                for n in pieces:
                    if n in wanted:
                        send(source, mine, n).wait_recv()

        on_each(action)

    def advance(load, store):
        for plane in range(planes):
            for tile in range(wt + 1):
                is_open = load(0, plane, tile, 0) != 0.0
                fields = [stream(load, (wt + 1, planes), slot, plane, tile, 0.0) for slot in range(Q)]
                result = collide_tile(fields, is_open, None, SOLID)
                for slot in range(Q):
                    store(slot, plane, tile, result[slot])

    def window(source):
        start = jnp.minimum(rows * source + 1, height - 1 - ROWS)

        def load(slot, plane, tile, dy):
            at = pl.ds(start - dy, ROWS)
            if tile == wt:
                return sides[place_of[slot], plane, at, :]
            return post[place_of[slot], plane, tile, at, :]

        def store(slot, plane, tile, value):
            post2[place_of[slot], plane, tile, pl.ds(ROWS + start, ROWS), :] = value

        advance(load, store)

    row = lax.broadcasted_iota(jnp.int32, (ROWS, LANES), 0)
    half = ROWS // 2

    def fill():
        for slot in range(Q):
            for plane in range(planes):
                for tile in range(wt):
                    ring[slot, plane, tile, HALO:half, :] = post[slot, plane, tile, 0:HALO, :]
                    ring[slot, plane, tile, half : half + HALO, :] = post[
                        slot, plane, tile, height - HALO : height, :
                    ]
        for group in range(groups):
            ring_edges[group, HALO:half, :] = edges[group, 0:HALO, :]
            ring_edges[group, half : half + HALO, :] = edges[group, height - HALO : height, :]

    def rim():
        top, low = ROWS - HALO, height + HALO

        def load(slot, plane, tile, dy):
            value = ring[place_of[slot], plane, tile]
            return pltpu.roll(value, dy % ROWS, 0) if dy else value

        def store(slot, plane, tile, value):
            place = place_of[slot]
            pltpu.store(
                post2.at[place, plane, tile, top : top + ROWS, :], value,
                mask=(row >= 1) & (row < 3),
            )
            pltpu.store(
                post2.at[place, plane, tile, low : low + ROWS, :], value,
                mask=(row >= half + 1) & (row < half + 3),
            )

        advance(load, store)

    def unpack_from(step, carry):
        at = pl.ds(pl.multiple_of(lax.rem(me + step, across) * rows, ROWS), rows)

        def store(slot, plane, value):
            sides[slot, plane, at, :] = value

        unpack(edges, at, store)
        return carry

    def unpack_ring():
        def store(slot, plane, value):
            ring[slot, plane, wt] = value

        unpack(ring_edges, pl.ds(0, ROWS), store)

    lax.fori_loop(1, across, unpack_from, 0)
    fill()
    settle((2, 3))
    window(me)
    for way in range(2):
        for copy in relay(way):
            copy.wait_recv()
    unpack_ring()
    rim()
    settle((4,))

    def window_from(step, carry):
        window(lax.rem(me + step, across))
        return carry

    lax.fori_loop(1, across, window_from, 0)

    def sent(mine):
        for target in peers(mine):
            for n in pieces:
                send(mine, target, n).wait_send()
        for way in range(2):
            for copy in relay(way):
                copy.wait_send()

    on_each(sent)


def finish(post, out_ref, flow, sems):
    _, planes, height, width = flow.shape
    wt = width // LANES

    def load(slot, plane, tile, dy):
        return post[place_of[slot], plane, tile, at - dy : at - dy + ROWS, :]

    copies = []
    for slot in range(Q):
        for plane in range(planes):
            for tile in range(wt):
                for start in range(0, height, ROWS):
                    at = ROWS + start
                    is_open = load(0, plane, tile, 0) != SOLID
                    value = stream(load, (wt + 1, planes), slot, plane, tile, SOLID)
                    flow[slot, plane, start : start + ROWS, tile * LANES : (tile + 1) * LANES] = jnp.where(
                        is_open, value, 0.0
                    )
        copies.append(pltpu.make_async_copy(flow.at[slot], out_ref.at[slot], sems.at[slot]))
        if slot:
            copies[slot - 1].start()
    copies[-1].start()
    for copy in copies:
        copy.wait()


def body(across, along, populations, pore):
    count, planes, rows, columns = populations.shape
    height = across * rows
    width = columns // across
    strips = columns // LANES
    wt = strips // across
    groups = -(-count * planes * 4 // LANES)
    tall = height + 2 * ROWS
    post2 = pl.pallas_call(
        functools.partial(kernel, across, along),
        out_shape=pltpu.VMEM((count, planes, wt + 1, tall, LANES), jnp.float32),
        in_specs=[pl.BlockSpec(memory_space=pltpu.HBM)] * 2,
        out_specs=pl.BlockSpec(memory_space=pltpu.VMEM),
        scratch_shapes=[
            pltpu.VMEM((count, planes, strips, rows, LANES), jnp.float32),
            pltpu.VMEM((planes, rows, columns), jnp.int32),
            pltpu.VMEM((count, planes, strips, rows, LANES), jnp.float32),
            pltpu.VMEM((count, planes, wt, height, LANES), jnp.float32),
            pltpu.VMEM((count, planes, height, LANES), jnp.float32),
            pltpu.VMEM((count, planes, wt + 1, ROWS, LANES), jnp.float32),
            pltpu.VMEM((across, groups, rows, LANES), jnp.float32),
            pltpu.VMEM((groups, height, LANES), jnp.float32),
            pltpu.VMEM((groups, ROWS, LANES), jnp.float32),
            pltpu.SemaphoreType.DMA((1 + strips,)),
            pltpu.SemaphoreType.DMA((across, 5)),
            pltpu.SemaphoreType.DMA((across, 5)),
            pltpu.SemaphoreType.DMA((2, 3)),
            pltpu.SemaphoreType.DMA((2, 3)),
        ],
        compiler_params=pltpu.CompilerParams(
            collective_id=0, has_side_effects=True, vmem_limit_bytes=VMEM_LIMIT
        ),
    )(*(pltpu.with_memory_space_constraint(x, pltpu.HBM) for x in (populations, pore)))
    return pl.pallas_call(
        finish,
        out_shape=jax.ShapeDtypeStruct((count, planes, height, width), jnp.float32),
        in_specs=[pl.BlockSpec(memory_space=pltpu.VMEM)],
        out_specs=pl.BlockSpec(memory_space=pl.ANY),
        scratch_shapes=[
            pltpu.VMEM((count, planes, height, width), jnp.float32),
            pltpu.SemaphoreType.DMA((count,)),
        ],
        compiler_params=pltpu.CompilerParams(vmem_limit_bytes=VMEM_LIMIT),
    )(post2)


def solution(mesh):
    return jax.shard_map(
        functools.partial(body, mesh.shape["px"], mesh.shape["py"]),
        mesh=mesh,
        in_specs=(P(None, None, ("py", "px"), None), P(None, ("py", "px"), None)),
        out_specs=P(None, None, "py", "px"),
        check_vma=False,
    )
```

```python
import functools

import jax
import jax.numpy as jnp
from jax import lax
from jax.experimental import pallas as pl
from jax.experimental.pallas import tpu as pltpu
from jax.sharding import PartitionSpec as P

MESH = pl.DeviceIdType.MESH

lattice_velocity = [
    (0, 0, 0),
    (1, 0, 0),
    (-1, 0, 0),
    (0, 1, 0),
    (0, -1, 0),
    (0, 0, 1),
    (0, 0, -1),
    (1, 1, 0),
    (-1, -1, 0),
    (1, -1, 0),
    (-1, 1, 0),
    (1, 0, 1),
    (-1, 0, -1),
    (1, 0, -1),
    (-1, 0, 1),
    (0, 1, 1),
    (0, -1, -1),
    (0, 1, -1),
    (0, -1, 1),
]
lattice_weights = [1.0 / 3.0] + [1.0 / 18.0] * 6 + [1.0 / 36.0] * 12
opposite = [0, 2, 1, 4, 3, 6, 5, 8, 7, 10, 9, 12, 11, 14, 13, 16, 15, 18, 17]
relax_time = 0.8
body_force = 0.005

Q = len(lattice_velocity)
LANES = 128
ROWS = 8
HALO = 2
VMEM_LIMIT = 32 * 1024 * 1024
SOLID = -3.0e38
TINY = 1.0e-30

order = sorted(range(Q), key=lambda slot: lattice_velocity[slot][1])
place_of = [order.index(slot) for slot in range(Q)]
RISE = sum(1 for vector in lattice_velocity if vector[1] < 0)
FALL = Q - sum(1 for vector in lattice_velocity if vector[1] > 0)
REST = place_of[0]


def total(values):
    return functools.reduce(lambda x, y: x + y, values)


def collide_tile(fields, is_open, guard, closed):
    keep = 1.0 - 1.0 / relax_time
    gain = 1.0 / relax_time
    density = jnp.where(is_open, total(fields), 1.0)
    inverse = 1.0 / density
    vel = []
    for column in range(3):
        plus = [fields[s] for s in range(Q) if lattice_velocity[s][column] > 0]
        minus = [fields[s] for s in range(Q) if lattice_velocity[s][column] < 0]
        vel.append((total(plus) - total(minus)) * inverse)
    vel[2] = vel[2] + relax_time * body_force
    speed = vel[0] * vel[0] + vel[1] * vel[1] + vel[2] * vel[2]
    base = 1.0 - 1.5 * speed
    result = [None] * Q
    scaled = {w: density * (gain * w) for w in sorted(set(lattice_weights))}

    def close(value):
        return jnp.where(is_open, value + guard if guard else value, closed)

    result[0] = close(keep * fields[0] + scaled[lattice_weights[0]] * base)
    for slot in range(1, Q, 2):
        other = opposite[slot]
        along = None
        for column in range(3):
            sign = lattice_velocity[slot][column]
            if sign == 0:
                continue
            term = vel[column]
            if along is None:
                along = term if sign > 0 else -term
            else:
                along = along + term if sign > 0 else along - term
        weight = scaled[lattice_weights[slot]]
        triple = 3.0 * along
        even = weight * (base + 0.5 * triple * triple)
        odd = weight * triple
        result[slot] = close(keep * fields[slot] + (even + odd))
        result[other] = close(keep * fields[other] + (even - odd))
    return result


def stream(load, sides, slot, plane, tile, closed):
    tiles, planes = sides
    dx, dy, dz = lattice_velocity[slot]
    source = (plane - dz) % planes
    value = load(slot, source, tile, dy)
    if dx:
        lane = lax.broadcasted_iota(jnp.int32, value.shape, 1)
        beside = load(slot, source, (tile - dx) % tiles, dy)
        value = jnp.where(lane == (LANES - 1 if dx > 0 else 0), beside, value)
        value = pltpu.roll(value, dx % LANES, 1)
    if slot:
        value = jnp.where(value != closed, value, load(opposite[slot], plane, tile, 0))
    return value


def kernel(
    across, along, pop_ref, pore_ref, post2,
    raw, voxels, box, post, sides, ring, packs, edges, ring_edges,
    load_sem, n_send, n_recv, h_send, h_recv, w_send, go,
):
    _, planes, strips, rows, _ = box.shape
    wt = strips // across
    height = across * rows
    groups = edges.shape[0]
    per_group = LANES // 4
    slabs = Q * planes
    me = lax.axis_index("px")
    here = lax.axis_index("py")
    up = lax.rem(here + along - 1, along)
    down = lax.rem(here + 1, along)
    first_row = here == 0
    last_row = here == along - 1
    odd = lax.rem(here, 2) == 1
    eager = odd & (here != along - 1)

    load_pore = pltpu.make_async_copy(pore_ref, voxels, load_sem.at[0])
    load_pore.start()

    def load_tile(step, k):
        tile = lax.rem(me + step, across) * wt + k
        cols = pl.ds(pl.multiple_of(tile * LANES, LANES), LANES)
        return pltpu.make_async_copy(
            pop_ref.at[:, :, :, cols], raw.at[:, :, tile], load_sem.at[1 + (step - 1) * wt + k]
        )

    for step in range(1, across + 1):
        for k in range(wt):
            load_tile(step, k).start()

    barrier = pltpu.get_barrier_semaphore()

    def greet(x, y):
        pl.semaphore_signal(barrier, inc=1, device_id=(x, y), device_id_type=MESH)

    for step in range(1, across):
        greet(lax.rem(me + step, across), here)

    @pl.when(here == along - 2)
    def _():
        greet(me, down)

    @pl.when(last_row)
    def _():
        greet(me, up)

    @pl.when(eager)
    def _():
        pl.semaphore_wait(barrier, across - 1)
        greet(me, up)
        greet(me, down)

    def enter():
        @pl.when(first_row)
        def _():
            pl.semaphore_wait(barrier, across - 1 + 1)
            greet(me, down)
            greet(me, along - 1)

            @pl.when(me != across - 1)
            def _():
                greet(across - 1, along - 1)

        @pl.when(last_row & (me != across - 1))
        def _():
            pl.semaphore_wait(barrier, across - 1 + 2)
            greet(me, 0)

        @pl.when(last_row & (me == across - 1))
        def _():
            pl.semaphore_wait(barrier, across - 1 + 2 + across - 1)
            greet(me, 0)

        @pl.when(jnp.logical_not(odd) & (here != 0))
        def _():
            pl.semaphore_wait(barrier, across - 1 + 2)
            greet(me, up)

            @pl.when(here != along - 2)
            def _():
                greet(me, down)

    load_pore.wait()

    def collide_strip(tile, own):
        cols = pl.ds(pl.multiple_of(tile * LANES, LANES), LANES)
        for plane in range(planes):
            fields = [raw[slot, plane, tile] for slot in range(Q)]
            is_open = voxels[plane, :, cols] > 0
            result = collide_tile(fields, is_open, TINY, 0.0)
            for slot in range(Q):
                box[place_of[slot], plane, tile] = result[slot]
                if own is not None:
                    at = pl.ds(pl.multiple_of(me * rows, ROWS), rows)
                    post[place_of[slot], plane, own, at, :] = result[slot]

    def outer(source):
        return (rows - HALO, rows) if source == across - 1 else (0, HALO)

    def inner(source):
        return (0, HALO) if source == across - 1 else (rows - HALO, rows)

    def rest(source):
        return (0, rows - HALO) if source == across - 1 else (HALO, rows)

    def middle(source):
        return (HALO, rows - HALO)

    def send(source, target, n):
        if n == 1:
            src, dst = packs.at[target], edges.at[:, source * rows : (source + 1) * rows, :]
        else:
            low, high = (outer, None, rest, inner, middle)[n](source)
            first, last = ((0, wt), None, (0, wt - 1), (wt - 1, wt), (wt - 1, wt))[n]
            src = box.at[:, :, target * wt + first : target * wt + last, low:high, :]
            start = source * rows
            dst = post.at[:, :, first:last, start + low : start + high, :]
        return pltpu.make_async_remote_copy(
            src_ref=src,
            dst_ref=dst,
            send_sem=n_send.at[target, n],
            recv_sem=n_recv.at[source, n],
            device_id=(target, here),
            device_id_type=MESH,
        )

    pieces = [0, 1, 2, 3, 4] if wt > 1 else [0, 1, 3, 4]

    def relay(way):
        if way == 0:
            near, beyond, part, to = 0, 1, (0, RISE), up
            near_to, beyond_to, low, low_to = ROWS - 2, ROWS - 1, 0, ROWS - HALO
        else:
            near, beyond, part, to = height - 1, height - 2, (FALL, Q), down
            near_to, beyond_to, low, low_to = 1, 0, height - HALO, 0
        some = slice(*part)
        refs = [
            (post.at[:, :, :, near : near + 1, :],
             ring.at[:, :, 0:wt, near_to : near_to + 1, :]),
            (post.at[some, :, :, beyond : beyond + 1, :],
             ring.at[some, :, 0:wt, beyond_to : beyond_to + 1, :]),
            (edges.at[:, low : low + HALO, :], ring_edges.at[:, low_to : low_to + HALO, :]),
        ]
        return [
            pltpu.make_async_remote_copy(
                src_ref=src,
                dst_ref=dst,
                send_sem=h_send.at[way, n],
                recv_sem=h_recv.at[way, n],
                device_id=(me, to),
                device_id_type=MESH,
            )
            for n, (src, dst) in enumerate(refs)
        ]

    def peers(mine):
        return [(mine + step) % across for step in range(1, across)]

    def on_each(action):
        for mine in range(across):
            pl.when(me == mine)(functools.partial(action, mine))

    def begin(wanted):
        def action(mine):
            for n in pieces:
                if n in wanted:
                    for target in peers(mine):
                        send(mine, target, n).start()

        on_each(action)

    for step in range(1, across):
        for k in range(wt):
            load_tile(step, k).wait()
            collide_strip(lax.rem(me + step, across) * wt + k, None)
        if step == 1:
            enter()
    begin((0,))
    for k in range(wt):
        load_tile(across, k).wait()
        collide_strip(me * wt + k, k)

    lane = lax.broadcasted_iota(jnp.int32, (rows, LANES), 1)
    for step in range(1, across + 1):
        target = lax.rem(me + step, across)
        first = lax.rem((target + 1) * wt, strips)
        last = lax.rem(target * wt + strips - 1, strips)
        own_at = pl.ds(pl.multiple_of(me * rows, ROWS), rows)
        for group in range(groups):
            packed = jnp.zeros((rows, LANES), jnp.float32)
            for place in range(per_group):
                slab = group * per_group + place
                if slab >= slabs:
                    break
                field, plane = slab // planes, slab % planes
                edge = jnp.where(lane < LANES // 2, box[field, plane, first], box[field, plane, last])
                if step == across:
                    sides[field, plane, own_at, :] = edge
                if place == 0:
                    packed = edge
                else:
                    moved = pltpu.roll(edge, 4 * place, 1)
                    packed = jnp.where((lane >= 4 * place - 2) & (lane < 4 * place + 2), moved, packed)
            packs[target, group] = packed
            if step == across:
                edges[group, own_at, :] = packed
        if step == across - 1:
            begin((1,))

            @pl.when(jnp.logical_not(odd))
            def _():
                begin((2, 3, 4))

    ends = ((0, 0), (across - 1, 1))

    def direct(target):
        cols = slice(target * wt, (target + 1) * wt)
        refs = [
            (box.at[:, :, cols, rows - 1 : rows, :], ring.at[:, :, 0:wt, 1:2, :]),
            (box.at[FALL:Q, :, cols, rows - HALO : rows - 1, :], ring.at[FALL:Q, :, 0:wt, 0:1, :]),
            (packs.at[target, :, rows - HALO : rows, :], ring_edges.at[:, 0:HALO, :]),
        ]
        return [
            pltpu.make_async_remote_copy(
                src_ref=src,
                dst_ref=dst,
                send_sem=w_send.at[target, n],
                recv_sem=h_recv.at[1, n],
                device_id=(target, 0),
                device_id_type=MESH,
            )
            for n, (src, dst) in enumerate(refs)
        ]

    last_strip = last_row & (me == across - 1)

    @pl.when(last_strip)
    def _():
        for target in range(across):
            for copy in direct(target):
                copy.start()

    lead = 2 if wt > 1 else 3

    @pl.when(odd)
    def _():
        pl.semaphore_wait(go, 1)
        begin((2, 3, 4))

    def lead_sent(mine):
        for target in peers(mine):
            send(mine, target, lead).wait_send()

    @pl.when(jnp.logical_not(odd))
    def _():
        on_each(lead_sent)
        pl.semaphore_signal(go, inc=1, device_id=(me, down), device_id_type=MESH)

    @pl.when(eager)
    def _():
        pl.semaphore_wait(barrier, 2)

    def unpack(packs_of, at, store):
        for slab in range(slabs):
            group, place = slab // per_group, slab % per_group
            packed = packs_of[group, at, :]
            moved = pltpu.roll(packed, LANES - 4 * place, 1) if place else packed
            store(slab // planes, slab % planes, moved)

    def pass_on(mine, source, way):
        if source != mine:
            send(source, mine, 0).wait_recv()
            send(source, mine, 1).wait_recv()

        def start():
            for copy in relay(way):
                copy.start()

        if way:
            pl.when(jnp.logical_not(last_row))(start)
        else:
            start()

    def relays(mine):
        @pl.when(first_row)
        def _():
            pass_on(mine, across - 1, 1)
            pl.semaphore_wait(barrier, 1)
            pass_on(mine, 0, 0)

        @pl.when(jnp.logical_not(first_row))
        def _():
            for source, way in sorted(ends, key=lambda end: end[0] != mine):
                pass_on(mine, source, way)

        for source in peers(mine):
            if source not in (0, across - 1):
                send(source, mine, 0).wait_recv()
                send(source, mine, 1).wait_recv()

    on_each(relays)

    def settle(wanted):
        def action(mine):
            for source in peers(mine):
                for n in pieces:
                    if n in wanted:
                        send(source, mine, n).wait_recv()

        on_each(action)

    def advance(load, store):
        for plane in range(planes):
            for tile in range(wt + 1):
                is_open = load(0, plane, tile, 0) != 0.0
                fields = [stream(load, (wt + 1, planes), slot, plane, tile, 0.0) for slot in range(Q)]
                result = collide_tile(fields, is_open, None, SOLID)
                for slot in range(Q):
                    store(slot, plane, tile, result[slot])

    def window(source):
        start = jnp.minimum(rows * source + 1, height - 1 - ROWS)

        def load(slot, plane, tile, dy):
            at = pl.ds(start - dy, ROWS)
            if tile == wt:
                return sides[place_of[slot], plane, at, :]
            return post[place_of[slot], plane, tile, at, :]

        def store(slot, plane, tile, value):
            post2[place_of[slot], plane, tile, pl.ds(ROWS + start, ROWS), :] = value

        advance(load, store)

    row = lax.broadcasted_iota(jnp.int32, (ROWS, LANES), 0)
    half = ROWS // 2

    def fill():
        for slot in range(Q):
            for plane in range(planes):
                for tile in range(wt):
                    ring[slot, plane, tile, HALO:half, :] = post[slot, plane, tile, 0:HALO, :]
                    ring[slot, plane, tile, half : half + HALO, :] = post[
                        slot, plane, tile, height - HALO : height, :
                    ]
        for group in range(groups):
            ring_edges[group, HALO:half, :] = edges[group, 0:HALO, :]
            ring_edges[group, half : half + HALO, :] = edges[group, height - HALO : height, :]

    def rim():
        top, low = ROWS - HALO, height + HALO

        def load(slot, plane, tile, dy):
            value = ring[place_of[slot], plane, tile]
            return pltpu.roll(value, dy % ROWS, 0) if dy else value

        def store(slot, plane, tile, value):
            place = place_of[slot]
            pltpu.store(
                post2.at[place, plane, tile, top : top + ROWS, :], value,
                mask=(row >= 1) & (row < 3),
            )
            pltpu.store(
                post2.at[place, plane, tile, low : low + ROWS, :], value,
                mask=(row >= half + 1) & (row < half + 3),
            )

        advance(load, store)

    def unpack_from(step, carry):
        at = pl.ds(pl.multiple_of(lax.rem(me + step, across) * rows, ROWS), rows)

        def store(slot, plane, value):
            sides[slot, plane, at, :] = value

        unpack(edges, at, store)
        return carry

    def unpack_ring():
        def store(slot, plane, value):
            ring[slot, plane, wt] = value

        unpack(ring_edges, pl.ds(0, ROWS), store)

    lax.fori_loop(1, across, unpack_from, 0)
    fill()
    settle((2, 3))
    window(me)
    for way in range(2):
        for copy in relay(way):
            copy.wait_recv()
    unpack_ring()
    rim()
    settle((4,))

    def window_from(step, carry):
        window(lax.rem(me + step, across))
        return carry

    lax.fori_loop(1, across, window_from, 0)

    def sent(mine):
        for target in peers(mine):
            for n in pieces:
                if n == lead:
                    pl.when(odd)(send(mine, target, n).wait_send)
                else:
                    send(mine, target, n).wait_send()

    on_each(sent)
    for copy in relay(0):
        copy.wait_send()

    @pl.when(jnp.logical_not(last_row))
    def _():
        for copy in relay(1):
            copy.wait_send()

    @pl.when(last_strip)
    def _():
        for target in range(across):
            for copy in direct(target):
                copy.wait_send()


def finish(post, out_ref, flow, sems):
    _, planes, height, width = flow.shape
    wt = width // LANES

    def load(slot, plane, tile, dy):
        return post[place_of[slot], plane, tile, at - dy : at - dy + ROWS, :]

    copies = []
    for slot in range(Q):
        for plane in range(planes):
            for tile in range(wt):
                for start in range(0, height, ROWS):
                    at = ROWS + start
                    is_open = load(0, plane, tile, 0) != SOLID
                    value = stream(load, (wt + 1, planes), slot, plane, tile, SOLID)
                    flow[slot, plane, start : start + ROWS, tile * LANES : (tile + 1) * LANES] = jnp.where(
                        is_open, value, 0.0
                    )
        copies.append(pltpu.make_async_copy(flow.at[slot], out_ref.at[slot], sems.at[slot]))
        if slot:
            copies[slot - 1].start()
    copies[-1].start()
    for copy in copies:
        copy.wait()


def body(across, along, populations, pore):
    count, planes, rows, columns = populations.shape
    height = across * rows
    width = columns // across
    strips = columns // LANES
    wt = strips // across
    groups = -(-count * planes * 4 // LANES)
    tall = height + 2 * ROWS
    post2 = pl.pallas_call(
        functools.partial(kernel, across, along),
        out_shape=pltpu.VMEM((count, planes, wt + 1, tall, LANES), jnp.float32),
        in_specs=[pl.BlockSpec(memory_space=pltpu.HBM)] * 2,
        out_specs=pl.BlockSpec(memory_space=pltpu.VMEM),
        scratch_shapes=[
            pltpu.VMEM((count, planes, strips, rows, LANES), jnp.float32),
            pltpu.VMEM((planes, rows, columns), jnp.int32),
            pltpu.VMEM((count, planes, strips, rows, LANES), jnp.float32),
            pltpu.VMEM((count, planes, wt, height, LANES), jnp.float32),
            pltpu.VMEM((count, planes, height, LANES), jnp.float32),
            pltpu.VMEM((count, planes, wt + 1, ROWS, LANES), jnp.float32),
            pltpu.VMEM((across, groups, rows, LANES), jnp.float32),
            pltpu.VMEM((groups, height, LANES), jnp.float32),
            pltpu.VMEM((groups, ROWS, LANES), jnp.float32),
            pltpu.SemaphoreType.DMA((1 + strips,)),
            pltpu.SemaphoreType.DMA((across, 5)),
            pltpu.SemaphoreType.DMA((across, 5)),
            pltpu.SemaphoreType.DMA((2, 3)),
            pltpu.SemaphoreType.DMA((2, 3)),
            pltpu.SemaphoreType.DMA((across, 3)),
            pltpu.SemaphoreType.REGULAR,
        ],
        compiler_params=pltpu.CompilerParams(
            collective_id=0, has_side_effects=True, vmem_limit_bytes=VMEM_LIMIT
        ),
    )(*(pltpu.with_memory_space_constraint(x, pltpu.HBM) for x in (populations, pore)))
    return pl.pallas_call(
        finish,
        out_shape=jax.ShapeDtypeStruct((count, planes, height, width), jnp.float32),
        in_specs=[pl.BlockSpec(memory_space=pltpu.VMEM)],
        out_specs=pl.BlockSpec(memory_space=pl.ANY),
        scratch_shapes=[
            pltpu.VMEM((count, planes, height, width), jnp.float32),
            pltpu.SemaphoreType.DMA((count,)),
        ],
        compiler_params=pltpu.CompilerParams(vmem_limit_bytes=VMEM_LIMIT),
    )(post2)


def solution(mesh):
    return jax.shard_map(
        functools.partial(body, mesh.shape["px"], mesh.shape["py"]),
        mesh=mesh,
        in_specs=(P(None, None, ("py", "px"), None), P(None, ("py", "px"), None)),
        out_specs=P(None, None, "py", "px"),
        check_vma=False,
    )
```

```python
import functools

import jax
import jax.numpy as jnp
from jax import lax
from jax.experimental import pallas as pl
from jax.experimental.pallas import tpu as pltpu
from jax.sharding import PartitionSpec as P

MESH = pl.DeviceIdType.MESH

lattice_velocity = [
    (0, 0, 0),
    (1, 0, 0),
    (-1, 0, 0),
    (0, 1, 0),
    (0, -1, 0),
    (0, 0, 1),
    (0, 0, -1),
    (1, 1, 0),
    (-1, -1, 0),
    (1, -1, 0),
    (-1, 1, 0),
    (1, 0, 1),
    (-1, 0, -1),
    (1, 0, -1),
    (-1, 0, 1),
    (0, 1, 1),
    (0, -1, -1),
    (0, 1, -1),
    (0, -1, 1),
]
lattice_weights = [1.0 / 3.0] + [1.0 / 18.0] * 6 + [1.0 / 36.0] * 12
opposite = [0, 2, 1, 4, 3, 6, 5, 8, 7, 10, 9, 12, 11, 14, 13, 16, 15, 18, 17]
relax_time = 0.8
body_force = 0.005

Q = len(lattice_velocity)
LANES = 128
ROWS = 8
HALO = 2
VMEM_LIMIT = 32 * 1024 * 1024
SOLID = -3.0e38
TINY = 1.0e-30

order = sorted(range(Q), key=lambda slot: lattice_velocity[slot][1])
place_of = [order.index(slot) for slot in range(Q)]
RISE = sum(1 for vector in lattice_velocity if vector[1] < 0)
FALL = Q - sum(1 for vector in lattice_velocity if vector[1] > 0)
PAIRS = [(s, opposite[s]) for s in range(Q) if lattice_velocity[s][0] > 0]


def total(values):
    return functools.reduce(lambda x, y: x + y, values)


def collide_tile(fields, is_open, guard, closed):
    keep = 1.0 - 1.0 / relax_time
    gain = 1.0 / relax_time
    density = jnp.where(is_open, total(fields), 1.0)
    inverse = 1.0 / density
    vel = []
    for column in range(3):
        plus = [fields[s] for s in range(Q) if lattice_velocity[s][column] > 0]
        minus = [fields[s] for s in range(Q) if lattice_velocity[s][column] < 0]
        vel.append((total(plus) - total(minus)) * inverse)
    vel[2] = vel[2] + relax_time * body_force
    speed = vel[0] * vel[0] + vel[1] * vel[1] + vel[2] * vel[2]
    base = 1.0 - 1.5 * speed
    result = [None] * Q
    scaled = {w: density * (gain * w) for w in sorted(set(lattice_weights))}

    def close(value):
        return jnp.where(is_open, value + guard if guard else value, closed)

    result[0] = close(keep * fields[0] + scaled[lattice_weights[0]] * base)
    for slot in range(1, Q, 2):
        other = opposite[slot]
        along = None
        for column in range(3):
            sign = lattice_velocity[slot][column]
            if sign == 0:
                continue
            term = vel[column]
            if along is None:
                along = term if sign > 0 else -term
            else:
                along = along + term if sign > 0 else along - term
        weight = scaled[lattice_weights[slot]]
        triple = 3.0 * along
        even = weight * (base + 0.5 * triple * triple)
        odd = weight * triple
        result[slot] = close(keep * fields[slot] + (even + odd))
        result[other] = close(keep * fields[other] + (even - odd))
    return result


def stream(load, sides, slot, plane, tile, closed, seam=None):
    tiles, planes = sides
    dx, dy, dz = lattice_velocity[slot]
    source = (plane - dz) % planes
    value = load(slot, source, tile, dy)
    if dx:
        lane = lax.broadcasted_iota(jnp.int32, value.shape, 1)
        beside = (seam or load)(slot, source, (tile - dx) % tiles, dy)
        value = jnp.where(lane == (LANES - 1 if dx > 0 else 0), beside, value)
        value = pltpu.roll(value, dx % LANES, 1)
    if slot:
        value = jnp.where(value != closed, value, load(opposite[slot], plane, tile, 0))
    return value


def kernel(
    across, along, pop_ref, pore_ref, post2,
    raw, voxels, box, post, sides, seams, ring, packs, edges, ring_edges,
    load_sem, n_send, n_recv, h_send, h_recv, w_send, go, ready,
):
    _, planes, strips, rows, _ = box.shape
    wt = strips // across
    height = across * rows
    groups = edges.shape[0]
    per_group = LANES // 4
    slabs = Q * planes
    me = lax.axis_index("px")
    here = lax.axis_index("py")
    up = lax.rem(here + along - 1, along)
    down = lax.rem(here + 1, along)
    first_row = here == 0
    last_row = here == along - 1
    odd = lax.rem(here, 2) == 1
    last_strip = last_row & (me == across - 1)

    load_pore = pltpu.make_async_copy(pore_ref, voxels, load_sem.at[0])
    load_pore.start()

    def load_tile(step, k, plane):
        tile = lax.rem(me + step, across) * wt + k
        cols = pl.ds(pl.multiple_of(tile * LANES, LANES), LANES)
        return pltpu.make_async_copy(
            pop_ref.at[:, plane, :, cols],
            raw.at[:, plane, tile],
            load_sem.at[1 + ((step - 1) * wt + k) * planes + plane],
        )

    halves = [(k, plane) for k in range(wt) for plane in range(planes)]
    for step in range(1, across + 1):
        for k, plane in halves:
            load_tile(step, k, plane).start()

    barrier = pltpu.get_barrier_semaphore()

    def greet(x, y):
        pl.semaphore_signal(barrier, inc=1, device_id=(x, y), device_id_type=MESH)

    def answer(y):
        pl.semaphore_signal(ready, inc=1, device_id=(me, y), device_id_type=MESH)

    for step in range(1, across):
        greet(lax.rem(me + step, across), here)

    @pl.when(odd)
    def _():
        greet(me, up)

        @pl.when(jnp.logical_not(last_row))
        def _():
            greet(me, down)

    @pl.when(first_row)
    def _():
        greet(me, along - 1)

        @pl.when(me != across - 1)
        def _():
            greet(across - 1, along - 1)

    def enter():
        greeted = jnp.where(odd, 0, 2) - jnp.where(first_row, 1, 0)
        greeted = greeted + jnp.where(last_row, jnp.where(me == across - 1, across, 1), 0)
        pl.semaphore_wait(barrier, across - 1 + greeted)

        @pl.when(jnp.logical_not(odd))
        def _():
            answer(down)

            @pl.when(here != 0)
            def _():
                answer(up)

        @pl.when(last_row)
        def _():
            answer(0)

    load_pore.wait()

    def collide_strip(tile, plane, own):
        cols = pl.ds(pl.multiple_of(tile * LANES, LANES), LANES)
        fields = [raw[slot, plane, tile] for slot in range(Q)]
        is_open = voxels[plane, :, cols] > 0
        result = collide_tile(fields, is_open, TINY, 0.0)
        for slot in range(Q):
            box[place_of[slot], plane, tile] = result[slot]
            if own is not None:
                at = pl.ds(pl.multiple_of(me * rows, ROWS), rows)
                post[place_of[slot], plane, own, at, :] = result[slot]

    def outer(source):
        return (rows - HALO, rows) if source == across - 1 else (0, HALO)

    def inner(source):
        return (0, HALO) if source == across - 1 else (rows - HALO, rows)

    def rest(source):
        return (0, rows - HALO) if source == across - 1 else (HALO, rows)

    def middle(source):
        return (HALO, rows - HALO)

    def send(source, target, n, part=None):
        if part:
            k, plane = part
            low, high = outer(source)
            return pltpu.make_async_remote_copy(
                src_ref=box.at[:, plane, target * wt + k, low:high, :],
                dst_ref=post.at[:, plane, k, source * rows + low : source * rows + high, :],
                send_sem=n_send.at[target, n],
                recv_sem=n_recv.at[source, n],
                device_id=(target, here),
                device_id_type=MESH,
            )
        if n == 1:
            src, dst = packs.at[target], edges.at[:, source * rows : (source + 1) * rows, :]
        else:
            low, high = (outer, None, rest, inner, middle)[n](source)
            first, last = ((0, wt), None, (0, wt - 1), (wt - 1, wt), (wt - 1, wt))[n]
            src = box.at[:, :, target * wt + first : target * wt + last, low:high, :]
            start = source * rows
            dst = post.at[:, :, first:last, start + low : start + high, :]
        return pltpu.make_async_remote_copy(
            src_ref=src,
            dst_ref=dst,
            send_sem=n_send.at[target, n],
            recv_sem=n_recv.at[source, n],
            device_id=(target, here),
            device_id_type=MESH,
        )

    pieces = [0, 1, 2, 3, 4] if wt > 1 else [0, 1, 3, 4]

    def relay(way):
        if way == 0:
            near, beyond, part, to = 0, 1, (0, RISE), up
            near_to, beyond_to, low, low_to = ROWS - 2, ROWS - 1, 0, ROWS - HALO
        else:
            near, beyond, part, to = height - 1, height - 2, (FALL, Q), down
            near_to, beyond_to, low, low_to = 1, 0, height - HALO, 0
        some = slice(*part)
        refs = [
            (post.at[:, :, :, near : near + 1, :],
             ring.at[:, :, 0:wt, near_to : near_to + 1, :]),
            (post.at[some, :, :, beyond : beyond + 1, :],
             ring.at[some, :, 0:wt, beyond_to : beyond_to + 1, :]),
            (edges.at[:, low : low + HALO, :], ring_edges.at[:, low_to : low_to + HALO, :]),
        ]
        return [
            pltpu.make_async_remote_copy(
                src_ref=src,
                dst_ref=dst,
                send_sem=h_send.at[way, n],
                recv_sem=h_recv.at[way, n],
                device_id=(me, to),
                device_id_type=MESH,
            )
            for n, (src, dst) in enumerate(refs)
        ]

    def peers(mine):
        return [(mine + step) % across for step in range(1, across)]

    def on_each(action):
        for mine in range(across):
            pl.when(me == mine)(functools.partial(action, mine))

    def begin(wanted):
        def action(mine):
            for n in pieces:
                if n in wanted:
                    for target in peers(mine):
                        send(mine, target, n).start()

        on_each(action)

    def direct(target, which=range(3)):
        cols = slice(target * wt, (target + 1) * wt)
        refs = [
            (box.at[:, :, cols, rows - 1 : rows, :], ring.at[:, :, 0:wt, 1:2, :]),
            (box.at[FALL:Q, :, cols, rows - HALO : rows - 1, :], ring.at[FALL:Q, :, 0:wt, 0:1, :]),
            (packs.at[target, :, rows - HALO : rows, :], ring_edges.at[:, 0:HALO, :]),
        ]
        return [
            pltpu.make_async_remote_copy(
                src_ref=src,
                dst_ref=dst,
                send_sem=w_send.at[target, n],
                recv_sem=h_recv.at[1, n],
                device_id=(target, 0),
                device_id_type=MESH,
            )
            for n, (src, dst) in enumerate(refs)
            if n in which
        ]

    def send_direct(targets, which):
        @pl.when(last_strip)
        def _():
            for target in targets:
                for copy in direct(target, which):
                    copy.start()


    for step in range(1, across):
        for k, plane in halves:
            load_tile(step, k, plane).wait()
            collide_strip(lax.rem(me + step, across) * wt + k, plane, None)
            if step == 1 and (k, plane) == (0, 0):
                enter()

            def begin_outer(mine):
                send(mine, (mine + step) % across, 0, (k, plane)).start()

            on_each(begin_outer)
    send_direct(range(across - 1), (0, 1))
    for k, plane in halves:
        load_tile(across, k, plane).wait()
        collide_strip(me * wt + k, plane, k)
    send_direct((across - 1,), (0, 1))

    lane = lax.broadcasted_iota(jnp.int32, (rows, LANES), 1)
    for step in range(1, across + 1):
        target = lax.rem(me + step, across)
        first = lax.rem((target + 1) * wt, strips)
        last = lax.rem(target * wt + strips - 1, strips)
        own_at = pl.ds(pl.multiple_of(me * rows, ROWS), rows)
        for group in range(groups):
            packed = jnp.zeros((rows, LANES), jnp.float32)
            for place in range(per_group):
                slab = group * per_group + place
                if slab >= slabs + len(PAIRS) * planes:
                    break
                field, plane = slab // planes, slab % planes
                if slab < slabs:
                    edge = jnp.where(lane < LANES // 2, box[field, plane, first], box[field, plane, last])
                    if step == across:
                        sides[field, plane, own_at, :] = edge
                else:
                    right, left = (place_of[slot] for slot in PAIRS[field - Q])
                    tile = target * wt + wt - 1
                    edge = jnp.where(lane < LANES // 2, box[left, plane, tile], box[right, plane, tile])
                    if step == across:
                        seams[field - Q, plane, own_at, :] = edge
                if place == 0:
                    packed = edge
                else:
                    moved = pltpu.roll(edge, 4 * place, 1)
                    packed = jnp.where((lane >= 4 * place - 2) & (lane < 4 * place + 2), moved, packed)
            packs[target, group] = packed
            if step == across:
                edges[group, own_at, :] = packed
        if step == across - 1:
            begin((1,))

            @pl.when(jnp.logical_not(odd))
            def _():
                begin((2, 3, 4))

    send_direct(range(across), (2,))
    ends = ((0, 0), (across - 1, 1))

    lead = 2 if wt > 1 else 3

    @pl.when(odd)
    def _():
        pl.semaphore_wait(go, 1)
        begin((2, 3, 4))

    def lead_sent(mine):
        for target in peers(mine):
            send(mine, target, lead).wait_send()

    @pl.when(jnp.logical_not(odd))
    def _():
        on_each(lead_sent)
        pl.semaphore_signal(go, inc=1, device_id=(me, down), device_id_type=MESH)

    @pl.when(odd)
    def _():
        pl.semaphore_wait(ready, jnp.where(last_row, 1, 2))

    def unpack(packs_of, at, store):
        for slab in range(slabs + len(PAIRS) * planes):
            group, place = slab // per_group, slab % per_group
            packed = packs_of[group, at, :]
            moved = pltpu.roll(packed, LANES - 4 * place, 1) if place else packed
            store(slab // planes, slab % planes, moved)

    def pass_on(mine, source, way):
        if source != mine:
            send(source, mine, 0).wait_recv()
            send(source, mine, 1).wait_recv()

        def start():
            for copy in relay(way):
                copy.start()

        if way:
            pl.when(jnp.logical_not(last_row))(start)
        else:
            start()

    def relays(mine):
        @pl.when(first_row)
        def _():
            pass_on(mine, across - 1, 1)
            pl.semaphore_wait(ready, 1)
            pass_on(mine, 0, 0)

        @pl.when(jnp.logical_not(first_row))
        def _():
            for source, way in sorted(ends, key=lambda end: end[0] != mine):
                pass_on(mine, source, way)

        for source in peers(mine):
            if source not in (0, across - 1):
                send(source, mine, 0).wait_recv()
                send(source, mine, 1).wait_recv()

    on_each(relays)

    def settle(wanted):
        def action(mine):
            for source in peers(mine):
                for n in pieces:
                    if n in wanted:
                        send(source, mine, n).wait_recv()

        on_each(action)

    every = list(range(wt + 1))
    before = [tile for tile in every if tile != wt - 1]

    def advance(load, store, tiles, seam=None):
        for tile in tiles:
            for plane in range(planes):
                is_open = load(0, plane, tile, 0) != 0.0
                fields = [stream(load, (wt + 1, planes), slot, plane, tile, 0.0, seam) for slot in range(Q)]
                result = collide_tile(fields, is_open, None, SOLID)
                for slot in range(Q):
                    store(slot, plane, tile, result[slot])

    def window(source, tiles):
        start = jnp.minimum(rows * source + 1, height - 1 - ROWS)

        def load(slot, plane, tile, dy):
            at = pl.ds(start - dy, ROWS)
            if tile == wt:
                return sides[place_of[slot], plane, at, :]
            return post[place_of[slot], plane, tile, at, :]

        def store(slot, plane, tile, value):
            post2[place_of[slot], plane, tile, pl.ds(ROWS + start, ROWS), :] = value

        def seam(slot, plane, tile, dy):
            if tile != wt - 1:
                return load(slot, plane, tile, dy)
            pair = [slot in both for both in PAIRS].index(True)
            return seams[pair, plane, pl.ds(start - dy, ROWS), :]

        advance(load, store, tiles, seam)

    row = lax.broadcasted_iota(jnp.int32, (ROWS, LANES), 0)
    half = ROWS // 2

    def fill():
        for slot in range(Q):
            for plane in range(planes):
                for tile in range(wt):
                    ring[slot, plane, tile, HALO:half, :] = post[slot, plane, tile, 0:HALO, :]
                    ring[slot, plane, tile, half : half + HALO, :] = post[
                        slot, plane, tile, height - HALO : height, :
                    ]
        for group in range(groups):
            ring_edges[group, HALO:half, :] = edges[group, 0:HALO, :]
            ring_edges[group, half : half + HALO, :] = edges[group, height - HALO : height, :]

    def rim():
        top, low = ROWS - HALO, height + HALO

        def load(slot, plane, tile, dy):
            value = ring[place_of[slot], plane, tile]
            return pltpu.roll(value, dy % ROWS, 0) if dy else value

        def store(slot, plane, tile, value):
            place = place_of[slot]
            pltpu.store(
                post2.at[place, plane, tile, top : top + ROWS, :], value,
                mask=(row >= 1) & (row < 3),
            )
            pltpu.store(
                post2.at[place, plane, tile, low : low + ROWS, :], value,
                mask=(row >= half + 1) & (row < half + 3),
            )

        advance(load, store, every)

    def unpack_from(step, carry):
        at = pl.ds(pl.multiple_of(lax.rem(me + step, across) * rows, ROWS), rows)

        def store(slot, plane, value):
            if slot < Q:
                sides[slot, plane, at, :] = value
            else:
                seams[slot - Q, plane, at, :] = value

        unpack(edges, at, store)
        return carry

    def unpack_ring():
        def store(slot, plane, value):
            if slot < Q:
                ring[slot, plane, wt] = value

        unpack(ring_edges, pl.ds(0, ROWS), store)

    lax.fori_loop(1, across, unpack_from, 0)
    fill()
    def windows(tiles):
        def window_from(step, carry):
            window(lax.rem(me + step, across), tiles)
            return carry

        lax.fori_loop(1, across, window_from, 0)

    settle((2,))
    windows(before)
    settle((3,))
    window(me, every)
    for way in range(2):
        for copy in relay(way):
            copy.wait_recv()
    unpack_ring()
    rim()
    settle((4,))
    windows([wt - 1])

    def sent(mine):
        for target in peers(mine):
            for n in pieces:
                if n == lead:
                    pl.when(odd)(send(mine, target, n).wait_send)
                else:
                    send(mine, target, n).wait_send()

    on_each(sent)
    for copy in relay(0):
        copy.wait_send()

    @pl.when(jnp.logical_not(last_row))
    def _():
        for copy in relay(1):
            copy.wait_send()

    @pl.when(last_strip)
    def _():
        for target in range(across):
            for copy in direct(target):
                copy.wait_send()


def finish(post, out_ref, flow, sems):
    _, planes, height, width = flow.shape
    wt = width // LANES

    def load(slot, plane, tile, dy):
        return post[place_of[slot], plane, tile, at - dy : at - dy + ROWS, :]

    copies = []
    for start in range(0, height, ROWS):
        for plane in range(planes):
            at = ROWS + start
            for tile in range(wt):
                is_open = load(0, plane, tile, 0) != SOLID
                for slot in range(Q):
                    value = stream(load, (wt + 1, planes), slot, plane, tile, SOLID)
                    flow[slot, plane, start : start + ROWS, tile * LANES : (tile + 1) * LANES] = jnp.where(
                        is_open, value, 0.0
                    )
            block = (slice(None), plane, slice(start, start + ROWS))
            copies.append(pltpu.make_async_copy(flow.at[block], out_ref.at[block], sems.at[len(copies)]))
            copies[-1].start()
    for copy in copies:
        copy.wait()


def body(across, along, populations, pore):
    count, planes, rows, columns = populations.shape
    height = across * rows
    width = columns // across
    strips = columns // LANES
    wt = strips // across
    groups = -(-(count + len(PAIRS)) * planes * 4 // LANES)
    tall = height + 2 * ROWS
    post2 = pl.pallas_call(
        functools.partial(kernel, across, along),
        out_shape=pltpu.VMEM((count, planes, wt + 1, tall, LANES), jnp.float32),
        in_specs=[pl.BlockSpec(memory_space=pltpu.HBM)] * 2,
        out_specs=pl.BlockSpec(memory_space=pltpu.VMEM),
        scratch_shapes=[
            pltpu.VMEM((count, planes, strips, rows, LANES), jnp.float32),
            pltpu.VMEM((planes, rows, columns), jnp.int32),
            pltpu.VMEM((count, planes, strips, rows, LANES), jnp.float32),
            pltpu.VMEM((count, planes, wt, height, LANES), jnp.float32),
            pltpu.VMEM((count, planes, height, LANES), jnp.float32),
            pltpu.VMEM((len(PAIRS), planes, height, LANES), jnp.float32),
            pltpu.VMEM((count, planes, wt + 1, ROWS, LANES), jnp.float32),
            pltpu.VMEM((across, groups, rows, LANES), jnp.float32),
            pltpu.VMEM((groups, height, LANES), jnp.float32),
            pltpu.VMEM((groups, ROWS, LANES), jnp.float32),
            pltpu.SemaphoreType.DMA((1 + strips * planes,)),
            pltpu.SemaphoreType.DMA((across, 5)),
            pltpu.SemaphoreType.DMA((across, 5)),
            pltpu.SemaphoreType.DMA((2, 3)),
            pltpu.SemaphoreType.DMA((2, 3)),
            pltpu.SemaphoreType.DMA((across, 3)),
            pltpu.SemaphoreType.REGULAR,
            pltpu.SemaphoreType.REGULAR,
        ],
        compiler_params=pltpu.CompilerParams(
            collective_id=0, has_side_effects=True, vmem_limit_bytes=VMEM_LIMIT
        ),
    )(*(pltpu.with_memory_space_constraint(x, pltpu.HBM) for x in (populations, pore)))
    return pl.pallas_call(
        finish,
        out_shape=jax.ShapeDtypeStruct((count, planes, height, width), jnp.float32),
        in_specs=[pl.BlockSpec(memory_space=pltpu.VMEM)],
        out_specs=pl.BlockSpec(memory_space=pl.ANY),
        scratch_shapes=[
            pltpu.VMEM((count, planes, height, width), jnp.float32),
            pltpu.SemaphoreType.DMA((planes * height // ROWS,)),
        ],
        compiler_params=pltpu.CompilerParams(vmem_limit_bytes=VMEM_LIMIT),
    )(post2)


def solution(mesh):
    return jax.shard_map(
        functools.partial(body, mesh.shape["px"], mesh.shape["py"]),
        mesh=mesh,
        in_specs=(P(None, None, ("py", "px"), None), P(None, ("py", "px"), None)),
        out_specs=P(None, None, "py", "px"),
        check_vma=False,
    )
```

```python
import functools

import jax
import jax.numpy as jnp
from jax import lax
from jax.experimental import pallas as pl
from jax.experimental.pallas import tpu as pltpu
from jax.sharding import PartitionSpec as P

MESH = pl.DeviceIdType.MESH

lattice_velocity = [
    (0, 0, 0),
    (1, 0, 0),
    (-1, 0, 0),
    (0, 1, 0),
    (0, -1, 0),
    (0, 0, 1),
    (0, 0, -1),
    (1, 1, 0),
    (-1, -1, 0),
    (1, -1, 0),
    (-1, 1, 0),
    (1, 0, 1),
    (-1, 0, -1),
    (1, 0, -1),
    (-1, 0, 1),
    (0, 1, 1),
    (0, -1, -1),
    (0, 1, -1),
    (0, -1, 1),
]
lattice_weights = [1.0 / 3.0] + [1.0 / 18.0] * 6 + [1.0 / 36.0] * 12
opposite = [0, 2, 1, 4, 3, 6, 5, 8, 7, 10, 9, 12, 11, 14, 13, 16, 15, 18, 17]
relax_time = 0.8
body_force = 0.005

Q = len(lattice_velocity)
LANES = 128
ROWS = 8
HALO = 2
VMEM_LIMIT = 32 * 1024 * 1024
SOLID = -3.0e38
TINY = 1.0e-30

order = sorted(range(Q), key=lambda slot: lattice_velocity[slot][1])
place_of = [order.index(slot) for slot in range(Q)]
RISE = sum(1 for vector in lattice_velocity if vector[1] < 0)
FALL = Q - sum(1 for vector in lattice_velocity if vector[1] > 0)
PAIRS = [(s, opposite[s]) for s in range(Q) if lattice_velocity[s][0] > 0]


def edge_layout(planes):
    spots, group, at = [], 0, 0
    for field in range(Q + len(PAIRS)):
        dx = lattice_velocity[order[field]][0] if field < Q else 0
        left, right = 1 + (dx > 0), 1 + (dx < 0)
        for _ in range(planes):
            if at + left + right > LANES:
                group, at = group + 1, 0
            spots.append((group, at + left, left, right))
            at += left + right
    return spots, group + 1


def total(values):
    return functools.reduce(lambda x, y: x + y, values)


def collide_tile(fields, is_open, guard, closed):
    keep = 1.0 - 1.0 / relax_time
    gain = 1.0 / relax_time
    density = jnp.where(is_open, total(fields), 1.0)
    inverse = 1.0 / density
    vel = []
    for column in range(3):
        plus = [fields[s] for s in range(Q) if lattice_velocity[s][column] > 0]
        minus = [fields[s] for s in range(Q) if lattice_velocity[s][column] < 0]
        vel.append((total(plus) - total(minus)) * inverse)
    vel[2] = vel[2] + relax_time * body_force
    speed = vel[0] * vel[0] + vel[1] * vel[1] + vel[2] * vel[2]
    base = 1.0 - 1.5 * speed
    result = [None] * Q
    scaled = {w: density * (gain * w) for w in sorted(set(lattice_weights))}

    def close(value):
        return jnp.where(is_open, value + guard if guard else value, closed)

    result[0] = close(keep * fields[0] + scaled[lattice_weights[0]] * base)
    for slot in range(1, Q, 2):
        other = opposite[slot]
        along = None
        for column in range(3):
            sign = lattice_velocity[slot][column]
            if sign == 0:
                continue
            term = vel[column]
            if along is None:
                along = term if sign > 0 else -term
            else:
                along = along + term if sign > 0 else along - term
        weight = scaled[lattice_weights[slot]]
        triple = 3.0 * along
        even = weight * (base + 0.5 * triple * triple)
        odd = weight * triple
        result[slot] = close(keep * fields[slot] + (even + odd))
        result[other] = close(keep * fields[other] + (even - odd))
    return result


def stream(load, sides, slot, plane, tile, closed, seam=None):
    tiles, planes = sides
    dx, dy, dz = lattice_velocity[slot]
    source = (plane - dz) % planes
    value = load(slot, source, tile, dy)
    if dx:
        lane = lax.broadcasted_iota(jnp.int32, value.shape, 1)
        beside = (seam or load)(slot, source, (tile - dx) % tiles, dy)
        value = jnp.where(lane == (LANES - 1 if dx > 0 else 0), beside, value)
        value = pltpu.roll(value, dx % LANES, 1)
    if slot:
        value = jnp.where(value != closed, value, load(opposite[slot], plane, tile, 0))
    return value


def kernel(
    across, along, pop_ref, pore_ref, post2, done,
    raw, voxels, box, post, sides, seams, ring, packs, edges, ring_edges,
    load_sem, n_send, n_recv, h_send, h_recv, w_send, go, ready,
):
    _, planes, strips, rows, _ = box.shape
    wt = strips // across
    height = across * rows
    spots, groups = edge_layout(planes)
    slabs = Q * planes
    me = lax.axis_index("px")
    here = lax.axis_index("py")
    up = lax.rem(here + along - 1, along)
    down = lax.rem(here + 1, along)
    first_row = here == 0
    last_row = here == along - 1
    odd = lax.rem(here, 2) == 1
    last_strip = last_row & (me == across - 1)

    load_pore = pltpu.make_async_copy(pore_ref, voxels, load_sem.at[0])
    load_pore.start()

    own_load = (across - 1) * wt * planes

    def load_tile(step, k, plane):
        tile = lax.rem(me + step, across) * wt + k
        cols = pl.ds(pl.multiple_of(tile * LANES, LANES), LANES)
        return pltpu.make_async_copy(
            pop_ref.at[:, plane, :, cols],
            raw.at[:, plane, tile],
            load_sem.at[1 + (((step - 1) * wt + k) * planes + plane if step < across else own_load)],
        )

    halves = [(k, plane) for k in range(wt) for plane in range(planes)]
    for step in range(1, across + 1):
        for k, plane in halves:
            load_tile(step, k, plane).start()

    barrier = pltpu.get_barrier_semaphore()

    def greet(x, y):
        pl.semaphore_signal(barrier, inc=1, device_id=(x, y), device_id_type=MESH)

    def answer(y):
        pl.semaphore_signal(ready, inc=1, device_id=(me, y), device_id_type=MESH)

    for step in range(1, across):
        greet(lax.rem(me + step, across), here)

    @pl.when(odd)
    def _():
        greet(me, up)

        @pl.when(jnp.logical_not(last_row))
        def _():
            greet(me, down)

    @pl.when(first_row)
    def _():
        greet(me, along - 1)

        @pl.when(me != across - 1)
        def _():
            greet(across - 1, along - 1)

    def enter():
        greeted = jnp.where(odd, 0, 2) - jnp.where(first_row, 1, 0)
        greeted = greeted + jnp.where(last_row, jnp.where(me == across - 1, across, 1), 0)
        pl.semaphore_wait(barrier, across - 1 + greeted)

        @pl.when(jnp.logical_not(odd))
        def _():
            answer(down)

            @pl.when(here != 0)
            def _():
                answer(up)

        @pl.when(last_row)
        def _():
            answer(0)

    load_pore.wait()

    def collide_strip(tile, plane, own):
        cols = pl.ds(pl.multiple_of(tile * LANES, LANES), LANES)
        fields = [raw[slot, plane, tile] for slot in range(Q)]
        is_open = voxels[plane, :, cols] > 0
        result = collide_tile(fields, is_open, TINY, 0.0)
        for slot in range(Q):
            box[place_of[slot], plane, tile] = result[slot]
            if own is not None:
                at = pl.ds(pl.multiple_of(me * rows, ROWS), rows)
                post[place_of[slot], plane, own, at, :] = result[slot]

    def outer(source):
        return (rows - HALO, rows) if source == across - 1 else (0, HALO)

    def inner(source):
        return (0, HALO) if source == across - 1 else (rows - HALO, rows)

    def rest(source):
        return (0, rows - HALO) if source == across - 1 else (HALO, rows)

    def middle(source):
        return (HALO, rows - HALO)

    def send(source, target, n, part=None):
        if part:
            k, plane = part
            low, high = outer(source)
            return pltpu.make_async_remote_copy(
                src_ref=box.at[:, plane, target * wt + k, low:high, :],
                dst_ref=post.at[:, plane, k, source * rows + low : source * rows + high, :],
                send_sem=n_send.at[(target - source) % across - 1, min(n, 3)],
                recv_sem=n_recv.at[(target - source) % across - 1, n],
                device_id=(target, here),
                device_id_type=MESH,
            )
        if n == 1:
            src, dst = packs.at[target], edges.at[:, source * rows : (source + 1) * rows, :]
        else:
            low, high = (outer, None, rest, inner, middle)[n](source)
            first, last = ((0, wt), None, (0, wt - 1), (wt - 1, wt), (wt - 1, wt))[n]
            src = box.at[:, :, target * wt + first : target * wt + last, low:high, :]
            start = source * rows
            dst = post.at[:, :, first:last, start + low : start + high, :]
        return pltpu.make_async_remote_copy(
            src_ref=src,
            dst_ref=dst,
            send_sem=n_send.at[(target - source) % across - 1, min(n, 3)],
            recv_sem=n_recv.at[(target - source) % across - 1, n],
            device_id=(target, here),
            device_id_type=MESH,
        )

    pieces = [0, 1, 2, 3, 4] if wt > 1 else [0, 1, 3, 4]

    def relay(way):
        if way == 0:
            near, beyond, part, to = 0, 1, (0, RISE), up
            near_to, beyond_to, low, low_to = ROWS - 2, ROWS - 1, 0, ROWS - HALO
        else:
            near, beyond, part, to = height - 1, height - 2, (FALL, Q), down
            near_to, beyond_to, low, low_to = 1, 0, height - HALO, 0
        some = slice(*part)
        refs = [
            (post.at[:, :, :, near : near + 1, :],
             ring.at[:, :, 0:wt, near_to : near_to + 1, :]),
            (post.at[some, :, :, beyond : beyond + 1, :],
             ring.at[some, :, 0:wt, beyond_to : beyond_to + 1, :]),
            (edges.at[:, low : low + HALO, :], ring_edges.at[:, low_to : low_to + HALO, :]),
        ]
        return [
            pltpu.make_async_remote_copy(
                src_ref=src,
                dst_ref=dst,
                send_sem=h_send.at[way, n // 2],
                recv_sem=h_recv.at[way, n // 2],
                device_id=(me, to),
                device_id_type=MESH,
            )
            for n, (src, dst) in enumerate(refs)
        ]

    def peers(mine):
        return [(mine + step) % across for step in range(1, across)]

    def on_each(action):
        for mine in range(across):
            pl.when(me == mine)(functools.partial(action, mine))

    def begin(wanted):
        def action(mine):
            for n in pieces:
                if n in wanted:
                    for target in peers(mine):
                        send(mine, target, n).start()

        on_each(action)

    def direct(target, which=range(3)):
        cols = slice(target * wt, (target + 1) * wt)
        refs = [
            (box.at[:, :, cols, rows - 1 : rows, :], ring.at[:, :, 0:wt, 1:2, :]),
            (box.at[FALL:Q, :, cols, rows - HALO : rows - 1, :], ring.at[FALL:Q, :, 0:wt, 0:1, :]),
            (packs.at[target, :, rows - HALO : rows, :], ring_edges.at[:, 0:HALO, :]),
        ]
        return [
            pltpu.make_async_remote_copy(
                src_ref=src,
                dst_ref=dst,
                send_sem=w_send.at[n // 2],
                recv_sem=h_recv.at[1, n // 2],
                device_id=(target, 0),
                device_id_type=MESH,
            )
            for n, (src, dst) in enumerate(refs)
            if n in which
        ]

    def send_direct(targets, which):
        @pl.when(last_strip)
        def _():
            for target in targets:
                for copy in direct(target, which):
                    copy.start()


    for step in range(1, across):
        for k, plane in halves:
            load_tile(step, k, plane).wait()
            collide_strip(lax.rem(me + step, across) * wt + k, plane, None)
            if step == 1 and (k, plane) == (0, 0):
                enter()

            def begin_outer(mine):
                send(mine, (mine + step) % across, 0, (k, plane)).start()

            on_each(begin_outer)
    send_direct(range(across - 1), (0, 1))
    own = raw.at[:, :, pl.ds(me * wt, wt)]
    pltpu.make_async_copy(own, own, load_sem.at[1 + own_load]).wait()
    for k, plane in halves:
        collide_strip(me * wt + k, plane, k)
    send_direct((across - 1,), (0, 1))

    lane = lax.broadcasted_iota(jnp.int32, (rows, LANES), 1)
    for step in range(1, across + 1):
        target = lax.rem(me + step, across)
        first = lax.rem((target + 1) * wt, strips)
        last = lax.rem(target * wt + strips - 1, strips)
        own_at = pl.ds(pl.multiple_of(me * rows, ROWS), rows)
        packed = [None] * groups
        for slab, (group, at, left_of, right_of) in enumerate(spots):
            field, plane = slab // planes, slab % planes
            if slab < slabs:
                edge = jnp.where(lane < LANES // 2, box[field, plane, first], box[field, plane, last])
                if step == across:
                    sides[field, plane, own_at, :] = edge
            else:
                right, left = (place_of[slot] for slot in PAIRS[field - Q])
                tile = target * wt + wt - 1
                edge = jnp.where(lane < LANES // 2, box[left, plane, tile], box[right, plane, tile])
                if step == across:
                    seams[field - Q, plane, own_at, :] = edge
            moved = pltpu.roll(edge, at, 1)
            if packed[group] is not None:
                moved = jnp.where((lane >= at - left_of) & (lane < at + right_of), moved, packed[group])
            packed[group] = moved
        for group in range(groups):
            packs[target, group] = packed[group]
            if step == across:
                edges[group, own_at, :] = packed[group]
        if step == across - 1:
            begin((1,))

            @pl.when(jnp.logical_not(odd))
            def _():
                begin((2, 3, 4))

    send_direct(range(across), (2,))
    ends = ((0, 0), (across - 1, 1))

    def both(sem, tiles):
        rows_of = box.at[0 : (Q + RISE) // 2, :, 0:tiles, 0:2, :]
        pltpu.make_async_copy(rows_of, rows_of, sem).wait()

    def some_edges(sem, refs):
        pltpu.make_async_copy(refs, refs, sem).wait()

    lead = 2 if wt > 1 else 0

    @pl.when(odd)
    def _():
        pl.semaphore_wait(go, 1)
        begin((2, 3, 4))

    def lead_sent(mine):
        for target in peers(mine):
            send(mine, target, lead).wait_send()

    @pl.when(jnp.logical_not(odd))
    def _():
        on_each(lead_sent)
        pl.semaphore_signal(go, inc=1, device_id=(me, down), device_id_type=MESH)

    @pl.when(odd)
    def _():
        pl.semaphore_wait(ready, jnp.where(last_row, 1, 2))

    def unpack(packs_of, at, store):
        for slab, (group, lane_at, _, _) in enumerate(spots):
            moved = pltpu.roll(packs_of[group, at, :], LANES - lane_at, 1)
            store(slab // planes, slab % planes, moved)

    def pass_on(mine, source, way):
        if source != mine:
            send(source, mine, 0).wait_recv()
            send(source, mine, 1).wait_recv()

        def start():
            for copy in relay(way):
                copy.start()

        if way:
            pl.when(jnp.logical_not(last_row))(start)
        else:
            start()

    def relays(mine):
        @pl.when(first_row)
        def _():
            pass_on(mine, across - 1, 1)
            pl.semaphore_wait(ready, 1)
            pass_on(mine, 0, 0)

        @pl.when(jnp.logical_not(first_row))
        def _():
            for source, way in sorted(ends, key=lambda end: end[0] != mine):
                pass_on(mine, source, way)

        for source in peers(mine):
            if source not in (0, across - 1):
                send(source, mine, 0).wait_recv()
                send(source, mine, 1).wait_recv()

    on_each(relays)

    def settle(wanted):
        def action(mine):
            for source in peers(mine):
                for n in pieces:
                    if n in wanted:
                        send(source, mine, n).wait_recv()

        on_each(action)

    every = list(range(wt + 1))
    before = [tile for tile in every if tile != wt - 1]

    def advance(load, store, tiles, seam=None):
        for tile in tiles:
            for plane in range(planes):
                is_open = load(0, plane, tile, 0) != 0.0
                fields = [stream(load, (wt + 1, planes), slot, plane, tile, 0.0, seam) for slot in range(Q)]
                result = collide_tile(fields, is_open, None, SOLID)
                for slot in range(Q):
                    store(slot, plane, tile, result[slot])

    def window(source, tiles):
        start = jnp.minimum(rows * source + 1, height - 1 - ROWS)

        def load(slot, plane, tile, dy):
            at = pl.ds(start - dy, ROWS)
            if tile == wt:
                return sides[place_of[slot], plane, at, :]
            return post[place_of[slot], plane, tile, at, :]

        def store(slot, plane, tile, value):
            post2[place_of[slot], plane, tile, pl.ds(ROWS + start, ROWS), :] = value

        def seam(slot, plane, tile, dy):
            if tile != wt - 1:
                return load(slot, plane, tile, dy)
            pair = [slot in both for both in PAIRS].index(True)
            return seams[pair, plane, pl.ds(start - dy, ROWS), :]

        advance(load, store, tiles, seam)

    row = lax.broadcasted_iota(jnp.int32, (ROWS, LANES), 0)
    half = ROWS // 2

    def fill():
        for slot in range(Q):
            for plane in range(planes):
                for tile in range(wt):
                    ring[slot, plane, tile, HALO:half, :] = post[slot, plane, tile, 0:HALO, :]
                    ring[slot, plane, tile, half : half + HALO, :] = post[
                        slot, plane, tile, height - HALO : height, :
                    ]
        for group in range(groups):
            ring_edges[group, HALO:half, :] = edges[group, 0:HALO, :]
            ring_edges[group, half : half + HALO, :] = edges[group, height - HALO : height, :]

    def rim():
        top, low = ROWS - HALO, height + HALO

        def load(slot, plane, tile, dy):
            value = ring[place_of[slot], plane, tile]
            return pltpu.roll(value, dy % ROWS, 0) if dy else value

        def store(slot, plane, tile, value):
            place = place_of[slot]
            pltpu.store(
                post2.at[place, plane, tile, top : top + ROWS, :], value,
                mask=(row >= 1) & (row < 3),
            )
            pltpu.store(
                post2.at[place, plane, tile, low : low + ROWS, :], value,
                mask=(row >= half + 1) & (row < half + 3),
            )

        advance(load, store, every)

    def unpack_from(step, carry):
        at = pl.ds(pl.multiple_of(lax.rem(me + step, across) * rows, ROWS), rows)

        def store(slot, plane, value):
            if slot < Q:
                sides[slot, plane, at, :] = value
            else:
                seams[slot - Q, plane, at, :] = value

        unpack(edges, at, store)
        return carry

    def unpack_ring():
        def store(slot, plane, value):
            if slot < Q:
                ring[slot, plane, wt] = value

        unpack(ring_edges, pl.ds(0, ROWS), store)

    lax.fori_loop(1, across, unpack_from, 0)
    fill()
    def windows(tiles):
        def window_from(step, carry):
            window(lax.rem(me + step, across), tiles)
            return carry

        lax.fori_loop(1, across, window_from, 0)

    settle((2,))
    windows(before)
    settle((3,))
    window(me, every)
    for way in range(2):
        both(h_recv.at[way, 0], wt)
        some_edges(h_recv.at[way, 1], ring_edges.at[:, 0:HALO, :])
    unpack_ring()
    rim()

    def own_flow():
        for plane in range(planes):
            for tile in range(wt):
                def store(slot, value):
                    done[slot, plane, :, tile * LANES : (tile + 1) * LANES] = value

                flow_tile(post2, pl.multiple_of(me * rows, ROWS), plane, tile, wt + 1, store)

    if across == 2:
        own_flow()
    settle((4,))
    windows([wt - 1])
    if across != 2:
        own_flow()

    def sent(mine):
        for target in peers(mine):
            for n in (0, 1, 2):
                if n not in pieces:
                    continue
                if n == lead:
                    pl.when(odd)(send(mine, target, n).wait_send)
                else:
                    send(mine, target, n).wait_send()
            low, high = rest(mine)
            last_tile = box.at[:, :, wt - 1 : wt, low:high, :]
            pltpu.make_async_copy(last_tile, last_tile, n_send.at[(target - mine) % across - 1, 3]).wait()

    on_each(sent)
    both(h_send.at[0, 0], wt)
    some_edges(h_send.at[0, 1], ring_edges.at[:, 0:HALO, :])

    @pl.when(jnp.logical_not(last_row))
    def _():
        both(h_send.at[1, 0], wt)
        some_edges(h_send.at[1, 1], ring_edges.at[:, 0:HALO, :])

    @pl.when(last_strip)
    def _():
        both(w_send.at[0], strips)
        some_edges(w_send.at[1], packs.at[:, :, 0:HALO, :])


def flow_tile(post, start, plane, tile, tiles, store):
    planes = post.shape[1]

    def load(slot, plane, tile, dy):
        return post[place_of[slot], plane, tile, pl.ds(ROWS + start - dy, ROWS), :]

    is_open = load(0, plane, tile, 0) != SOLID
    for slot in range(Q):
        value = stream(load, (tiles, planes), slot, plane, tile, SOLID)
        store(slot, jnp.where(is_open, value, 0.0))


def finish(across, post, done, out_ref, flow, sems):
    _, planes, rows, width = done.shape
    wt = width // LANES
    me = lax.axis_index("px")

    def own_copy():
        at = pl.ds(pl.multiple_of(me * rows, ROWS), rows)
        return pltpu.make_async_copy(done, out_ref.at[:, :, at, :], sems.at[0])

    def copy_of(step, plane):
        at = pl.ds(pl.multiple_of(lax.rem(me + step, across) * rows, ROWS), rows)
        return pltpu.make_async_copy(
            flow.at[step - 1, :, plane], out_ref.at[:, plane, at, :], sems.at[1 + (step - 1) * planes + plane]
        )

    own_copy().start()

    def write(step, carry):
        for plane in range(planes):
            for tile in range(wt):
                def store(slot, value):
                    flow[step - 1, slot, plane, :, tile * LANES : (tile + 1) * LANES] = value

                start = pl.multiple_of(lax.rem(me + step, across) * rows, ROWS)
                flow_tile(post, start, plane, tile, wt + 1, store)
            copy_of(step, plane).start()
        return carry

    lax.fori_loop(1, across, write, 0)
    own_copy().wait()

    def written(step, carry):
        for plane in range(planes):
            copy_of(step, plane).wait()
        return carry

    lax.fori_loop(1, across, written, 0)


def body(across, along, populations, pore):
    count, planes, rows, columns = populations.shape
    height = across * rows
    width = columns // across
    strips = columns // LANES
    wt = strips // across
    groups = edge_layout(planes)[1]
    tall = height + 2 * ROWS
    post2, done = pl.pallas_call(
        functools.partial(kernel, across, along),
        out_shape=(
            pltpu.VMEM((count, planes, wt + 1, tall, LANES), jnp.float32),
            pltpu.VMEM((count, planes, rows, width), jnp.float32),
        ),
        in_specs=[pl.BlockSpec(memory_space=pltpu.HBM)] * 2,
        out_specs=[pl.BlockSpec(memory_space=pltpu.VMEM)] * 2,
        scratch_shapes=[
            pltpu.VMEM((count, planes, strips, rows, LANES), jnp.float32),
            pltpu.VMEM((planes, rows, columns), jnp.int32),
            pltpu.VMEM((count, planes, strips, rows, LANES), jnp.float32),
            pltpu.VMEM((count, planes, wt, height, LANES), jnp.float32),
            pltpu.VMEM((count, planes, height, LANES), jnp.float32),
            pltpu.VMEM((len(PAIRS), planes, height, LANES), jnp.float32),
            pltpu.VMEM((count, planes, wt + 1, ROWS, LANES), jnp.float32),
            pltpu.VMEM((across, groups, rows, LANES), jnp.float32),
            pltpu.VMEM((groups, height, LANES), jnp.float32),
            pltpu.VMEM((groups, ROWS, LANES), jnp.float32),
            pltpu.SemaphoreType.DMA((2 + (across - 1) * wt * planes,)),
            pltpu.SemaphoreType.DMA((across - 1, 4)),
            pltpu.SemaphoreType.DMA((across - 1, 5)),
            pltpu.SemaphoreType.DMA((2, 2)),
            pltpu.SemaphoreType.DMA((2, 2)),
            pltpu.SemaphoreType.DMA((2,)),
            pltpu.SemaphoreType.REGULAR,
            pltpu.SemaphoreType.REGULAR,
        ],
        compiler_params=pltpu.CompilerParams(
            collective_id=0, has_side_effects=True, vmem_limit_bytes=VMEM_LIMIT
        ),
    )(*(pltpu.with_memory_space_constraint(x, pltpu.HBM) for x in (populations, pore)))
    return pl.pallas_call(
        functools.partial(finish, across),
        out_shape=jax.ShapeDtypeStruct((count, planes, height, width), jnp.float32),
        in_specs=[pl.BlockSpec(memory_space=pltpu.VMEM)] * 2,
        out_specs=pl.BlockSpec(memory_space=pl.ANY),
        scratch_shapes=[
            pltpu.VMEM((across - 1, count, planes, rows, width), jnp.float32),
            pltpu.SemaphoreType.DMA((1 + (across - 1) * planes,)),
        ],
        compiler_params=pltpu.CompilerParams(vmem_limit_bytes=VMEM_LIMIT),
    )(post2, done)


def solution(mesh):
    return jax.shard_map(
        functools.partial(body, mesh.shape["px"], mesh.shape["py"]),
        mesh=mesh,
        in_specs=(P(None, None, ("py", "px"), None), P(None, ("py", "px"), None)),
        out_specs=P(None, None, "py", "px"),
        check_vma=False,
    )
```

```python
import functools

import jax
import jax.numpy as jnp
from jax import lax
from jax.experimental import pallas as pl
from jax.experimental.pallas import tpu as pltpu
from jax.sharding import PartitionSpec as P

MESH = pl.DeviceIdType.MESH

lattice_velocity = [
    (0, 0, 0),
    (1, 0, 0),
    (-1, 0, 0),
    (0, 1, 0),
    (0, -1, 0),
    (0, 0, 1),
    (0, 0, -1),
    (1, 1, 0),
    (-1, -1, 0),
    (1, -1, 0),
    (-1, 1, 0),
    (1, 0, 1),
    (-1, 0, -1),
    (1, 0, -1),
    (-1, 0, 1),
    (0, 1, 1),
    (0, -1, -1),
    (0, 1, -1),
    (0, -1, 1),
]
lattice_weights = [1.0 / 3.0] + [1.0 / 18.0] * 6 + [1.0 / 36.0] * 12
opposite = [0, 2, 1, 4, 3, 6, 5, 8, 7, 10, 9, 12, 11, 14, 13, 16, 15, 18, 17]
relax_time = 0.8
body_force = 0.005

Q = len(lattice_velocity)
LANES = 128
ROWS = 8
HALO = 2
VMEM_LIMIT = 32 * 1024 * 1024
SOLID = -3.0e38
TINY = 1.0e-30

order = sorted(range(Q), key=lambda slot: lattice_velocity[slot][1])
place_of = [order.index(slot) for slot in range(Q)]
RISE = sum(1 for vector in lattice_velocity if vector[1] < 0)
FALL = Q - sum(1 for vector in lattice_velocity if vector[1] > 0)
PAIRS = [(s, opposite[s]) for s in range(Q) if lattice_velocity[s][0] > 0]


def edge_layout(planes):
    spots, group, at = [], 0, 0
    for field in range(Q + len(PAIRS)):
        dx = lattice_velocity[order[field]][0] if field < Q else 0
        left, right = 1 + (dx > 0), 1 + (dx < 0)
        for _ in range(planes):
            if at + left + right > LANES:
                group, at = group + 1, 0
            spots.append((group, at + left, left, right))
            at += left + right
    return spots, group + 1


def total(values):
    while len(values) > 1:
        pairs = [x + y for x, y in zip(values[::2], values[1::2])]
        values = pairs + values[2 * len(pairs) :]
    return values[0]


def collide_tile(fields, is_open, guard, closed):
    keep = 1.0 - 1.0 / relax_time
    gain = 1.0 / relax_time
    density = jnp.where(is_open, total(fields), 1.0)
    inverse = 1.0 / density
    vel = []
    for column in range(3):
        plus = [fields[s] for s in range(Q) if lattice_velocity[s][column] > 0]
        minus = [fields[s] for s in range(Q) if lattice_velocity[s][column] < 0]
        vel.append((total(plus) - total(minus)) * inverse)
    vel[2] = vel[2] + relax_time * body_force
    speed = vel[0] * vel[0] + vel[1] * vel[1] + vel[2] * vel[2]
    base = 1.0 - 1.5 * speed
    result = [None] * Q
    scaled = {w: density * (gain * w) for w in sorted(set(lattice_weights))}

    def close(value):
        return jnp.where(is_open, value + guard if guard else value, closed)

    result[0] = close(keep * fields[0] + scaled[lattice_weights[0]] * base)
    for slot in range(1, Q, 2):
        other = opposite[slot]
        along = None
        for column in range(3):
            sign = lattice_velocity[slot][column]
            if sign == 0:
                continue
            term = vel[column]
            if along is None:
                along = term if sign > 0 else -term
            else:
                along = along + term if sign > 0 else along - term
        weight = scaled[lattice_weights[slot]]
        triple = 3.0 * along
        even = weight * (base + 0.5 * triple * triple)
        odd = weight * triple
        result[slot] = close(keep * fields[slot] + (even + odd))
        result[other] = close(keep * fields[other] + (even - odd))
    return result


def stream(load, sides, slot, plane, tile, closed, seam=None):
    tiles, planes = sides
    dx, dy, dz = lattice_velocity[slot]
    source = (plane - dz) % planes
    value = load(slot, source, tile, dy)
    if dx:
        lane = lax.broadcasted_iota(jnp.int32, value.shape, 1)
        beside = (seam or load)(slot, source, (tile - dx) % tiles, dy)
        value = jnp.where(lane == (LANES - 1 if dx > 0 else 0), beside, value)
        value = pltpu.roll(value, dx % LANES, 1)
    if slot:
        value = jnp.where(value != closed, value, load(opposite[slot], plane, tile, 0))
    return value


def kernel(
    across, along, pop_ref, pore_ref, post2, done,
    raw, voxels, box, post, sides, seams, ring, packs, edges, ring_edges, via,
    load_sem, n_send, n_recv, h_send, h_recv, w_send, via_sem, go, ready, path,
):
    _, planes, strips, rows, _ = box.shape
    wt = strips // across
    height = across * rows
    spots, groups = edge_layout(planes)
    slabs = Q * planes
    me = lax.axis_index("px")
    here = lax.axis_index("py")
    up = lax.rem(here + along - 1, along)
    down = lax.rem(here + 1, along)
    first_row = here == 0
    last_row = here == along - 1
    odd = lax.rem(here, 2) == 1
    last_strip = last_row & (me == across - 1)
    quarter = along // 4
    short = odd & (here < quarter)
    goes_by = odd & (here >= quarter) & (here < 2 * quarter) & (me == 0)

    load_pore = pltpu.make_async_copy(pore_ref, voxels, load_sem.at[0])
    load_pore.start()

    own_load = (across - 1) * wt * planes

    def load_tile(step, k, plane):
        tile = lax.rem(me + step, across) * wt + k
        cols = pl.ds(pl.multiple_of(tile * LANES, LANES), LANES)
        return pltpu.make_async_copy(
            pop_ref.at[:, plane, :, cols],
            raw.at[:, plane, tile],
            load_sem.at[1 + (((step - 1) * wt + k) * planes + plane if step < across else own_load)],
        )

    halves = [(k, plane) for k in range(wt) for plane in range(planes)]
    for step in range(1, across + 1):
        for k, plane in halves:
            load_tile(step, k, plane).start()

    barrier = pltpu.get_barrier_semaphore()

    def greet(x, y):
        pl.semaphore_signal(barrier, inc=1, device_id=(x, y), device_id_type=MESH)

    def answer(y):
        pl.semaphore_signal(ready, inc=1, device_id=(me, y), device_id_type=MESH)

    for step in range(1, across):
        greet(lax.rem(me + step, across), here)

    @pl.when(odd)
    def _():
        greet(me, up)

        @pl.when(jnp.logical_not(last_row))
        def _():
            greet(me, down)

    @pl.when(short & (me == 0))
    def _():
        greet(0, here + quarter)

    @pl.when(first_row)
    def _():
        greet(me, along - 1)

        @pl.when(me != across - 1)
        def _():
            greet(across - 1, along - 1)

    def enter():
        greeted = jnp.where(odd, 0, 2) - jnp.where(first_row, 1, 0)
        greeted = greeted + jnp.where(last_row, jnp.where(me == across - 1, across, 1), 0)
        greeted = greeted + jnp.where(goes_by, 1, 0)
        pl.semaphore_wait(barrier, across - 1 + greeted)

        @pl.when(goes_by)
        def _():
            pl.semaphore_signal(path, inc=1, device_id=(0, here - quarter), device_id_type=MESH)

        @pl.when(jnp.logical_not(odd))
        def _():
            answer(down)

            @pl.when(here != 0)
            def _():
                answer(up)

        @pl.when(last_row)
        def _():
            answer(0)

    load_pore.wait()

    def collide_strip(tile, plane, own):
        cols = pl.ds(pl.multiple_of(tile * LANES, LANES), LANES)
        fields = [raw[slot, plane, tile] for slot in range(Q)]
        is_open = voxels[plane, :, cols] > 0
        result = collide_tile(fields, is_open, TINY, 0.0)
        for slot in range(Q):
            box[place_of[slot], plane, tile] = result[slot]
            if own is not None:
                at = pl.ds(pl.multiple_of(me * rows, ROWS), rows)
                post[place_of[slot], plane, own, at, :] = result[slot]

    def outer(source):
        return (rows - HALO, rows) if source == across - 1 else (0, HALO)

    def inner(source):
        return (0, HALO) if source == across - 1 else (rows - HALO, rows)

    def rest(source):
        return (0, rows - HALO) if source == across - 1 else (HALO, rows)

    def middle(source):
        return (HALO, rows - HALO)

    def send(source, target, n, part=None):
        if part:
            k, plane = part
            low, high = outer(source)
            return pltpu.make_async_remote_copy(
                src_ref=box.at[:, plane, target * wt + k, low:high, :],
                dst_ref=post.at[:, plane, k, source * rows + low : source * rows + high, :],
                send_sem=n_send.at[(target - source) % across - 1, min(n, 3)],
                recv_sem=n_recv.at[(target - source) % across - 1, n],
                device_id=(target, here),
                device_id_type=MESH,
            )
        if n == 1:
            src, dst = packs.at[target], edges.at[:, source * rows : (source + 1) * rows, :]
        else:
            low, high = (outer, None, rest, inner, middle)[n](source)
            first, last = ((0, wt), None, (0, wt - 1), (wt - 1, wt), (wt - 1, wt))[n]
            src = box.at[:, :, target * wt + first : target * wt + last, low:high, :]
            start = source * rows
            dst = post.at[:, :, first:last, start + low : start + high, :]
        return pltpu.make_async_remote_copy(
            src_ref=src,
            dst_ref=dst,
            send_sem=n_send.at[(target - source) % across - 1, min(n, 3)],
            recv_sem=n_recv.at[(target - source) % across - 1, n],
            device_id=(target, here),
            device_id_type=MESH,
        )

    pieces = [0, 1, 2, 3, 4] if wt > 1 else [0, 1, 3, 4]

    def relay(way):
        if way == 0:
            near, beyond, part, to = 0, 1, (0, RISE), up
            near_to, beyond_to, low, low_to = ROWS - 2, ROWS - 1, 0, ROWS - HALO
        else:
            near, beyond, part, to = height - 1, height - 2, (FALL, Q), down
            near_to, beyond_to, low, low_to = 1, 0, height - HALO, 0
        some = slice(*part)
        refs = [
            (post.at[:, :, :, near : near + 1, :],
             ring.at[:, :, 0:wt, near_to : near_to + 1, :]),
            (post.at[some, :, :, beyond : beyond + 1, :],
             ring.at[some, :, 0:wt, beyond_to : beyond_to + 1, :]),
            (edges.at[:, low : low + HALO, :], ring_edges.at[:, low_to : low_to + HALO, :]),
        ]
        return [
            pltpu.make_async_remote_copy(
                src_ref=src,
                dst_ref=dst,
                send_sem=h_send.at[way, n // 2],
                recv_sem=h_recv.at[way, n // 2],
                device_id=(me, to),
                device_id_type=MESH,
            )
            for n, (src, dst) in enumerate(refs)
        ]

    def peers(mine):
        return [(mine + step) % across for step in range(1, across)]

    def on_each(action):
        for mine in range(across):
            pl.when(me == mine)(functools.partial(action, mine))

    def begin(wanted):
        def action(mine):
            for n in pieces:
                if n in wanted:
                    for target in peers(mine):
                        send(mine, target, n).start()

        on_each(action)

    def direct(target, which=range(3)):
        cols = slice(target * wt, (target + 1) * wt)
        refs = [
            (box.at[:, :, cols, rows - 1 : rows, :], ring.at[:, :, 0:wt, 1:2, :]),
            (box.at[FALL:Q, :, cols, rows - HALO : rows - 1, :], ring.at[FALL:Q, :, 0:wt, 0:1, :]),
            (packs.at[target, :, rows - HALO : rows, :], ring_edges.at[:, 0:HALO, :]),
        ]
        return [
            pltpu.make_async_remote_copy(
                src_ref=src,
                dst_ref=dst,
                send_sem=w_send.at[n // 2],
                recv_sem=h_recv.at[1, n // 2],
                device_id=(target, 0),
                device_id_type=MESH,
            )
            for n, (src, dst) in enumerate(refs)
            if n in which
        ]

    def send_direct(targets, which):
        @pl.when(last_strip)
        def _():
            for target in targets:
                for copy in direct(target, which):
                    copy.start()


    for step in range(1, across):
        for k, plane in halves:
            load_tile(step, k, plane).wait()
            collide_strip(lax.rem(me + step, across) * wt + k, plane, None)
            if step == 1 and (k, plane) == (0, 0):
                enter()

            def begin_outer(mine):
                send(mine, (mine + step) % across, 0, (k, plane)).start()

            on_each(begin_outer)
    send_direct(range(across - 1), (0, 1))
    own = raw.at[:, :, pl.ds(me * wt, wt)]
    pltpu.make_async_copy(own, own, load_sem.at[1 + own_load]).wait()
    for k, plane in halves:
        collide_strip(me * wt + k, plane, k)
    send_direct((across - 1,), (0, 1))

    lane = lax.broadcasted_iota(jnp.int32, (rows, LANES), 1)
    for step in range(1, across + 1):
        target = lax.rem(me + step, across)
        first = lax.rem((target + 1) * wt, strips)
        last = lax.rem(target * wt + strips - 1, strips)
        own_at = pl.ds(pl.multiple_of(me * rows, ROWS), rows)
        packed = [None] * groups
        for slab, (group, at, left_of, right_of) in enumerate(spots):
            field, plane = slab // planes, slab % planes
            if slab < slabs:
                edge = jnp.where(lane < LANES // 2, box[field, plane, first], box[field, plane, last])
                if step == across:
                    sides[field, plane, own_at, :] = edge
            else:
                right, left = (place_of[slot] for slot in PAIRS[field - Q])
                tile = target * wt + wt - 1
                edge = jnp.where(lane < LANES // 2, box[left, plane, tile], box[right, plane, tile])
                if step == across:
                    seams[field - Q, plane, own_at, :] = edge
            moved = pltpu.roll(edge, at, 1)
            if packed[group] is not None:
                moved = jnp.where((lane >= at - left_of) & (lane < at + right_of), moved, packed[group])
            packed[group] = moved
        for group in range(groups):
            packs[target, group] = packed[group]
            if step == across:
                edges[group, own_at, :] = packed[group]
        if step == across - 1:
            begin((1,))

            @pl.when(jnp.logical_not(odd))
            def _():
                begin((2, 3, 4))

    send_direct(range(across), (2,))
    ends = ((0, 0), (across - 1, 1))

    def both(sem, tiles):
        rows_of = box.at[0 : (Q + RISE) // 2, :, 0:tiles, 0:2, :]
        pltpu.make_async_copy(rows_of, rows_of, sem).wait()

    def some_edges(sem, refs):
        pltpu.make_async_copy(refs, refs, sem).wait()

    lead = 2 if wt > 1 else 0

    end = across - 1
    low, high = inner(end)
    around = pltpu.make_async_remote_copy(
        src_ref=box.at[:, :, wt - 1 : wt, low:high, :],
        dst_ref=via,
        send_sem=n_send.at[(0 - end) % across - 1, 3],
        recv_sem=via_sem.at[0],
        device_id=(0, here + quarter),
        device_id_type=MESH,
    )
    onward = pltpu.make_async_remote_copy(
        src_ref=via,
        dst_ref=post.at[:, :, wt - 1 : wt, end * rows + low : end * rows + high, :],
        send_sem=via_sem.at[1],
        recv_sem=n_recv.at[(0 - end) % across - 1, 3],
        device_id=(0, here - quarter),
        device_id_type=MESH,
    )

    @pl.when(short & (me == 0))
    def _():
        pl.semaphore_wait(path, 1)
        pl.semaphore_signal(path, inc=1, device_id=(end, here), device_id_type=MESH)

    @pl.when(short & (me == end))
    def _():
        pl.semaphore_wait(path, 1)
        around.start()

    def begin_late(mine):
        for n in pieces:
            for target in peers(mine):
                if n == 3 and (mine, target) == (end, 0):
                    pl.when(jnp.logical_not(short))(send(mine, target, n).start)
                elif n >= 2:
                    send(mine, target, n).start()

    @pl.when(odd)
    def _():
        pl.semaphore_wait(go, 1)
        on_each(begin_late)

    def lead_sent(mine):
        for target in peers(mine):
            send(mine, target, lead).wait_send()

    @pl.when(jnp.logical_not(odd))
    def _():
        on_each(lead_sent)
        pl.semaphore_signal(go, inc=1, device_id=(me, down), device_id_type=MESH)

    @pl.when(odd)
    def _():
        pl.semaphore_wait(ready, jnp.where(last_row, 1, 2))

    def unpack(packs_of, at, store):
        for slab, (group, lane_at, _, _) in enumerate(spots):
            moved = pltpu.roll(packs_of[group, at, :], LANES - lane_at, 1)
            store(slab // planes, slab % planes, moved)

    def pass_on(mine, source, way):
        if source != mine:
            send(source, mine, 0).wait_recv()
            send(source, mine, 1).wait_recv()

        def start():
            for copy in relay(way):
                copy.start()

        if way:
            pl.when(jnp.logical_not(last_row))(start)
        else:
            start()

    def relays(mine):
        @pl.when(first_row)
        def _():
            pass_on(mine, across - 1, 1)
            pl.semaphore_wait(ready, 1)
            pass_on(mine, 0, 0)

        @pl.when(jnp.logical_not(first_row))
        def _():
            for source, way in sorted(ends, key=lambda end: end[0] != mine):
                pass_on(mine, source, way)

        for source in peers(mine):
            if source not in (0, across - 1):
                send(source, mine, 0).wait_recv()
                send(source, mine, 1).wait_recv()

    on_each(relays)

    def settle(wanted):
        def action(mine):
            for source in peers(mine):
                for n in pieces:
                    if n in wanted:
                        send(source, mine, n).wait_recv()

        on_each(action)

    every = list(range(wt + 1))
    before = [tile for tile in every if tile != wt - 1]

    def advance(load, store, tiles, seam=None):
        for tile in tiles:
            for plane in range(planes):
                is_open = load(0, plane, tile, 0) != 0.0
                fields = [stream(load, (wt + 1, planes), slot, plane, tile, 0.0, seam) for slot in range(Q)]
                result = collide_tile(fields, is_open, None, SOLID)
                for slot in range(Q):
                    store(slot, plane, tile, result[slot])

    def window(source, tiles):
        start = jnp.minimum(rows * source + 1, height - 1 - ROWS)

        def load(slot, plane, tile, dy):
            at = pl.ds(start - dy, ROWS)
            if tile == wt:
                return sides[place_of[slot], plane, at, :]
            return post[place_of[slot], plane, tile, at, :]

        def store(slot, plane, tile, value):
            post2[place_of[slot], plane, tile, pl.ds(ROWS + start, ROWS), :] = value

        def seam(slot, plane, tile, dy):
            if tile != wt - 1:
                return load(slot, plane, tile, dy)
            pair = [slot in both for both in PAIRS].index(True)
            return seams[pair, plane, pl.ds(start - dy, ROWS), :]

        advance(load, store, tiles, seam)

    row = lax.broadcasted_iota(jnp.int32, (ROWS, LANES), 0)
    half = ROWS // 2

    def fill():
        for slot in range(Q):
            for plane in range(planes):
                for tile in range(wt):
                    ring[slot, plane, tile, HALO:half, :] = post[slot, plane, tile, 0:HALO, :]
                    ring[slot, plane, tile, half : half + HALO, :] = post[
                        slot, plane, tile, height - HALO : height, :
                    ]
        for group in range(groups):
            ring_edges[group, HALO:half, :] = edges[group, 0:HALO, :]
            ring_edges[group, half : half + HALO, :] = edges[group, height - HALO : height, :]

    def rim():
        top, low = ROWS - HALO, height + HALO

        def load(slot, plane, tile, dy):
            value = ring[place_of[slot], plane, tile]
            return pltpu.roll(value, dy % ROWS, 0) if dy else value

        def store(slot, plane, tile, value):
            place = place_of[slot]
            pltpu.store(
                post2.at[place, plane, tile, top : top + ROWS, :], value,
                mask=(row >= 1) & (row < 3),
            )
            pltpu.store(
                post2.at[place, plane, tile, low : low + ROWS, :], value,
                mask=(row >= half + 1) & (row < half + 3),
            )

        advance(load, store, every)

    def unpack_from(step, carry):
        at = pl.ds(pl.multiple_of(lax.rem(me + step, across) * rows, ROWS), rows)

        def store(slot, plane, value):
            if slot < Q:
                sides[slot, plane, at, :] = value
            else:
                seams[slot - Q, plane, at, :] = value

        unpack(edges, at, store)
        return carry

    def unpack_ring():
        def store(slot, plane, value):
            if slot < Q:
                ring[slot, plane, wt] = value

        unpack(ring_edges, pl.ds(0, ROWS), store)

    lax.fori_loop(1, across, unpack_from, 0)
    fill()
    def windows(tiles):
        def window_from(step, carry):
            window(lax.rem(me + step, across), tiles)
            return carry

        lax.fori_loop(1, across, window_from, 0)

    @pl.when(goes_by)
    def _():
        around.wait_recv()
        onward.start()

    settle((2,))
    windows(before)
    settle((3,))
    window(me, every)
    def halo():
        for way in range(2):
            both(h_recv.at[way, 0], wt)
            some_edges(h_recv.at[way, 1], ring_edges.at[:, 0:HALO, :])
        unpack_ring()
        rim()

    def own_flow():
        for plane in range(planes):
            for tile in range(wt):
                def store(slot, value):
                    done[slot, plane, :, tile * LANES : (tile + 1) * LANES] = value

                flow_tile(post2, pl.multiple_of(me * rows, ROWS), plane, tile, wt + 1, store)

    def last_windows():
        settle((4,))
        windows([wt - 1])

    @pl.when(odd)
    def _():
        halo()
        if across == 2:
            own_flow()
        last_windows()
        if across != 2:
            own_flow()

    @pl.when(jnp.logical_not(odd))
    def _():
        last_windows()
        halo()
        own_flow()

    def sent(mine):
        for target in peers(mine):
            for n in (0, 1, 2):
                if n not in pieces:
                    continue
                if n == lead:
                    pl.when(odd)(send(mine, target, n).wait_send)
                else:
                    send(mine, target, n).wait_send()
            low, high = rest(mine)
            last_tile = box.at[:, :, wt - 1 : wt, low:high, :]
            pltpu.make_async_copy(last_tile, last_tile, n_send.at[(target - mine) % across - 1, 3]).wait()

    pl.when(goes_by)(onward.wait_send)
    on_each(sent)
    both(h_send.at[0, 0], wt)
    some_edges(h_send.at[0, 1], ring_edges.at[:, 0:HALO, :])

    @pl.when(jnp.logical_not(last_row))
    def _():
        both(h_send.at[1, 0], wt)
        some_edges(h_send.at[1, 1], ring_edges.at[:, 0:HALO, :])

    @pl.when(last_strip)
    def _():
        both(w_send.at[0], strips)
        some_edges(w_send.at[1], packs.at[:, :, 0:HALO, :])


def flow_tile(post, start, plane, tile, tiles, store):
    planes = post.shape[1]

    def load(slot, plane, tile, dy):
        return post[place_of[slot], plane, tile, pl.ds(ROWS + start - dy, ROWS), :]

    is_open = load(0, plane, tile, 0) != SOLID
    for slot in range(Q):
        value = stream(load, (tiles, planes), slot, plane, tile, SOLID)
        store(slot, jnp.where(is_open, value, 0.0))


def finish(across, post, done, out_ref, flow, sems):
    _, planes, rows, width = done.shape
    wt = width // LANES
    me = lax.axis_index("px")

    def own_copy():
        at = pl.ds(pl.multiple_of(me * rows, ROWS), rows)
        return pltpu.make_async_copy(done, out_ref.at[:, :, at, :], sems.at[0])

    def copy_of(step, plane):
        at = pl.ds(pl.multiple_of(lax.rem(me + step, across) * rows, ROWS), rows)
        return pltpu.make_async_copy(
            flow.at[step - 1, :, plane], out_ref.at[:, plane, at, :], sems.at[1 + (step - 1) * planes + plane]
        )

    own_copy().start()

    def write(step, carry):
        for plane in range(planes):
            for tile in range(wt):
                def store(slot, value):
                    flow[step - 1, slot, plane, :, tile * LANES : (tile + 1) * LANES] = value

                start = pl.multiple_of(lax.rem(me + step, across) * rows, ROWS)
                flow_tile(post, start, plane, tile, wt + 1, store)
            copy_of(step, plane).start()
        return carry

    lax.fori_loop(1, across, write, 0)
    own_copy().wait()

    def written(step, carry):
        for plane in range(planes):
            copy_of(step, plane).wait()
        return carry

    lax.fori_loop(1, across, written, 0)


def body(across, along, populations, pore):
    count, planes, rows, columns = populations.shape
    height = across * rows
    width = columns // across
    strips = columns // LANES
    wt = strips // across
    groups = edge_layout(planes)[1]
    tall = height + 2 * ROWS
    post2, done = pl.pallas_call(
        functools.partial(kernel, across, along),
        out_shape=(
            pltpu.VMEM((count, planes, wt + 1, tall, LANES), jnp.float32),
            pltpu.VMEM((count, planes, rows, width), jnp.float32),
        ),
        in_specs=[pl.BlockSpec(memory_space=pltpu.HBM)] * 2,
        out_specs=[pl.BlockSpec(memory_space=pltpu.VMEM)] * 2,
        scratch_shapes=[
            pltpu.VMEM((count, planes, strips, rows, LANES), jnp.float32),
            pltpu.VMEM((planes, rows, columns), jnp.int32),
            pltpu.VMEM((count, planes, strips, rows, LANES), jnp.float32),
            pltpu.VMEM((count, planes, wt, height, LANES), jnp.float32),
            pltpu.VMEM((count, planes, height, LANES), jnp.float32),
            pltpu.VMEM((len(PAIRS), planes, height, LANES), jnp.float32),
            pltpu.VMEM((count, planes, wt + 1, ROWS, LANES), jnp.float32),
            pltpu.VMEM((across, groups, rows, LANES), jnp.float32),
            pltpu.VMEM((groups, height, LANES), jnp.float32),
            pltpu.VMEM((groups, ROWS, LANES), jnp.float32),
            pltpu.VMEM((count, planes, 1, HALO, LANES), jnp.float32),
            pltpu.SemaphoreType.DMA((2 + (across - 1) * wt * planes,)),
            pltpu.SemaphoreType.DMA((across - 1, 4)),
            pltpu.SemaphoreType.DMA((across - 1, 5)),
            pltpu.SemaphoreType.DMA((2, 2)),
            pltpu.SemaphoreType.DMA((2, 2)),
            pltpu.SemaphoreType.DMA((2,)),
            pltpu.SemaphoreType.DMA((2,)),
            pltpu.SemaphoreType.REGULAR,
            pltpu.SemaphoreType.REGULAR,
            pltpu.SemaphoreType.REGULAR,
        ],
        compiler_params=pltpu.CompilerParams(
            collective_id=0, has_side_effects=True, vmem_limit_bytes=VMEM_LIMIT
        ),
    )(*(pltpu.with_memory_space_constraint(x, pltpu.HBM) for x in (populations, pore)))
    return pl.pallas_call(
        functools.partial(finish, across),
        out_shape=jax.ShapeDtypeStruct((count, planes, height, width), jnp.float32),
        in_specs=[pl.BlockSpec(memory_space=pltpu.VMEM)] * 2,
        out_specs=pl.BlockSpec(memory_space=pl.ANY),
        scratch_shapes=[
            pltpu.VMEM((across - 1, count, planes, rows, width), jnp.float32),
            pltpu.SemaphoreType.DMA((1 + (across - 1) * planes,)),
        ],
        compiler_params=pltpu.CompilerParams(vmem_limit_bytes=VMEM_LIMIT),
    )(post2, done)


def solution(mesh):
    return jax.shard_map(
        functools.partial(body, mesh.shape["px"], mesh.shape["py"]),
        mesh=mesh,
        in_specs=(P(None, None, ("py", "px"), None), P(None, ("py", "px"), None)),
        out_specs=P(None, None, "py", "px"),
        check_vma=False,
    )
```

```python
import functools

import jax
import jax.numpy as jnp
from jax import lax
from jax.experimental import pallas as pl
from jax.experimental.pallas import tpu as pltpu
from jax.sharding import PartitionSpec as P

MESH = pl.DeviceIdType.MESH

lattice_velocity = [
    (0, 0, 0),
    (1, 0, 0),
    (-1, 0, 0),
    (0, 1, 0),
    (0, -1, 0),
    (0, 0, 1),
    (0, 0, -1),
    (1, 1, 0),
    (-1, -1, 0),
    (1, -1, 0),
    (-1, 1, 0),
    (1, 0, 1),
    (-1, 0, -1),
    (1, 0, -1),
    (-1, 0, 1),
    (0, 1, 1),
    (0, -1, -1),
    (0, 1, -1),
    (0, -1, 1),
]
lattice_weights = [1.0 / 3.0] + [1.0 / 18.0] * 6 + [1.0 / 36.0] * 12
opposite = [0, 2, 1, 4, 3, 6, 5, 8, 7, 10, 9, 12, 11, 14, 13, 16, 15, 18, 17]
relax_time = 0.8
body_force = 0.005

Q = len(lattice_velocity)
LANES = 128
ROWS = 8
HALO = 2
VMEM_LIMIT = 32 * 1024 * 1024
SOLID = -3.0e38
TINY = 1.0e-30

order = sorted(range(Q), key=lambda slot: lattice_velocity[slot][1])
place_of = [order.index(slot) for slot in range(Q)]
RISE = sum(1 for vector in lattice_velocity if vector[1] < 0)
FALL = Q - sum(1 for vector in lattice_velocity if vector[1] > 0)
PAIRS = [(s, opposite[s]) for s in range(Q) if lattice_velocity[s][0] > 0]


def edge_layout(planes):
    spots, group, at = [], 0, 0
    for field in range(Q + len(PAIRS)):
        dx = lattice_velocity[order[field]][0] if field < Q else 0
        left, right = 1 + (dx > 0), 1 + (dx < 0)
        for _ in range(planes):
            if at + left + right > LANES:
                group, at = group + 1, 0
            spots.append((group, at + left, left, right))
            at += left + right
    return spots, group + 1


def total(values):
    while len(values) > 1:
        pairs = [x + y for x, y in zip(values[::2], values[1::2])]
        values = pairs + values[2 * len(pairs) :]
    return values[0]


def collide_tile(fields, is_open, guard, closed):
    keep = 1.0 - 1.0 / relax_time
    gain = 1.0 / relax_time
    density = jnp.where(is_open, total(fields), 1.0)
    inverse = 1.0 / density
    vel = []
    for column in range(3):
        plus = [fields[s] for s in range(Q) if lattice_velocity[s][column] > 0]
        minus = [fields[s] for s in range(Q) if lattice_velocity[s][column] < 0]
        vel.append((total(plus) - total(minus)) * inverse)
    vel[2] = vel[2] + relax_time * body_force
    speed = vel[0] * vel[0] + vel[1] * vel[1] + vel[2] * vel[2]
    base = 1.0 - 1.5 * speed
    result = [None] * Q
    scaled = {w: density * (gain * w) for w in sorted(set(lattice_weights))}

    def close(value):
        return jnp.where(is_open, value + guard if guard else value, closed)

    result[0] = close(keep * fields[0] + scaled[lattice_weights[0]] * base)
    for slot in range(1, Q, 2):
        other = opposite[slot]
        along = None
        for column in range(3):
            sign = lattice_velocity[slot][column]
            if sign == 0:
                continue
            term = vel[column]
            if along is None:
                along = term if sign > 0 else -term
            else:
                along = along + term if sign > 0 else along - term
        weight = scaled[lattice_weights[slot]]
        triple = 3.0 * along
        even = weight * (base + 0.5 * triple * triple)
        odd = weight * triple
        result[slot] = close(keep * fields[slot] + (even + odd))
        result[other] = close(keep * fields[other] + (even - odd))
    return result


def stream(load, sides, slot, plane, tile, closed, seam=None):
    tiles, planes = sides
    dx, dy, dz = lattice_velocity[slot]
    source = (plane - dz) % planes
    value = load(slot, source, tile, dy)
    if dx:
        lane = lax.broadcasted_iota(jnp.int32, value.shape, 1)
        beside = (seam or load)(slot, source, (tile - dx) % tiles, dy)
        value = jnp.where(lane == (LANES - 1 if dx > 0 else 0), beside, value)
        value = pltpu.roll(value, dx % LANES, 1)
    if slot:
        value = jnp.where(value != closed, value, load(opposite[slot], plane, tile, 0))
    return value


def kernel(
    across, along, pop_ref, pore_ref, post2, done,
    raw, voxels, box, post, sides, seams, ring, packs, edges, ring_edges, via,
    load_sem, n_send, n_recv, h_send, h_recv, w_send, via_sem, go, ready, path,
):
    _, planes, strips, rows, _ = box.shape
    wt = strips // across
    height = across * rows
    spots, groups = edge_layout(planes)
    slabs = Q * planes
    me = lax.axis_index("px")
    here = lax.axis_index("py")
    up = lax.rem(here + along - 1, along)
    down = lax.rem(here + 1, along)
    first_row = here == 0
    last_row = here == along - 1
    odd = lax.rem(here, 2) == 1
    last_strip = last_row & (me == across - 1)
    end = across - 1
    quarter = along // 4
    short = odd & (here < quarter)
    goes_by = odd & (here >= quarter) & (here < 2 * quarter) & (me == 0)

    load_pore = pltpu.make_async_copy(pore_ref, voxels, load_sem.at[0])
    load_pore.start()

    own_load = (across - 1) * wt * planes

    def load_tile(step, k, plane):
        tile = lax.rem(me + step, across) * wt + k
        cols = pl.ds(pl.multiple_of(tile * LANES, LANES), LANES)
        return pltpu.make_async_copy(
            pop_ref.at[:, plane, :, cols],
            raw.at[:, plane, tile],
            load_sem.at[1 + (((step - 1) * wt + k) * planes + plane if step < across else own_load)],
        )

    halves = [(k, plane) for k in range(wt) for plane in range(planes)]
    for step in range(1, across + 1):
        for k, plane in halves:
            load_tile(step, k, plane).start()

    barrier = pltpu.get_barrier_semaphore()

    def greet(x, y):
        pl.semaphore_signal(barrier, inc=1, device_id=(x, y), device_id_type=MESH)

    def answer(y):
        pl.semaphore_signal(ready, inc=1, device_id=(me, y), device_id_type=MESH)

    for step in range(1, across):
        greet(lax.rem(me + step, across), here)

    @pl.when(odd)
    def _():
        greet(me, up)

        @pl.when(jnp.logical_not(last_row))
        def _():
            greet(me, down)

    @pl.when(short & (me == 0))
    def _():
        greet(0, here + quarter)

    @pl.when(first_row)
    def _():
        greet(me, along - 1)

        @pl.when(me != across - 1)
        def _():
            greet(across - 1, along - 1)

    def enter():
        greeted = jnp.where(odd, 0, 2) - jnp.where(first_row, 1, 0)
        greeted = greeted + jnp.where(last_row, jnp.where(me == across - 1, across, 1), 0)
        greeted = greeted + jnp.where(goes_by, 1, 0)
        pl.semaphore_wait(barrier, across - 1 + greeted)

        @pl.when(goes_by)
        def _():
            pl.semaphore_signal(path, inc=1, device_id=(0, here - quarter), device_id_type=MESH)

        @pl.when(jnp.logical_not(odd))
        def _():
            answer(down)

            @pl.when(here != 0)
            def _():
                answer(up)

        @pl.when(last_row)
        def _():
            answer(0)

    load_pore.wait()

    def collide_strip(tile, plane, own):
        cols = pl.ds(pl.multiple_of(tile * LANES, LANES), LANES)
        fields = [raw[slot, plane, tile] for slot in range(Q)]
        is_open = voxels[plane, :, cols] > 0
        result = collide_tile(fields, is_open, TINY, 0.0)
        for slot in range(Q):
            box[place_of[slot], plane, tile] = result[slot]
            if own is not None:
                at = pl.ds(pl.multiple_of(me * rows, ROWS), rows)
                post[place_of[slot], plane, own, at, :] = result[slot]

    def outer(source):
        return (rows - HALO, rows) if source == across - 1 else (0, HALO)

    def inner(source):
        return (0, HALO) if source == across - 1 else (rows - HALO, rows)

    def middle(source):
        return (HALO, rows - HALO)

    def send(source, target, n, part=None):
        if part:
            k, plane = part
            low, high = outer(source)
            return pltpu.make_async_remote_copy(
                src_ref=box.at[:, plane, target * wt + k, low:high, :],
                dst_ref=post.at[:, plane, k, source * rows + low : source * rows + high, :],
                send_sem=n_send.at[(target - source) % across - 1, (0, 1, 2, 2, 3, 3)[n]],
                recv_sem=n_recv.at[(target - source) % across - 1, (0, 1, 2, 2, 3, 4)[n]],
                device_id=(target, here),
                device_id_type=MESH,
            )
        if n == 1:
            src, dst = packs.at[target], edges.at[:, source * rows : (source + 1) * rows, :]
        else:
            low, high = (outer, None, inner, inner, middle, middle)[n](source)
            first, last = ((0, wt), None, (0, wt - 1), (wt - 1, wt))[n if n < 4 else n - 2]
            src = box.at[:, :, target * wt + first : target * wt + last, low:high, :]
            start = source * rows
            dst = post.at[:, :, first:last, start + low : start + high, :]
        return pltpu.make_async_remote_copy(
            src_ref=src,
            dst_ref=dst,
            send_sem=n_send.at[(target - source) % across - 1, (0, 1, 2, 2, 3, 3)[n]],
            recv_sem=n_recv.at[(target - source) % across - 1, (0, 1, 2, 2, 3, 4)[n]],
            device_id=(target, here),
            device_id_type=MESH,
        )

    pieces = [0, 1, 2, 3, 4, 5] if wt > 1 else [0, 1, 3, 5]

    def relay(way):
        if way == 0:
            near, beyond, part, to = 0, 1, (0, RISE), up
            near_to, beyond_to, low, low_to = ROWS - 2, ROWS - 1, 0, ROWS - HALO
        else:
            near, beyond, part, to = height - 1, height - 2, (FALL, Q), down
            near_to, beyond_to, low, low_to = 1, 0, height - HALO, 0
        some = slice(*part)
        refs = [
            (post.at[:, :, :, near : near + 1, :],
             ring.at[:, :, 0:wt, near_to : near_to + 1, :]),
            (post.at[some, :, :, beyond : beyond + 1, :],
             ring.at[some, :, 0:wt, beyond_to : beyond_to + 1, :]),
            (edges.at[:, low : low + HALO, :], ring_edges.at[:, low_to : low_to + HALO, :]),
        ]
        return [
            pltpu.make_async_remote_copy(
                src_ref=src,
                dst_ref=dst,
                send_sem=h_send.at[way, n // 2],
                recv_sem=h_recv.at[way, n // 2],
                device_id=(me, to),
                device_id_type=MESH,
            )
            for n, (src, dst) in enumerate(refs)
        ]

    def peers(mine):
        return [(mine + step) % across for step in range(1, across)]

    def on_each(action):
        for mine in range(across):
            pl.when(me == mine)(functools.partial(action, mine))

    def begin(wanted):
        def action(mine):
            for n in pieces:
                if n in wanted:
                    for target in peers(mine):
                        send(mine, target, n).start()

        on_each(action)

    def direct(target, which=range(3)):
        cols = slice(target * wt, (target + 1) * wt)
        refs = [
            (box.at[:, :, cols, rows - 1 : rows, :], ring.at[:, :, 0:wt, 1:2, :]),
            (box.at[FALL:Q, :, cols, rows - HALO : rows - 1, :], ring.at[FALL:Q, :, 0:wt, 0:1, :]),
            (packs.at[target, :, rows - HALO : rows, :], ring_edges.at[:, 0:HALO, :]),
        ]
        return [
            pltpu.make_async_remote_copy(
                src_ref=src,
                dst_ref=dst,
                send_sem=w_send.at[n // 2],
                recv_sem=h_recv.at[1, n // 2],
                device_id=(target, 0),
                device_id_type=MESH,
            )
            for n, (src, dst) in enumerate(refs)
            if n in which
        ]

    def send_direct(targets, which):
        @pl.when(last_strip)
        def _():
            for target in targets:
                for copy in direct(target, which):
                    copy.start()


    for step in range(1, across):
        for k, plane in halves:
            load_tile(step, k, plane).wait()
            collide_strip(lax.rem(me + step, across) * wt + k, plane, None)
            if step == 1 and (k, plane) == (0, 0):
                enter()

            def begin_outer(mine):
                send(mine, (mine + step) % across, 0, (k, plane)).start()

            on_each(begin_outer)
    send_direct(range(across - 1), (0, 1))
    own = raw.at[:, :, pl.ds(me * wt, wt)]
    pltpu.make_async_copy(own, own, load_sem.at[1 + own_load]).wait()
    for k, plane in halves:
        collide_strip(me * wt + k, plane, k)
    send_direct((across - 1,), (0, 1))

    lane = lax.broadcasted_iota(jnp.int32, (rows, LANES), 1)
    for step in range(1, across + 1):
        target = lax.rem(me + step, across)
        first = lax.rem((target + 1) * wt, strips)
        last = lax.rem(target * wt + strips - 1, strips)
        own_at = pl.ds(pl.multiple_of(me * rows, ROWS), rows)
        packed = [None] * groups
        for slab, (group, at, left_of, right_of) in enumerate(spots):
            field, plane = slab // planes, slab % planes
            if slab < slabs:
                edge = jnp.where(lane < LANES // 2, box[field, plane, first], box[field, plane, last])
                if step == across:
                    sides[field, plane, own_at, :] = edge
            else:
                right, left = (place_of[slot] for slot in PAIRS[field - Q])
                tile = target * wt + wt - 1
                edge = jnp.where(lane < LANES // 2, box[left, plane, tile], box[right, plane, tile])
                if step == across:
                    seams[field - Q, plane, own_at, :] = edge
            moved = pltpu.roll(edge, at, 1)
            if packed[group] is not None:
                moved = jnp.where((lane >= at - left_of) & (lane < at + right_of), moved, packed[group])
            packed[group] = moved
        for group in range(groups):
            packs[target, group] = packed[group]
            if step == across:
                edges[group, own_at, :] = packed[group]
        if step == across - 1:
            begin((1,))

            @pl.when(jnp.logical_not(odd))
            def _():
                begin((2, 3, 4, 5))

    send_direct(range(across), (2,))

    def both(sem, tiles):
        rows_of = box.at[0 : (Q + RISE) // 2, :, 0:tiles, 0:2, :]
        pltpu.make_async_copy(rows_of, rows_of, sem).wait()

    def some_edges(sem, refs):
        pltpu.make_async_copy(refs, refs, sem).wait()

    def all_of(sem, part, mine):
        low, high = part(mine)
        refs = box.at[:, :, 0:wt, low:high, :]
        pltpu.make_async_copy(refs, refs, sem).wait()


    low, high = inner(end)
    around = pltpu.make_async_remote_copy(
        src_ref=box.at[:, :, wt - 1 : wt, low:high, :],
        dst_ref=via,
        send_sem=n_send.at[(0 - end) % across - 1, 2],
        recv_sem=via_sem.at[0],
        device_id=(0, here + quarter),
        device_id_type=MESH,
    )
    onward = pltpu.make_async_remote_copy(
        src_ref=via,
        dst_ref=post.at[:, :, wt - 1 : wt, end * rows + low : end * rows + high, :],
        send_sem=via_sem.at[1],
        recv_sem=n_recv.at[(0 - end) % across - 1, 2],
        device_id=(0, here - quarter),
        device_id_type=MESH,
    )

    @pl.when(short & (me == 0))
    def _():
        pl.semaphore_wait(path, 1)
        pl.semaphore_signal(path, inc=1, device_id=(end, here), device_id_type=MESH)

    @pl.when(odd)
    def _():
        pl.semaphore_wait(ready, jnp.where(last_row, 1, 2))

    def start_relay(way):
        for copy in relay(way):
            copy.start()

    @pl.when((me == 0) & jnp.logical_not(first_row))
    def _():
        start_relay(0)

    @pl.when((me == end) & jnp.logical_not(last_row))
    def _():
        start_relay(1)

    @pl.when(short & (me == end))
    def _():
        pl.semaphore_wait(path, 1)
        around.start()

    def begin_late(mine):
        for n in pieces:
            for target in peers(mine):
                if n == 3 and (mine, target) == (end, 0):
                    pl.when(jnp.logical_not(short))(send(mine, target, n).start)
                elif n >= 2:
                    send(mine, target, n).start()

    @pl.when(odd)
    def _():
        pl.semaphore_wait(go, 1)
        on_each(begin_late)

    def lead_sent(mine):
        for target in peers(mine):
            all_of(n_send.at[(target - mine) % across - 1, 2], inner, mine)

    @pl.when(jnp.logical_not(odd))
    def _():
        on_each(lead_sent)
        pl.semaphore_signal(go, inc=1, device_id=(me, down), device_id_type=MESH)

    def unpack(packs_of, at, store):
        for slab, (group, lane_at, _, _) in enumerate(spots):
            moved = pltpu.roll(packs_of[group, at, :], LANES - lane_at, 1)
            store(slab // planes, slab % planes, moved)

    def take_outer(source, mine):
        send(source, mine, 0).wait_recv()
        send(source, mine, 1).wait_recv()

    def relays(mine):
        if mine != end:
            take_outer(end, mine)
            pl.when(jnp.logical_not(last_row))(functools.partial(start_relay, 1))
        if mine != 0:
            take_outer(0, mine)
            pl.when(jnp.logical_not(first_row))(functools.partial(start_relay, 0))

        @pl.when(first_row)
        def _():
            pl.semaphore_wait(ready, 1)
            start_relay(0)

        for source in peers(mine):
            if source not in (0, end):
                take_outer(source, mine)

    on_each(relays)

    def settle(n):
        def action(mine):
            for source in peers(mine):
                if n == 2:
                    all_of(n_recv.at[(mine - source) % across - 1, 2], inner, source)
                elif n + 1 in pieces:
                    send(source, mine, n + 1).wait_recv()

        on_each(action)

    every = list(range(wt + 1))
    before = [tile for tile in every if tile != wt - 1]

    def advance(load, store, tiles, seam=None):
        for tile in tiles:
            for plane in range(planes):
                is_open = load(0, plane, tile, 0) != 0.0
                fields = [stream(load, (wt + 1, planes), slot, plane, tile, 0.0, seam) for slot in range(Q)]
                result = collide_tile(fields, is_open, None, SOLID)
                for slot in range(Q):
                    store(slot, plane, tile, result[slot])

    def window(source, tiles):
        start = jnp.minimum(rows * source + 1, height - 1 - ROWS)

        def load(slot, plane, tile, dy):
            at = pl.ds(start - dy, ROWS)
            if tile == wt:
                return sides[place_of[slot], plane, at, :]
            return post[place_of[slot], plane, tile, at, :]

        def store(slot, plane, tile, value):
            post2[place_of[slot], plane, tile, pl.ds(ROWS + start, ROWS), :] = value

        def seam(slot, plane, tile, dy):
            if tile != wt - 1:
                return load(slot, plane, tile, dy)
            pair = [slot in both for both in PAIRS].index(True)
            return seams[pair, plane, pl.ds(start - dy, ROWS), :]

        advance(load, store, tiles, seam)

    row = lax.broadcasted_iota(jnp.int32, (ROWS, LANES), 0)
    half = ROWS // 2

    def fill():
        for slot in range(Q):
            for plane in range(planes):
                for tile in range(wt):
                    ring[slot, plane, tile, HALO:half, :] = post[slot, plane, tile, 0:HALO, :]
                    ring[slot, plane, tile, half : half + HALO, :] = post[
                        slot, plane, tile, height - HALO : height, :
                    ]
        for group in range(groups):
            ring_edges[group, HALO:half, :] = edges[group, 0:HALO, :]
            ring_edges[group, half : half + HALO, :] = edges[group, height - HALO : height, :]

    def rim():
        top, low = ROWS - HALO, height + HALO

        def load(slot, plane, tile, dy):
            value = ring[place_of[slot], plane, tile]
            return pltpu.roll(value, dy % ROWS, 0) if dy else value

        def store(slot, plane, tile, value):
            place = place_of[slot]
            pltpu.store(
                post2.at[place, plane, tile, top : top + ROWS, :], value,
                mask=(row >= 1) & (row < 3),
            )
            pltpu.store(
                post2.at[place, plane, tile, low : low + ROWS, :], value,
                mask=(row >= half + 1) & (row < half + 3),
            )

        advance(load, store, every)

    def unpack_from(step, carry):
        at = pl.ds(pl.multiple_of(lax.rem(me + step, across) * rows, ROWS), rows)

        def store(slot, plane, value):
            if slot < Q:
                sides[slot, plane, at, :] = value
            else:
                seams[slot - Q, plane, at, :] = value

        unpack(edges, at, store)
        return carry

    def unpack_ring():
        def store(slot, plane, value):
            if slot < Q:
                ring[slot, plane, wt] = value

        unpack(ring_edges, pl.ds(0, ROWS), store)

    lax.fori_loop(1, across, unpack_from, 0)
    fill()
    def windows(tiles):
        def window_from(step, carry):
            window(lax.rem(me + step, across), tiles)
            return carry

        lax.fori_loop(1, across, window_from, 0)

    @pl.when(goes_by)
    def _():
        around.wait_recv()
        onward.start()

    def halo():
        for way in range(2):
            both(h_recv.at[way, 0], wt)
            some_edges(h_recv.at[way, 1], ring_edges.at[:, 0:HALO, :])
        unpack_ring()
        rim()

    def own_flow():
        for plane in range(planes):
            for tile in range(wt):
                def store(slot, value):
                    done[slot, plane, :, tile * LANES : (tile + 1) * LANES] = value

                flow_tile(post2, pl.multiple_of(me * rows, ROWS), plane, tile, wt + 1, store)

    def own_window():
        settle(2)
        window(me, every)

    def first_windows():
        settle(3)
        windows(before)

    def last_windows():
        settle(4)
        windows([wt - 1])

    @pl.when(odd)
    def _():
        halo()
        own_window()
        if across == 2:
            own_flow()
        first_windows()
        last_windows()
        if across != 2:
            own_flow()

    @pl.when(jnp.logical_not(odd))
    def _():
        own_window()
        first_windows()
        last_windows()
        halo()
        own_flow()

    def sent(mine):
        for target in peers(mine):
            send(mine, target, 0).wait_send()
            send(mine, target, 1).wait_send()
            sem = (target - mine) % across - 1
            pl.when(odd)(functools.partial(all_of, n_send.at[sem, 2], inner, mine))
            all_of(n_send.at[sem, 3], middle, mine)

    pl.when(goes_by)(onward.wait_send)
    on_each(sent)
    both(h_send.at[0, 0], wt)
    some_edges(h_send.at[0, 1], ring_edges.at[:, 0:HALO, :])

    @pl.when(jnp.logical_not(last_row))
    def _():
        both(h_send.at[1, 0], wt)
        some_edges(h_send.at[1, 1], ring_edges.at[:, 0:HALO, :])

    @pl.when(last_strip)
    def _():
        both(w_send.at[0], strips)
        some_edges(w_send.at[1], packs.at[:, :, 0:HALO, :])


def flow_tile(post, start, plane, tile, tiles, store):
    planes = post.shape[1]

    def load(slot, plane, tile, dy):
        return post[place_of[slot], plane, tile, pl.ds(ROWS + start - dy, ROWS), :]

    is_open = load(0, plane, tile, 0) != SOLID
    for slot in range(Q):
        value = stream(load, (tiles, planes), slot, plane, tile, SOLID)
        store(slot, jnp.where(is_open, value, 0.0))


def finish(across, post, done, out_ref, flow, sems):
    _, planes, rows, width = done.shape
    wt = width // LANES
    me = lax.axis_index("px")

    def own_copy():
        at = pl.ds(pl.multiple_of(me * rows, ROWS), rows)
        return pltpu.make_async_copy(done, out_ref.at[:, :, at, :], sems.at[0])

    def copy_of(step, plane):
        at = pl.ds(pl.multiple_of(lax.rem(me + step, across) * rows, ROWS), rows)
        return pltpu.make_async_copy(
            flow.at[step - 1, :, plane], out_ref.at[:, plane, at, :], sems.at[1 + (step - 1) * planes + plane]
        )

    own_copy().start()

    def write(step, carry):
        for plane in range(planes):
            for tile in range(wt):
                def store(slot, value):
                    flow[step - 1, slot, plane, :, tile * LANES : (tile + 1) * LANES] = value

                start = pl.multiple_of(lax.rem(me + step, across) * rows, ROWS)
                flow_tile(post, start, plane, tile, wt + 1, store)
            copy_of(step, plane).start()
        return carry

    lax.fori_loop(1, across, write, 0)
    own_copy().wait()

    def written(step, carry):
        for plane in range(planes):
            copy_of(step, plane).wait()
        return carry

    lax.fori_loop(1, across, written, 0)


def body(across, along, populations, pore):
    count, planes, rows, columns = populations.shape
    height = across * rows
    width = columns // across
    strips = columns // LANES
    wt = strips // across
    groups = edge_layout(planes)[1]
    tall = height + 2 * ROWS
    post2, done = pl.pallas_call(
        functools.partial(kernel, across, along),
        out_shape=(
            pltpu.VMEM((count, planes, wt + 1, tall, LANES), jnp.float32),
            pltpu.VMEM((count, planes, rows, width), jnp.float32),
        ),
        in_specs=[pl.BlockSpec(memory_space=pltpu.HBM)] * 2,
        out_specs=[pl.BlockSpec(memory_space=pltpu.VMEM)] * 2,
        scratch_shapes=[
            pltpu.VMEM((count, planes, strips, rows, LANES), jnp.float32),
            pltpu.VMEM((planes, rows, columns), jnp.int32),
            pltpu.VMEM((count, planes, strips, rows, LANES), jnp.float32),
            pltpu.VMEM((count, planes, wt, height, LANES), jnp.float32),
            pltpu.VMEM((count, planes, height, LANES), jnp.float32),
            pltpu.VMEM((len(PAIRS), planes, height, LANES), jnp.float32),
            pltpu.VMEM((count, planes, wt + 1, ROWS, LANES), jnp.float32),
            pltpu.VMEM((across, groups, rows, LANES), jnp.float32),
            pltpu.VMEM((groups, height, LANES), jnp.float32),
            pltpu.VMEM((groups, ROWS, LANES), jnp.float32),
            pltpu.VMEM((count, planes, 1, HALO, LANES), jnp.float32),
            pltpu.SemaphoreType.DMA((2 + (across - 1) * wt * planes,)),
            pltpu.SemaphoreType.DMA((across - 1, 4)),
            pltpu.SemaphoreType.DMA((across - 1, 5)),
            pltpu.SemaphoreType.DMA((2, 2)),
            pltpu.SemaphoreType.DMA((2, 2)),
            pltpu.SemaphoreType.DMA((2,)),
            pltpu.SemaphoreType.DMA((2,)),
            pltpu.SemaphoreType.REGULAR,
            pltpu.SemaphoreType.REGULAR,
            pltpu.SemaphoreType.REGULAR,
        ],
        compiler_params=pltpu.CompilerParams(
            collective_id=0, has_side_effects=True, vmem_limit_bytes=VMEM_LIMIT
        ),
    )(*(pltpu.with_memory_space_constraint(x, pltpu.HBM) for x in (populations, pore)))
    return pl.pallas_call(
        functools.partial(finish, across),
        out_shape=jax.ShapeDtypeStruct((count, planes, height, width), jnp.float32),
        in_specs=[pl.BlockSpec(memory_space=pltpu.VMEM)] * 2,
        out_specs=pl.BlockSpec(memory_space=pl.ANY),
        scratch_shapes=[
            pltpu.VMEM((across - 1, count, planes, rows, width), jnp.float32),
            pltpu.SemaphoreType.DMA((1 + (across - 1) * planes,)),
        ],
        compiler_params=pltpu.CompilerParams(vmem_limit_bytes=VMEM_LIMIT),
    )(post2, done)


def solution(mesh):
    return jax.shard_map(
        functools.partial(body, mesh.shape["px"], mesh.shape["py"]),
        mesh=mesh,
        in_specs=(P(None, None, ("py", "px"), None), P(None, ("py", "px"), None)),
        out_specs=P(None, None, "py", "px"),
        check_vma=False,
    )
```

```python
import functools

import jax
import jax.numpy as jnp
from jax import lax
from jax.experimental import pallas as pl
from jax.experimental.pallas import tpu as pltpu
from jax.sharding import PartitionSpec as P

MESH = pl.DeviceIdType.MESH

lattice_velocity = [
    (0, 0, 0),
    (1, 0, 0),
    (-1, 0, 0),
    (0, 1, 0),
    (0, -1, 0),
    (0, 0, 1),
    (0, 0, -1),
    (1, 1, 0),
    (-1, -1, 0),
    (1, -1, 0),
    (-1, 1, 0),
    (1, 0, 1),
    (-1, 0, -1),
    (1, 0, -1),
    (-1, 0, 1),
    (0, 1, 1),
    (0, -1, -1),
    (0, 1, -1),
    (0, -1, 1),
]
lattice_weights = [1.0 / 3.0] + [1.0 / 18.0] * 6 + [1.0 / 36.0] * 12
opposite = [0, 2, 1, 4, 3, 6, 5, 8, 7, 10, 9, 12, 11, 14, 13, 16, 15, 18, 17]
relax_time = 0.8
body_force = 0.005

Q = len(lattice_velocity)
LANES = 128
ROWS = 8
HALO = 2
VMEM_LIMIT = 32 * 1024 * 1024
SOLID = -3.0e38
TINY = 1.0e-30

order = sorted(range(Q), key=lambda slot: lattice_velocity[slot][1])
place_of = [order.index(slot) for slot in range(Q)]
RISE = sum(1 for vector in lattice_velocity if vector[1] < 0)
FALL = Q - sum(1 for vector in lattice_velocity if vector[1] > 0)
PAIRS = [(s, opposite[s]) for s in range(Q) if lattice_velocity[s][0] > 0]


def edge_layout(planes):
    spots, group, at = [], 0, 0
    for field in range(Q + len(PAIRS)):
        dx = lattice_velocity[order[field]][0] if field < Q else 0
        left, right = 1 + (dx > 0), 1 + (dx < 0)
        for _ in range(planes):
            if at + left + right > LANES:
                group, at = group + 1, 0
            spots.append((group, at + left, left, right))
            at += left + right
    return spots, group + 1


def total(values):
    while len(values) > 1:
        pairs = [x + y for x, y in zip(values[::2], values[1::2])]
        values = pairs + values[2 * len(pairs) :]
    return values[0]


def collide_tile(fields, is_open, guard, closed):
    keep = 1.0 - 1.0 / relax_time
    gain = 1.0 / relax_time
    density = jnp.where(is_open, total(fields), 1.0)
    inverse = 1.0 / density
    vel = []
    for column in range(3):
        plus = [fields[s] for s in range(Q) if lattice_velocity[s][column] > 0]
        minus = [fields[s] for s in range(Q) if lattice_velocity[s][column] < 0]
        vel.append((total(plus) - total(minus)) * inverse)
    vel[2] = vel[2] + relax_time * body_force
    speed = vel[0] * vel[0] + vel[1] * vel[1] + vel[2] * vel[2]
    base = 1.0 - 1.5 * speed
    result = [None] * Q
    scaled = {w: density * (gain * w) for w in sorted(set(lattice_weights))}

    def close(value):
        return jnp.where(is_open, value + guard if guard else value, closed)

    result[0] = close(keep * fields[0] + scaled[lattice_weights[0]] * base)
    for slot in range(1, Q, 2):
        other = opposite[slot]
        along = None
        for column in range(3):
            sign = lattice_velocity[slot][column]
            if sign == 0:
                continue
            term = vel[column]
            if along is None:
                along = term if sign > 0 else -term
            else:
                along = along + term if sign > 0 else along - term
        weight = scaled[lattice_weights[slot]]
        triple = 3.0 * along
        even = weight * (base + 0.5 * triple * triple)
        odd = weight * triple
        result[slot] = close(keep * fields[slot] + (even + odd))
        result[other] = close(keep * fields[other] + (even - odd))
    return result


def stream(load, sides, slot, plane, tile, closed, seam=None):
    tiles, planes = sides
    dx, dy, dz = lattice_velocity[slot]
    source = (plane - dz) % planes
    value = load(slot, source, tile, dy)
    if dx:
        lane = lax.broadcasted_iota(jnp.int32, value.shape, 1)
        beside = (seam or load)(slot, source, (tile - dx) % tiles, dy)
        value = jnp.where(lane == (LANES - 1 if dx > 0 else 0), beside, value)
        value = pltpu.roll(value, dx % LANES, 1)
    if slot:
        value = jnp.where(value != closed, value, load(opposite[slot], plane, tile, 0))
    return value


def kernel(
    across, along, pop_ref, pore_ref, post2, done,
    raw, voxels, box, post, sides, seams, ring, packs, edges, ring_edges, via,
    load_sem, n_send, n_recv, h_send, h_recv, w_send, via_sem, go, ready, path,
):
    _, planes, strips, rows, _ = box.shape
    wt = strips // across
    height = across * rows
    spots, groups = edge_layout(planes)
    slabs = Q * planes

    def load_tile(tile, plane, cols):
        return pltpu.make_async_copy(
            pop_ref.at[:, plane, :, cols],
            raw.at[:, plane, tile],
            load_sem.at[1 + tile * planes + plane],
        )

    load_pore = pltpu.make_async_copy(pore_ref, voxels, load_sem.at[0])
    for tile in range(strips):
        for plane in range(planes):
            load_tile(tile, plane, slice(tile * LANES, (tile + 1) * LANES)).start()
        if tile == 0:
            load_pore.start()

    me = lax.axis_index("px")
    here = lax.axis_index("py")
    up = lax.rem(here + along - 1, along)
    down = lax.rem(here + 1, along)
    first_row = here == 0
    last_row = here == along - 1
    odd = lax.rem(here, 2) == 1
    last_strip = last_row & (me == across - 1)
    end = across - 1
    quarter = along // 4
    short = odd & (here < quarter)
    goes_by = odd & (here >= quarter) & (here < 2 * quarter) & (me == 0)

    halves = [(k, plane) for k in range(wt) for plane in range(planes)]

    def loaded(tile, plane):
        load_tile(tile, plane, slice(0, LANES)).wait()

    barrier = pltpu.get_barrier_semaphore()

    def greet(x, y):
        pl.semaphore_signal(barrier, inc=1, device_id=(x, y), device_id_type=MESH)

    def answer(y):
        pl.semaphore_signal(ready, inc=1, device_id=(me, y), device_id_type=MESH)

    for step in range(1, across):
        greet(lax.rem(me + step, across), here)

    @pl.when(odd)
    def _():
        greet(me, up)

        @pl.when(jnp.logical_not(last_row))
        def _():
            greet(me, down)

    @pl.when(short & (me == 0))
    def _():
        greet(0, here + quarter)

    @pl.when(first_row)
    def _():
        greet(me, along - 1)

        @pl.when(me != across - 1)
        def _():
            greet(across - 1, along - 1)

    def enter():
        greeted = jnp.where(odd, 0, 2) - jnp.where(first_row, 1, 0)
        greeted = greeted + jnp.where(last_row, jnp.where(me == across - 1, across, 1), 0)
        greeted = greeted + jnp.where(goes_by, 1, 0)
        pl.semaphore_wait(barrier, across - 1 + greeted)

    def answers():
        @pl.when(goes_by)
        def _():
            pl.semaphore_signal(path, inc=1, device_id=(0, here - quarter), device_id_type=MESH)

        @pl.when(jnp.logical_not(odd))
        def _():
            answer(down)

            @pl.when(here != 0)
            def _():
                answer(up)

        @pl.when(last_row)
        def _():
            answer(0)

    load_pore.wait()

    def collide_strip(tile, plane, own):
        cols = pl.ds(pl.multiple_of(tile * LANES, LANES), LANES)
        fields = [raw[slot, plane, tile] for slot in range(Q)]
        is_open = voxels[plane, :, cols] > 0
        result = collide_tile(fields, is_open, TINY, 0.0)
        for slot in range(Q):
            box[place_of[slot], plane, tile] = result[slot]
            if own is not None:
                at = pl.ds(pl.multiple_of(me * rows, ROWS), rows)
                post[place_of[slot], plane, own, at, :] = result[slot]

    def outer(source):
        return (rows - HALO, rows) if source == across - 1 else (0, HALO)

    def inner(source):
        return (0, HALO) if source == across - 1 else (rows - HALO, rows)

    def middle(source):
        return (HALO, rows - HALO)

    def send(source, target, n, part=None):
        if part:
            k, plane = part
            low, high = outer(source)
            return pltpu.make_async_remote_copy(
                src_ref=box.at[:, plane, target * wt + k, low:high, :],
                dst_ref=post.at[:, plane, k, source * rows + low : source * rows + high, :],
                send_sem=n_send.at[(target - source) % across - 1, (0, 1, 2, 2, 3, 3)[n]],
                recv_sem=n_recv.at[(target - source) % across - 1, (0, 1, 2, 2, 3, 4)[n]],
                device_id=(target, here),
                device_id_type=MESH,
            )
        if n == 1:
            src, dst = packs.at[target], edges.at[:, source * rows : (source + 1) * rows, :]
        else:
            low, high = (outer, None, inner, inner, middle, middle)[n](source)
            first, last = ((0, wt), None, (0, wt - 1), (wt - 1, wt))[n if n < 4 else n - 2]
            src = box.at[:, :, target * wt + first : target * wt + last, low:high, :]
            start = source * rows
            dst = post.at[:, :, first:last, start + low : start + high, :]
        return pltpu.make_async_remote_copy(
            src_ref=src,
            dst_ref=dst,
            send_sem=n_send.at[(target - source) % across - 1, (0, 1, 2, 2, 3, 3)[n]],
            recv_sem=n_recv.at[(target - source) % across - 1, (0, 1, 2, 2, 3, 4)[n]],
            device_id=(target, here),
            device_id_type=MESH,
        )

    pieces = [0, 1, 2, 3, 4, 5] if wt > 1 else [0, 1, 3, 5]

    def relay(way):
        if way == 0:
            near, beyond, part, to = 0, 1, (0, RISE), up
            near_to, beyond_to, low, low_to = ROWS - 2, ROWS - 1, 0, ROWS - HALO
        else:
            near, beyond, part, to = height - 1, height - 2, (FALL, Q), down
            near_to, beyond_to, low, low_to = 1, 0, height - HALO, 0
        some = slice(*part)
        refs = [
            (post.at[:, :, :, near : near + 1, :],
             ring.at[:, :, 0:wt, near_to : near_to + 1, :]),
            (post.at[some, :, :, beyond : beyond + 1, :],
             ring.at[some, :, 0:wt, beyond_to : beyond_to + 1, :]),
            (edges.at[:, low : low + HALO, :], ring_edges.at[:, low_to : low_to + HALO, :]),
        ]
        return [
            pltpu.make_async_remote_copy(
                src_ref=src,
                dst_ref=dst,
                send_sem=h_send.at[way, n // 2],
                recv_sem=h_recv.at[way, n // 2],
                device_id=(me, to),
                device_id_type=MESH,
            )
            for n, (src, dst) in enumerate(refs)
        ]

    def peers(mine):
        return [(mine + step) % across for step in range(1, across)]

    def on_each(action):
        for mine in range(across):
            pl.when(me == mine)(functools.partial(action, mine))

    def begin(wanted):
        def action(mine):
            for n in pieces:
                if n in wanted:
                    for target in peers(mine):
                        send(mine, target, n).start()

        on_each(action)

    def direct(target, which=range(3)):
        cols = slice(target * wt, (target + 1) * wt)
        refs = [
            (box.at[:, :, cols, rows - 1 : rows, :], ring.at[:, :, 0:wt, 1:2, :]),
            (box.at[FALL:Q, :, cols, rows - HALO : rows - 1, :], ring.at[FALL:Q, :, 0:wt, 0:1, :]),
            (packs.at[target, :, rows - HALO : rows, :], ring_edges.at[:, 0:HALO, :]),
        ]
        return [
            pltpu.make_async_remote_copy(
                src_ref=src,
                dst_ref=dst,
                send_sem=w_send.at[n // 2],
                recv_sem=h_recv.at[1, n // 2],
                device_id=(target, 0),
                device_id_type=MESH,
            )
            for n, (src, dst) in enumerate(refs)
            if n in which
        ]

    def send_direct(targets, which):
        @pl.when(last_strip)
        def _():
            for target in targets:
                for copy in direct(target, which):
                    copy.start()


    for step in range(1, across):
        for k, plane in halves:
            tile = lax.rem(me + step, across) * wt + k
            loaded(tile, plane)
            collide_strip(tile, plane, None)
            if step == 1 and (k, plane) == (0, 0):
                enter()

            def begin_outer(mine):
                send(mine, (mine + step) % across, 0, (k, plane)).start()

            on_each(begin_outer)
            if step == 1 and (k, plane) == (0, 0):
                answers()
    send_direct(range(across - 1), (0, 1))
    for k, plane in halves:
        loaded(me * wt + k, plane)
    for k, plane in halves:
        collide_strip(me * wt + k, plane, k)
    send_direct((across - 1,), (0, 1))

    lane = lax.broadcasted_iota(jnp.int32, (rows, LANES), 1)
    for step in range(1, across + 1):
        target = lax.rem(me + step, across)
        first = lax.rem((target + 1) * wt, strips)
        last = lax.rem(target * wt + strips - 1, strips)
        own_at = pl.ds(pl.multiple_of(me * rows, ROWS), rows)
        packed = [None] * groups
        for slab, (group, at, left_of, right_of) in enumerate(spots):
            field, plane = slab // planes, slab % planes
            if slab < slabs:
                edge = jnp.where(lane < LANES // 2, box[field, plane, first], box[field, plane, last])
                if step == across:
                    sides[field, plane, own_at, :] = edge
            else:
                right, left = (place_of[slot] for slot in PAIRS[field - Q])
                tile = target * wt + wt - 1
                edge = jnp.where(lane < LANES // 2, box[left, plane, tile], box[right, plane, tile])
                if step == across:
                    seams[field - Q, plane, own_at, :] = edge
            moved = pltpu.roll(edge, at, 1)
            if packed[group] is not None:
                moved = jnp.where((lane >= at - left_of) & (lane < at + right_of), moved, packed[group])
            packed[group] = moved
        for group in range(groups):
            packs[target, group] = packed[group]
            if step == across:
                edges[group, own_at, :] = packed[group]
        if step == across - 1:
            begin((1,))
            send_direct(range(across - 1), (2,))

            @pl.when(jnp.logical_not(odd))
            def _():
                begin((2, 3, 4, 5))

    send_direct((across - 1,), (2,))

    def both(sem, tiles):
        rows_of = box.at[0 : (Q + RISE) // 2, :, 0:tiles, 0:2, :]
        pltpu.make_async_copy(rows_of, rows_of, sem).wait()

    def some_edges(sem, refs):
        pltpu.make_async_copy(refs, refs, sem).wait()

    def all_of(sem, part, mine):
        low, high = part(mine)
        refs = box.at[:, :, 0:wt, low:high, :]
        pltpu.make_async_copy(refs, refs, sem).wait()


    low, high = inner(end)
    around = pltpu.make_async_remote_copy(
        src_ref=box.at[:, :, wt - 1 : wt, low:high, :],
        dst_ref=via,
        send_sem=n_send.at[(0 - end) % across - 1, 2],
        recv_sem=via_sem.at[0],
        device_id=(0, here + quarter),
        device_id_type=MESH,
    )
    onward = pltpu.make_async_remote_copy(
        src_ref=via,
        dst_ref=post.at[:, :, wt - 1 : wt, end * rows + low : end * rows + high, :],
        send_sem=via_sem.at[1],
        recv_sem=n_recv.at[(0 - end) % across - 1, 2],
        device_id=(0, here - quarter),
        device_id_type=MESH,
    )

    @pl.when(short & (me == 0))
    def _():
        pl.semaphore_wait(path, 1)
        pl.semaphore_signal(path, inc=1, device_id=(end, here), device_id_type=MESH)

    @pl.when(odd)
    def _():
        pl.semaphore_wait(ready, jnp.where(last_row, 1, 2))

    def start_relay(way):
        for copy in relay(way):
            copy.start()

    @pl.when((me == 0) & jnp.logical_not(first_row))
    def _():
        start_relay(0)

    @pl.when((me == end) & jnp.logical_not(last_row))
    def _():
        start_relay(1)

    @pl.when(short & (me == end))
    def _():
        pl.semaphore_wait(path, 1)
        around.start()

    def begin_late(mine):
        for n in pieces:
            for target in peers(mine):
                if n == 3 and (mine, target) == (end, 0):
                    pl.when(jnp.logical_not(short))(send(mine, target, n).start)
                elif n >= 2:
                    send(mine, target, n).start()

    @pl.when(odd)
    def _():
        pl.semaphore_wait(go, 1)
        on_each(begin_late)

    def lead_sent(mine):
        for target in peers(mine):
            all_of(n_send.at[(target - mine) % across - 1, 2], inner, mine)

    @pl.when(jnp.logical_not(odd))
    def _():
        on_each(lead_sent)
        pl.semaphore_signal(go, inc=1, device_id=(me, down), device_id_type=MESH)

    def unpack(packs_of, at, store):
        for slab, (group, lane_at, _, _) in enumerate(spots):
            moved = pltpu.roll(packs_of[group, at, :], LANES - lane_at, 1)
            store(slab // planes, slab % planes, moved)

    def take_outer(source, mine):
        send(source, mine, 0).wait_recv()
        send(source, mine, 1).wait_recv()

    def relays(mine):
        if mine != end:
            take_outer(end, mine)
            pl.when(jnp.logical_not(last_row))(functools.partial(start_relay, 1))
        if mine != 0:
            take_outer(0, mine)
            pl.when(jnp.logical_not(first_row))(functools.partial(start_relay, 0))

        @pl.when(first_row)
        def _():
            pl.semaphore_wait(ready, 1)
            start_relay(0)

        for source in peers(mine):
            if source not in (0, end):
                take_outer(source, mine)

    on_each(relays)

    def settle(n):
        def action(mine):
            for source in peers(mine):
                if n == 2:
                    all_of(n_recv.at[(mine - source) % across - 1, 2], inner, source)
                elif n + 1 in pieces:
                    send(source, mine, n + 1).wait_recv()

        on_each(action)

    every = list(range(wt + 1))
    before = [tile for tile in every if tile != wt - 1]

    def advance(load, store, tiles, seam=None):
        for tile in tiles:
            for plane in range(planes):
                is_open = load(0, plane, tile, 0) != 0.0
                fields = [stream(load, (wt + 1, planes), slot, plane, tile, 0.0, seam) for slot in range(Q)]
                result = collide_tile(fields, is_open, None, SOLID)
                for slot in range(Q):
                    store(slot, plane, tile, result[slot])

    def window(source, tiles):
        start = jnp.minimum(rows * source + 1, height - 1 - ROWS)

        def load(slot, plane, tile, dy):
            at = pl.ds(start - dy, ROWS)
            if tile == wt:
                return sides[place_of[slot], plane, at, :]
            return post[place_of[slot], plane, tile, at, :]

        def store(slot, plane, tile, value):
            post2[place_of[slot], plane, tile, pl.ds(ROWS + start, ROWS), :] = value

        def seam(slot, plane, tile, dy):
            if tile != wt - 1:
                return load(slot, plane, tile, dy)
            pair = [slot in both for both in PAIRS].index(True)
            return seams[pair, plane, pl.ds(start - dy, ROWS), :]

        advance(load, store, tiles, seam)

    row = lax.broadcasted_iota(jnp.int32, (ROWS, LANES), 0)
    half = ROWS // 2

    def fill():
        for slot in range(Q):
            for plane in range(planes):
                for tile in range(wt):
                    ring[slot, plane, tile, HALO:half, :] = post[slot, plane, tile, 0:HALO, :]
                    ring[slot, plane, tile, half : half + HALO, :] = post[
                        slot, plane, tile, height - HALO : height, :
                    ]
        for group in range(groups):
            ring_edges[group, HALO:half, :] = edges[group, 0:HALO, :]
            ring_edges[group, half : half + HALO, :] = edges[group, height - HALO : height, :]

    def rim():
        top, low = ROWS - HALO, height + HALO

        def load(slot, plane, tile, dy):
            value = ring[place_of[slot], plane, tile]
            return pltpu.roll(value, dy % ROWS, 0) if dy else value

        def store(slot, plane, tile, value):
            place = place_of[slot]
            pltpu.store(
                post2.at[place, plane, tile, top : top + ROWS, :], value,
                mask=(row >= 1) & (row < 3),
            )
            pltpu.store(
                post2.at[place, plane, tile, low : low + ROWS, :], value,
                mask=(row >= half + 1) & (row < half + 3),
            )

        advance(load, store, every)

    def unpack_from(step, carry):
        at = pl.ds(pl.multiple_of(lax.rem(me + step, across) * rows, ROWS), rows)

        def store(slot, plane, value):
            if slot < Q:
                sides[slot, plane, at, :] = value
            else:
                seams[slot - Q, plane, at, :] = value

        unpack(edges, at, store)
        return carry

    def unpack_ring():
        def store(slot, plane, value):
            if slot < Q:
                ring[slot, plane, wt] = value

        unpack(ring_edges, pl.ds(0, ROWS), store)

    lax.fori_loop(1, across, unpack_from, 0)
    fill()
    def windows(tiles):
        def window_from(step, carry):
            window(lax.rem(me + step, across), tiles)
            return carry

        lax.fori_loop(1, across, window_from, 0)

    @pl.when(goes_by)
    def _():
        around.wait_recv()
        onward.start()

    def halo():
        for way in range(2):
            both(h_recv.at[way, 0], wt)
            some_edges(h_recv.at[way, 1], ring_edges.at[:, 0:HALO, :])
        unpack_ring()
        rim()

    def own_flow():
        for plane in range(planes):
            for tile in range(wt):
                def store(slot, value):
                    done[slot, plane, :, tile * LANES : (tile + 1) * LANES] = value

                flow_tile(post2, pl.multiple_of(me * rows, ROWS), plane, tile, wt + 1, store)

    def own_window():
        settle(2)
        window(me, every)

    def first_windows():
        settle(3)
        windows(before)

    def last_windows():
        settle(4)
        windows([wt - 1])

    def sent(mine):
        for target in peers(mine):
            send(mine, target, 0).wait_send()
            send(mine, target, 1).wait_send()
            sem = (target - mine) % across - 1
            pl.when(odd)(functools.partial(all_of, n_send.at[sem, 2], inner, mine))
            all_of(n_send.at[sem, 3], middle, mine)

    def all_sent():
        pl.when(goes_by)(onward.wait_send)
        on_each(sent)
        both(h_send.at[0, 0], wt)
        some_edges(h_send.at[0, 1], ring_edges.at[:, 0:HALO, :])

        @pl.when(jnp.logical_not(last_row))
        def _():
            both(h_send.at[1, 0], wt)
            some_edges(h_send.at[1, 1], ring_edges.at[:, 0:HALO, :])

        @pl.when(last_strip)
        def _():
            both(w_send.at[0], strips)
            some_edges(w_send.at[1], packs.at[:, :, 0:HALO, :])

    @pl.when(odd)
    def _():
        halo()
        own_window()
        if across == 2:
            own_flow()
        first_windows()
        all_sent()
        last_windows()
        if across != 2:
            own_flow()

    @pl.when(jnp.logical_not(odd))
    def _():
        own_window()
        first_windows()
        last_windows()
        all_sent()
        halo()
        own_flow()


def flow_tile(post, start, plane, tile, tiles, store):
    planes = post.shape[1]

    def load(slot, plane, tile, dy):
        return post[place_of[slot], plane, tile, pl.ds(ROWS + start - dy, ROWS), :]

    is_open = load(0, plane, tile, 0) != SOLID
    for slot in range(Q):
        value = stream(load, (tiles, planes), slot, plane, tile, SOLID)
        store(slot, jnp.where(is_open, value, 0.0))


def finish(across, post, done, out_ref, flow, sems):
    _, planes, rows, width = done.shape
    wt = width // LANES
    me = lax.axis_index("px")

    def own_copy():
        at = pl.ds(pl.multiple_of(me * rows, ROWS), rows)
        return pltpu.make_async_copy(done, out_ref.at[:, :, at, :], sems.at[0])

    def copy_of(step, plane):
        at = pl.ds(pl.multiple_of(lax.rem(me + step, across) * rows, ROWS), rows)
        return pltpu.make_async_copy(
            flow.at[step - 1, :, plane], out_ref.at[:, plane, at, :], sems.at[1 + (step - 1) * planes + plane]
        )

    own_copy().start()

    def write(step, carry):
        for plane in range(planes):
            for tile in range(wt):
                def store(slot, value):
                    flow[step - 1, slot, plane, :, tile * LANES : (tile + 1) * LANES] = value

                start = pl.multiple_of(lax.rem(me + step, across) * rows, ROWS)
                flow_tile(post, start, plane, tile, wt + 1, store)
            copy_of(step, plane).start()
        return carry

    lax.fori_loop(1, across, write, 0)
    own_copy().wait()

    def written(step, carry):
        for plane in range(planes):
            copy_of(step, plane).wait()
        return carry

    lax.fori_loop(1, across, written, 0)


def body(across, along, populations, pore):
    count, planes, rows, columns = populations.shape
    height = across * rows
    width = columns // across
    strips = columns // LANES
    wt = strips // across
    groups = edge_layout(planes)[1]
    tall = height + 2 * ROWS
    post2, done = pl.pallas_call(
        functools.partial(kernel, across, along),
        out_shape=(
            pltpu.VMEM((count, planes, wt + 1, tall, LANES), jnp.float32),
            pltpu.VMEM((count, planes, rows, width), jnp.float32),
        ),
        in_specs=[pl.BlockSpec(memory_space=pltpu.HBM)] * 2,
        out_specs=[pl.BlockSpec(memory_space=pltpu.VMEM)] * 2,
        scratch_shapes=[
            pltpu.VMEM((count, planes, strips, rows, LANES), jnp.float32),
            pltpu.VMEM((planes, rows, columns), jnp.int32),
            pltpu.VMEM((count, planes, strips, rows, LANES), jnp.float32),
            pltpu.VMEM((count, planes, wt, height, LANES), jnp.float32),
            pltpu.VMEM((count, planes, height, LANES), jnp.float32),
            pltpu.VMEM((len(PAIRS), planes, height, LANES), jnp.float32),
            pltpu.VMEM((count, planes, wt + 1, ROWS, LANES), jnp.float32),
            pltpu.VMEM((across, groups, rows, LANES), jnp.float32),
            pltpu.VMEM((groups, height, LANES), jnp.float32),
            pltpu.VMEM((groups, ROWS, LANES), jnp.float32),
            pltpu.VMEM((count, planes, 1, HALO, LANES), jnp.float32),
            pltpu.SemaphoreType.DMA((1 + strips * planes,)),
            pltpu.SemaphoreType.DMA((across - 1, 4)),
            pltpu.SemaphoreType.DMA((across - 1, 5)),
            pltpu.SemaphoreType.DMA((2, 2)),
            pltpu.SemaphoreType.DMA((2, 2)),
            pltpu.SemaphoreType.DMA((2,)),
            pltpu.SemaphoreType.DMA((2,)),
            pltpu.SemaphoreType.REGULAR,
            pltpu.SemaphoreType.REGULAR,
            pltpu.SemaphoreType.REGULAR,
        ],
        compiler_params=pltpu.CompilerParams(
            collective_id=0, has_side_effects=True, vmem_limit_bytes=VMEM_LIMIT
        ),
    )(*(pltpu.with_memory_space_constraint(x, pltpu.HBM) for x in (populations, pore)))
    return pl.pallas_call(
        functools.partial(finish, across),
        out_shape=jax.ShapeDtypeStruct((count, planes, height, width), jnp.float32),
        in_specs=[pl.BlockSpec(memory_space=pltpu.VMEM)] * 2,
        out_specs=pl.BlockSpec(memory_space=pl.ANY),
        scratch_shapes=[
            pltpu.VMEM((across - 1, count, planes, rows, width), jnp.float32),
            pltpu.SemaphoreType.DMA((1 + (across - 1) * planes,)),
        ],
        compiler_params=pltpu.CompilerParams(vmem_limit_bytes=VMEM_LIMIT),
    )(post2, done)


def solution(mesh):
    return jax.shard_map(
        functools.partial(body, mesh.shape["px"], mesh.shape["py"]),
        mesh=mesh,
        in_specs=(P(None, None, ("py", "px"), None), P(None, ("py", "px"), None)),
        out_specs=P(None, None, "py", "px"),
        check_vma=False,
    )
```

```python
import functools

import jax
import jax.numpy as jnp
from jax import lax
from jax.experimental import pallas as pl
from jax.experimental.pallas import tpu as pltpu
from jax.sharding import PartitionSpec as P

MESH = pl.DeviceIdType.MESH

lattice_velocity = [
    (0, 0, 0),
    (1, 0, 0),
    (-1, 0, 0),
    (0, 1, 0),
    (0, -1, 0),
    (0, 0, 1),
    (0, 0, -1),
    (1, 1, 0),
    (-1, -1, 0),
    (1, -1, 0),
    (-1, 1, 0),
    (1, 0, 1),
    (-1, 0, -1),
    (1, 0, -1),
    (-1, 0, 1),
    (0, 1, 1),
    (0, -1, -1),
    (0, 1, -1),
    (0, -1, 1),
]
lattice_weights = [1.0 / 3.0] + [1.0 / 18.0] * 6 + [1.0 / 36.0] * 12
opposite = [0, 2, 1, 4, 3, 6, 5, 8, 7, 10, 9, 12, 11, 14, 13, 16, 15, 18, 17]
relax_time = 0.8
body_force = 0.005

Q = len(lattice_velocity)
LANES = 128
ROWS = 8
HALO = 2
VMEM_LIMIT = 32 * 1024 * 1024
SOLID = -3.0e38
TINY = 1.0e-30

order = sorted(range(Q), key=lambda slot: lattice_velocity[slot][1])
place_of = [order.index(slot) for slot in range(Q)]
RISE = sum(1 for vector in lattice_velocity if vector[1] < 0)
FALL = Q - sum(1 for vector in lattice_velocity if vector[1] > 0)
PAIRS = [(s, opposite[s]) for s in range(Q) if lattice_velocity[s][0] > 0]


def edge_layout(planes):
    spots, group, at = [], 0, 0
    for field in range(Q + len(PAIRS)):
        dx = lattice_velocity[order[field]][0] if field < Q else 0
        left, right = 1 + (dx > 0), 1 + (dx < 0)
        for _ in range(planes):
            if at + left + right > LANES:
                group, at = group + 1, 0
            spots.append((group, at + left, left, right))
            at += left + right
    return spots, group + 1


def total(values):
    while len(values) > 1:
        pairs = [x + y for x, y in zip(values[::2], values[1::2])]
        values = pairs + values[2 * len(pairs) :]
    return values[0]


def collide_tile(fields, is_open, guard, closed):
    keep = 1.0 - 1.0 / relax_time
    gain = 1.0 / relax_time
    density = jnp.where(is_open, total(fields), 1.0)
    inverse = 1.0 / density
    vel = []
    for column in range(3):
        plus = [fields[s] for s in range(Q) if lattice_velocity[s][column] > 0]
        minus = [fields[s] for s in range(Q) if lattice_velocity[s][column] < 0]
        vel.append((total(plus) - total(minus)) * inverse)
    vel[2] = vel[2] + relax_time * body_force
    speed = vel[0] * vel[0] + vel[1] * vel[1] + vel[2] * vel[2]
    base = 1.0 - 1.5 * speed
    result = [None] * Q
    scaled = {w: density * (gain * w) for w in sorted(set(lattice_weights))}

    def close(value):
        return jnp.where(is_open, value + guard if guard else value, closed)

    result[0] = close(keep * fields[0] + scaled[lattice_weights[0]] * base)
    for slot in range(1, Q, 2):
        other = opposite[slot]
        along = None
        for column in range(3):
            sign = lattice_velocity[slot][column]
            if sign == 0:
                continue
            term = vel[column]
            if along is None:
                along = term if sign > 0 else -term
            else:
                along = along + term if sign > 0 else along - term
        weight = scaled[lattice_weights[slot]]
        triple = 3.0 * along
        even = weight * (base + 0.5 * triple * triple)
        odd = weight * triple
        result[slot] = close(keep * fields[slot] + (even + odd))
        result[other] = close(keep * fields[other] + (even - odd))
    return result


def stream(load, sides, slot, plane, tile, closed, seam=None):
    tiles, planes = sides
    dx, dy, dz = lattice_velocity[slot]
    source = (plane - dz) % planes
    value = load(slot, source, tile, dy)
    if dx:
        lane = lax.broadcasted_iota(jnp.int32, value.shape, 1)
        beside = (seam or load)(slot, source, (tile - dx) % tiles, dy)
        value = jnp.where(lane == (LANES - 1 if dx > 0 else 0), beside, value)
        value = pltpu.roll(value, dx % LANES, 1)
    if slot:
        value = jnp.where(value != closed, value, load(opposite[slot], plane, tile, 0))
    return value


def kernel(
    across, along, pop_ref, pore_ref, post2, done,
    raw, voxels, box, post, sides, seams, ring, packs, edges, ring_edges, via,
    load_sem, n_send, n_recv, h_send, h_recv, via_sem, go, ready, path,
):
    _, planes, strips, rows, _ = box.shape
    wt = strips // across
    height = across * rows
    spots, groups = edge_layout(planes)
    slabs = Q * planes

    def load_tile(tile, plane, cols):
        return pltpu.make_async_copy(
            pop_ref.at[:, plane, :, cols],
            raw.at[:, plane, tile],
            load_sem.at[1 + tile * planes + plane],
        )

    load_pore = pltpu.make_async_copy(pore_ref, voxels, load_sem.at[0])
    for tile in range(strips):
        for plane in range(planes):
            load_tile(tile, plane, slice(tile * LANES, (tile + 1) * LANES)).start()
        if tile == 0:
            load_pore.start()

    me = lax.axis_index("px")
    here = lax.axis_index("py")
    up = lax.rem(here + along - 1, along)
    down = lax.rem(here + 1, along)
    first_row = here == 0
    last_row = here == along - 1
    odd = lax.rem(here, 2) == 1
    last_strip = last_row & (me == across - 1)
    end = across - 1
    quarter = along // 4
    short = odd & (here < quarter)
    goes_by = odd & (here >= quarter) & (here < 2 * quarter) & (me == 0)

    halves = [(k, plane) for k in range(wt) for plane in range(planes)]

    def loaded(tile, plane):
        load_tile(tile, plane, slice(0, LANES)).wait()

    barrier = pltpu.get_barrier_semaphore()

    def greet(x, y):
        pl.semaphore_signal(barrier, inc=1, device_id=(x, y), device_id_type=MESH)

    def answer(y):
        pl.semaphore_signal(ready, inc=1, device_id=(me, y), device_id_type=MESH)

    for step in range(1, across):
        greet(lax.rem(me + step, across), here)

    @pl.when(odd)
    def _():
        greet(me, up)

        @pl.when(jnp.logical_not(last_row))
        def _():
            greet(me, down)

    @pl.when(short & (me == 0))
    def _():
        greet(0, here + quarter)

    @pl.when(first_row)
    def _():
        greet(me, along - 1)

        @pl.when(me != across - 1)
        def _():
            greet(across - 1, along - 1)

    def enter():
        greeted = jnp.where(odd, 0, 2) - jnp.where(first_row, 1, 0)
        greeted = greeted + jnp.where(last_row, jnp.where(me == across - 1, across, 1), 0)
        greeted = greeted + jnp.where(goes_by, 1, 0)
        pl.semaphore_wait(barrier, across - 1 + greeted)

    def answers():
        @pl.when(goes_by)
        def _():
            pl.semaphore_signal(path, inc=1, device_id=(0, here - quarter), device_id_type=MESH)

        @pl.when(jnp.logical_not(odd))
        def _():
            answer(down)

            @pl.when(here != 0)
            def _():
                answer(up)

        @pl.when(last_row)
        def _():
            answer(0)

    load_pore.wait()

    def collide_strip(tile, plane, own):
        cols = pl.ds(pl.multiple_of(tile * LANES, LANES), LANES)
        fields = [raw[slot, plane, tile] for slot in range(Q)]
        is_open = voxels[plane, :, cols] > 0
        result = collide_tile(fields, is_open, TINY, 0.0)
        for slot in range(Q):
            box[place_of[slot], plane, tile] = result[slot]
            if own is not None:
                at = pl.ds(pl.multiple_of(me * rows, ROWS), rows)
                post[place_of[slot], plane, own, at, :] = result[slot]

    def outer(source):
        return (rows - HALO, rows) if source == across - 1 else (0, HALO)

    def inner(source):
        return (0, HALO) if source == across - 1 else (rows - HALO, rows)

    def middle(source):
        return (HALO, rows - HALO)

    def send(source, target, n, part=None):
        if part:
            k, plane = part
            low, high = outer(source)
            return pltpu.make_async_remote_copy(
                src_ref=box.at[:, plane, target * wt + k, low:high, :],
                dst_ref=post.at[:, plane, k, source * rows + low : source * rows + high, :],
                send_sem=n_send.at[(target - source) % across - 1, (0, 1, 2, 2, 3, 3)[n]],
                recv_sem=n_recv.at[(target - source) % across - 1, (0, 1, 2, 2, 3, 4)[n]],
                device_id=(target, here),
                device_id_type=MESH,
            )
        if n == 1:
            src, dst = packs.at[target], edges.at[:, source * rows : (source + 1) * rows, :]
        else:
            low, high = (outer, None, inner, inner, middle, middle)[n](source)
            first, last = ((0, wt), None, (0, wt - 1), (wt - 1, wt))[n if n < 4 else n - 2]
            src = box.at[:, :, target * wt + first : target * wt + last, low:high, :]
            start = source * rows
            dst = post.at[:, :, first:last, start + low : start + high, :]
        return pltpu.make_async_remote_copy(
            src_ref=src,
            dst_ref=dst,
            send_sem=n_send.at[(target - source) % across - 1, (0, 1, 2, 2, 3, 3)[n]],
            recv_sem=n_recv.at[(target - source) % across - 1, (0, 1, 2, 2, 3, 4)[n]],
            device_id=(target, here),
            device_id_type=MESH,
        )

    pieces = [0, 1, 2, 3, 4, 5] if wt > 1 else [0, 1, 3, 5]

    def relay(way):
        if way == 0:
            near, beyond, part, to = 0, 1, (0, RISE), up
            near_to, beyond_to, low, low_to = ROWS - 2, ROWS - 1, 0, ROWS - HALO
        else:
            near, beyond, part, to = height - 1, height - 2, (FALL, Q), down
            near_to, beyond_to, low, low_to = 1, 0, height - HALO, 0
        some = slice(*part)
        refs = [
            (post.at[:, :, :, near : near + 1, :],
             ring.at[:, :, 0:wt, near_to : near_to + 1, :]),
            (post.at[some, :, :, beyond : beyond + 1, :],
             ring.at[some, :, 0:wt, beyond_to : beyond_to + 1, :]),
            (edges.at[:, low : low + HALO, :], ring_edges.at[:, low_to : low_to + HALO, :]),
        ]
        return [
            pltpu.make_async_remote_copy(
                src_ref=src,
                dst_ref=dst,
                send_sem=h_send.at[way, n // 2],
                recv_sem=h_recv.at[way, n // 2],
                device_id=(me, to),
                device_id_type=MESH,
            )
            for n, (src, dst) in enumerate(refs)
        ]

    def peers(mine):
        return [(mine + step) % across for step in range(1, across)]

    def on_each(action):
        for mine in range(across):
            pl.when(me == mine)(functools.partial(action, mine))

    def begin(wanted):
        def action(mine):
            for n in pieces:
                if n in wanted:
                    for target in peers(mine):
                        send(mine, target, n).start()

        on_each(action)

    def direct(target, which=range(3)):
        cols = slice(target * wt, (target + 1) * wt)
        refs = [
            (box.at[:, :, cols, rows - 1 : rows, :], ring.at[:, :, 0:wt, 1:2, :]),
            (box.at[FALL:Q, :, cols, rows - HALO : rows - 1, :], ring.at[FALL:Q, :, 0:wt, 0:1, :]),
            (packs.at[target, :, rows - HALO : rows, :], ring_edges.at[:, 0:HALO, :]),
        ]
        return [
            pltpu.make_async_remote_copy(
                src_ref=src,
                dst_ref=dst,
                send_sem=h_send.at[1, n // 2],
                recv_sem=h_recv.at[1, n // 2],
                device_id=(target, 0),
                device_id_type=MESH,
            )
            for n, (src, dst) in enumerate(refs)
            if n in which
        ]

    def send_direct(targets, which):
        @pl.when(last_strip)
        def _():
            for target in targets:
                for copy in direct(target, which):
                    copy.start()


    for step in range(1, across):
        for k, plane in halves:
            tile = lax.rem(me + step, across) * wt + k
            loaded(tile, plane)
            collide_strip(tile, plane, None)
            if step == 1 and (k, plane) == (0, 0):
                enter()

            def begin_outer(mine):
                send(mine, (mine + step) % across, 0, (k, plane)).start()

            on_each(begin_outer)
            if step == 1 and (k, plane) == (0, 0):
                answers()
    send_direct(range(across - 1), (0, 1))
    for k, plane in halves:
        loaded(me * wt + k, plane)
    for k, plane in halves:
        collide_strip(me * wt + k, plane, k)
    send_direct((across - 1,), (0, 1))

    lane = lax.broadcasted_iota(jnp.int32, (rows, LANES), 1)
    for step in range(1, across + 1):
        target = lax.rem(me + step, across)
        first = lax.rem((target + 1) * wt, strips)
        last = lax.rem(target * wt + strips - 1, strips)
        own_at = pl.ds(pl.multiple_of(me * rows, ROWS), rows)
        packed = [None] * groups
        for slab, (group, at, left_of, right_of) in enumerate(spots):
            field, plane = slab // planes, slab % planes
            if slab < slabs:
                edge = jnp.where(lane < LANES // 2, box[field, plane, first], box[field, plane, last])
                if step == across:
                    sides[field, plane, own_at, :] = edge
            else:
                right, left = (place_of[slot] for slot in PAIRS[field - Q])
                tile = target * wt + wt - 1
                edge = jnp.where(lane < LANES // 2, box[left, plane, tile], box[right, plane, tile])
                if step == across:
                    seams[field - Q, plane, own_at, :] = edge
            moved = pltpu.roll(edge, at, 1)
            if packed[group] is not None:
                moved = jnp.where((lane >= at - left_of) & (lane < at + right_of), moved, packed[group])
            packed[group] = moved
        for group in range(groups):
            packs[target, group] = packed[group]
            if step == across:
                edges[group, own_at, :] = packed[group]
        if step == across - 1:
            begin((1,))
            send_direct(range(across - 1), (2,))

            @pl.when(jnp.logical_not(odd))
            def _():
                begin((2, 3, 4, 5))

    send_direct((across - 1,), (2,))

    def both(sem, tiles):
        rows_of = box.at[0 : (Q + RISE) // 2, :, 0:tiles, 0:2, :]
        pltpu.make_async_copy(rows_of, rows_of, sem).wait()

    def some_edges(sem, refs):
        pltpu.make_async_copy(refs, refs, sem).wait()

    def all_of(sem, part, mine):
        low, high = part(mine)
        refs = box.at[:, :, 0:wt, low:high, :]
        pltpu.make_async_copy(refs, refs, sem).wait()


    low, high = inner(end)
    around = pltpu.make_async_remote_copy(
        src_ref=box.at[:, :, wt - 1 : wt, low:high, :],
        dst_ref=via,
        send_sem=n_send.at[(0 - end) % across - 1, 2],
        recv_sem=via_sem.at[0],
        device_id=(0, here + quarter),
        device_id_type=MESH,
    )
    onward = pltpu.make_async_remote_copy(
        src_ref=via,
        dst_ref=post.at[:, :, wt - 1 : wt, end * rows + low : end * rows + high, :],
        send_sem=via_sem.at[1],
        recv_sem=n_recv.at[(0 - end) % across - 1, 2],
        device_id=(0, here - quarter),
        device_id_type=MESH,
    )

    @pl.when(short & (me == 0))
    def _():
        pl.semaphore_wait(path, 1)
        pl.semaphore_signal(path, inc=1, device_id=(end, here), device_id_type=MESH)

    @pl.when(odd)
    def _():
        pl.semaphore_wait(ready, jnp.where(last_row, 1, 2))

    def start_relay(way):
        for copy in relay(way):
            copy.start()

    @pl.when((me == 0) & jnp.logical_not(first_row))
    def _():
        start_relay(0)

    @pl.when((me == end) & jnp.logical_not(last_row))
    def _():
        start_relay(1)

    @pl.when(short & (me == end))
    def _():
        pl.semaphore_wait(path, 1)
        around.start()

    def begin_late(mine):
        for n in pieces:
            for target in peers(mine):
                if n == 3 and (mine, target) == (end, 0):
                    pl.when(jnp.logical_not(short))(send(mine, target, n).start)
                elif n >= 2:
                    send(mine, target, n).start()

    @pl.when(odd)
    def _():
        pl.semaphore_wait(go, 1)
        on_each(begin_late)

    def lead_sent(mine):
        for target in peers(mine):
            all_of(n_send.at[(target - mine) % across - 1, 2], inner, mine)

    @pl.when(jnp.logical_not(odd))
    def _():
        on_each(lead_sent)
        pl.semaphore_signal(go, inc=1, device_id=(me, down), device_id_type=MESH)

    def unpack(packs_of, at, store):
        for slab, (group, lane_at, _, _) in enumerate(spots):
            moved = pltpu.roll(packs_of[group, at, :], LANES - lane_at, 1)
            store(slab // planes, slab % planes, moved)

    def take_outer(source, mine):
        send(source, mine, 0).wait_recv()
        send(source, mine, 1).wait_recv()

    def relays(mine):
        if mine != end:
            take_outer(end, mine)
            pl.when(jnp.logical_not(last_row))(functools.partial(start_relay, 1))
        if mine != 0:
            take_outer(0, mine)
            pl.when(jnp.logical_not(first_row))(functools.partial(start_relay, 0))

        @pl.when(first_row)
        def _():
            pl.semaphore_wait(ready, 1)
            start_relay(0)

        for source in peers(mine):
            if source not in (0, end):
                take_outer(source, mine)

    on_each(relays)

    def settle(n):
        def action(mine):
            for source in peers(mine):
                if n == 2:
                    all_of(n_recv.at[(mine - source) % across - 1, 2], inner, source)
                elif n + 1 in pieces:
                    send(source, mine, n + 1).wait_recv()

        on_each(action)

    every = list(range(wt + 1))
    before = [tile for tile in every if tile != wt - 1]

    def advance(load, store, tiles, seam=None):
        for tile in tiles:
            for plane in range(planes):
                is_open = load(0, plane, tile, 0) != 0.0
                fields = [stream(load, (wt + 1, planes), slot, plane, tile, 0.0, seam) for slot in range(Q)]
                result = collide_tile(fields, is_open, None, SOLID)
                for slot in range(Q):
                    store(slot, plane, tile, result[slot])

    def window(source, tiles):
        start = jnp.minimum(rows * source + 1, height - 1 - ROWS)

        def load(slot, plane, tile, dy):
            at = pl.ds(start - dy, ROWS)
            if tile == wt:
                return sides[place_of[slot], plane, at, :]
            return post[place_of[slot], plane, tile, at, :]

        def store(slot, plane, tile, value):
            post2[place_of[slot], plane, tile, pl.ds(ROWS + start, ROWS), :] = value

        def seam(slot, plane, tile, dy):
            if tile != wt - 1:
                return load(slot, plane, tile, dy)
            pair = [slot in both for both in PAIRS].index(True)
            return seams[pair, plane, pl.ds(start - dy, ROWS), :]

        advance(load, store, tiles, seam)

    row = lax.broadcasted_iota(jnp.int32, (ROWS, LANES), 0)
    half = ROWS // 2

    def fill():
        for slot in range(Q):
            for plane in range(planes):
                for tile in range(wt):
                    ring[slot, plane, tile, HALO:half, :] = post[slot, plane, tile, 0:HALO, :]
                    ring[slot, plane, tile, half : half + HALO, :] = post[
                        slot, plane, tile, height - HALO : height, :
                    ]
        for group in range(groups):
            ring_edges[group, HALO:half, :] = edges[group, 0:HALO, :]
            ring_edges[group, half : half + HALO, :] = edges[group, height - HALO : height, :]

    def rim():
        top, low = ROWS - HALO, height + HALO

        def load(slot, plane, tile, dy):
            value = ring[place_of[slot], plane, tile]
            return pltpu.roll(value, dy % ROWS, 0) if dy else value

        def store(slot, plane, tile, value):
            place = place_of[slot]
            pltpu.store(
                post2.at[place, plane, tile, top : top + ROWS, :], value,
                mask=(row >= 1) & (row < 3),
            )
            pltpu.store(
                post2.at[place, plane, tile, low : low + ROWS, :], value,
                mask=(row >= half + 1) & (row < half + 3),
            )

        advance(load, store, every)

    def unpack_from(step, carry):
        at = pl.ds(pl.multiple_of(lax.rem(me + step, across) * rows, ROWS), rows)

        def store(slot, plane, value):
            if slot < Q:
                sides[slot, plane, at, :] = value
            else:
                seams[slot - Q, plane, at, :] = value

        unpack(edges, at, store)
        return carry

    def unpack_ring():
        def store(slot, plane, value):
            if slot < Q:
                ring[slot, plane, wt] = value

        unpack(ring_edges, pl.ds(0, ROWS), store)

    lax.fori_loop(1, across, unpack_from, 0)
    fill()
    def windows(tiles):
        def window_from(step, carry):
            window(lax.rem(me + step, across), tiles)
            return carry

        lax.fori_loop(1, across, window_from, 0)

    @pl.when(goes_by)
    def _():
        around.wait_recv()
        onward.start()

    def halo():
        for way in range(2):
            both(h_recv.at[way, 0], wt)
            some_edges(h_recv.at[way, 1], ring_edges.at[:, 0:HALO, :])
        unpack_ring()
        rim()

    def own_flow():
        for plane in range(planes):
            for tile in range(wt):
                def store(slot, value):
                    done[slot, plane, :, tile * LANES : (tile + 1) * LANES] = value

                flow_tile(post2, pl.multiple_of(me * rows, ROWS), plane, tile, wt + 1, store)

    def own_window():
        settle(2)
        window(me, every)

    def first_windows():
        settle(3)
        windows(before)

    def last_windows():
        settle(4)
        windows([wt - 1])

    def sent(mine):
        for target in peers(mine):
            send(mine, target, 0).wait_send()
            send(mine, target, 1).wait_send()
            sem = (target - mine) % across - 1
            pl.when(odd)(functools.partial(all_of, n_send.at[sem, 2], inner, mine))
            all_of(n_send.at[sem, 3], middle, mine)

    def all_sent():
        pl.when(goes_by)(onward.wait_send)
        on_each(sent)
        both(h_send.at[0, 0], wt)
        some_edges(h_send.at[0, 1], ring_edges.at[:, 0:HALO, :])

        @pl.when(jnp.logical_not(last_row))
        def _():
            both(h_send.at[1, 0], wt)
            some_edges(h_send.at[1, 1], ring_edges.at[:, 0:HALO, :])

        @pl.when(last_strip)
        def _():
            both(h_send.at[1, 0], strips)
            some_edges(h_send.at[1, 1], packs.at[:, :, 0:HALO, :])

    @pl.when(odd)
    def _():
        halo()
        own_window()
        if across == 2:
            own_flow()
        first_windows()
        all_sent()
        last_windows()
        if across != 2:
            own_flow()

    @pl.when(jnp.logical_not(odd))
    def _():
        own_window()
        first_windows()
        last_windows()
        all_sent()
        halo()
        own_flow()


def flow_tile(post, start, plane, tile, tiles, store):
    planes = post.shape[1]

    def load(slot, plane, tile, dy):
        return post[place_of[slot], plane, tile, pl.ds(ROWS + start - dy, ROWS), :]

    is_open = load(0, plane, tile, 0) != SOLID
    for slot in range(Q):
        value = stream(load, (tiles, planes), slot, plane, tile, SOLID)
        store(slot, jnp.where(is_open, value, 0.0))


def finish(across, post, done, out_ref, flow, sems):
    _, planes, rows, width = done.shape
    wt = width // LANES
    me = lax.axis_index("px")

    def own_copy():
        at = pl.ds(pl.multiple_of(me * rows, ROWS), rows)
        return pltpu.make_async_copy(done, out_ref.at[:, :, at, :], sems.at[0])

    def copy_of(step, plane):
        at = pl.ds(pl.multiple_of(lax.rem(me + step, across) * rows, ROWS), rows)
        return pltpu.make_async_copy(
            flow.at[step - 1, :, plane], out_ref.at[:, plane, at, :], sems.at[1 + (step - 1) * planes + plane]
        )

    own_copy().start()

    def write(step, carry):
        for plane in range(planes):
            for tile in range(wt):
                def store(slot, value):
                    flow[step - 1, slot, plane, :, tile * LANES : (tile + 1) * LANES] = value

                start = pl.multiple_of(lax.rem(me + step, across) * rows, ROWS)
                flow_tile(post, start, plane, tile, wt + 1, store)
            copy_of(step, plane).start()
        return carry

    lax.fori_loop(1, across, write, 0)
    own_copy().wait()

    def written(step, carry):
        for plane in range(planes):
            copy_of(step, plane).wait()
        return carry

    lax.fori_loop(1, across, written, 0)


def body(across, along, populations, pore):
    count, planes, rows, columns = populations.shape
    height = across * rows
    width = columns // across
    strips = columns // LANES
    wt = strips // across
    groups = edge_layout(planes)[1]
    tall = height + 2 * ROWS
    post2, done = pl.pallas_call(
        functools.partial(kernel, across, along),
        out_shape=(
            pltpu.VMEM((count, planes, wt + 1, tall, LANES), jnp.float32),
            pltpu.VMEM((count, planes, rows, width), jnp.float32),
        ),
        in_specs=[pl.BlockSpec(memory_space=pltpu.HBM)] * 2,
        out_specs=[pl.BlockSpec(memory_space=pltpu.VMEM)] * 2,
        scratch_shapes=[
            pltpu.VMEM((count, planes, strips, rows, LANES), jnp.float32),
            pltpu.VMEM((planes, rows, columns), jnp.int32),
            pltpu.VMEM((count, planes, strips, rows, LANES), jnp.float32),
            pltpu.VMEM((count, planes, wt, height, LANES), jnp.float32),
            pltpu.VMEM((count, planes, height, LANES), jnp.float32),
            pltpu.VMEM((len(PAIRS), planes, height, LANES), jnp.float32),
            pltpu.VMEM((count, planes, wt + 1, ROWS, LANES), jnp.float32),
            pltpu.VMEM((across, groups, rows, LANES), jnp.float32),
            pltpu.VMEM((groups, height, LANES), jnp.float32),
            pltpu.VMEM((groups, ROWS, LANES), jnp.float32),
            pltpu.VMEM((count, planes, 1, HALO, LANES), jnp.float32),
            pltpu.SemaphoreType.DMA((1 + strips * planes,)),
            pltpu.SemaphoreType.DMA((across - 1, 4)),
            pltpu.SemaphoreType.DMA((across - 1, 5)),
            pltpu.SemaphoreType.DMA((2, 2)),
            pltpu.SemaphoreType.DMA((2, 2)),
            pltpu.SemaphoreType.DMA((2,)),
            pltpu.SemaphoreType.REGULAR,
            pltpu.SemaphoreType.REGULAR,
            pltpu.SemaphoreType.REGULAR,
        ],
        compiler_params=pltpu.CompilerParams(
            collective_id=0, has_side_effects=True, vmem_limit_bytes=VMEM_LIMIT
        ),
    )(*(pltpu.with_memory_space_constraint(x, pltpu.HBM) for x in (populations, pore)))
    return pl.pallas_call(
        functools.partial(finish, across),
        out_shape=jax.ShapeDtypeStruct((count, planes, height, width), jnp.float32),
        in_specs=[pl.BlockSpec(memory_space=pltpu.VMEM)] * 2,
        out_specs=pl.BlockSpec(memory_space=pl.ANY),
        scratch_shapes=[
            pltpu.VMEM((across - 1, count, planes, rows, width), jnp.float32),
            pltpu.SemaphoreType.DMA((1 + (across - 1) * planes,)),
        ],
        compiler_params=pltpu.CompilerParams(vmem_limit_bytes=VMEM_LIMIT),
    )(post2, done)


def solution(mesh):
    return jax.shard_map(
        functools.partial(body, mesh.shape["px"], mesh.shape["py"]),
        mesh=mesh,
        in_specs=(P(None, None, ("py", "px"), None), P(None, ("py", "px"), None)),
        out_specs=P(None, None, "py", "px"),
        check_vma=False,
    )
```
